32 devices in a mesh: ctx: 8 (over z, x), uly: 4 (over y, core).
Axes of the slice: x: 2, y: 2, z: 4, core: 2. Of those that a mesh axis runs over, the one named last changes fastest.
Arguments:
- tokens: bfloat16 [4096, 2304], P(('ctx', 'uly')), may hold values from -6 to 6
- cotangent: bfloat16 [4096, 2304], P(('ctx', 'uly')), may hold values from -6 to 6
- span_order: int32 [16], replicated, may hold values from 0 to 15, as said below
- segments: int32 [4096], replicated, may hold values from 0 to 1, as said below
- w_query: bfloat16 [2304, 2048], P(('ctx', 'uly')), may hold values from -0.125 to 0.125
- w_key: bfloat16 [2304, 1024], P(('ctx', 'uly')), may hold values from -0.125 to 0.125
- w_value: bfloat16 [2304, 1024], P(('ctx', 'uly')), may hold values from -0.125 to 0.125
- w_out: bfloat16 [2304, 2048], P('ctx', 'uly'), may hold values from -0.125 to 0.125
- w_gate: bfloat16 [2304, 9216], P('ctx', 'uly'), may hold values from -0.125 to 0.125
- w_up: bfloat16 [2304, 9216], P('ctx', 'uly'), may hold values from -0.125 to 0.125
- w_down: bfloat16 [2304, 9216], P('ctx', 'uly'), may hold values from -0.0625 to 0.0625
- gain_attn_in: bfloat16 [2304], P(('ctx', 'uly')), may hold values from 0.099609375 to 1.8984375
- gain_attn_out: bfloat16 [2304], P(('ctx', 'uly')), may hold values from 0.099609375 to 1.8984375
- gain_ffn_in: bfloat16 [2304], P(('ctx', 'uly')), may hold values from 0.099609375 to 1.8984375
- gain_ffn_out: bfloat16 [2304], P(('ctx', 'uly')), may hold values from 0.099609375 to 1.8984375
Outputs:
- block_out: bfloat16 [4096, 2304], P(('ctx', 'uly'))
- grad_tokens: float32 [4096, 2304], P(('ctx', 'uly'))
- grad_query: float32 [2304, 2048], P(('ctx', 'uly'))
- grad_key: float32 [2304, 1024], P(('ctx', 'uly'))
- grad_value: float32 [2304, 1024], P(('ctx', 'uly'))
- grad_outproj: float32 [2304, 2048], P('ctx', 'uly')
- grad_gate: float32 [2304, 9216], P('ctx', 'uly')
- grad_up: float32 [2304, 9216], P('ctx', 'uly')
- grad_down: float32 [2304, 9216], P('ctx', 'uly')
- grad_gain_attn_in: float32 [2304], P(('ctx', 'uly'))
- grad_gain_attn_out: float32 [2304], P(('ctx', 'uly'))
- grad_gain_ffn_in: float32 [2304], P(('ctx', 'uly'))
- grad_gain_ffn_out: float32 [2304], P(('ctx', 'uly'))
The draws below stay inside these ranges and needn't reach their ends.
Inputs may be any that keep to these rules, and one draw needn't show every extreme that they name: `span_order`: A permutation; entries 2c and 2c + 1 are two blocks of positions that sum to 15. `segments`: never falls along the stream; 2 sequences, each of at least 1024 positions.
All inputs are finite; a program needn't handle non-finite values.
Results may differ from the reference program's by a relative error of at most 0.029.
Values may be sent and summed in bfloat16 or wider, within the bound.
A program may use at most 448 MiB of HBM per device.

```python
import math
import jax
import jax.numpy as jnp
from jax import lax

D = 2304
HEADS = 8
KV_HEADS = 4
HEAD_DIM = 256
FF = 9216
TOKENS = 4096
SPAN = 256
NCHUNK = 16


def draw_span_order(key, part):
    half = NCHUNK // 2
    first = jax.random.permutation(jax.random.fold_in(key, 11), half).astype(jnp.int32)
    flips = jax.random.randint(jax.random.fold_in(key, 12), (half,), 0, 2).astype(jnp.int32)
    leading = jnp.where(flips == 1, NCHUNK - 1 - first, first).astype(jnp.int32)
    paired = jnp.stack([leading, NCHUNK - 1 - leading], axis=1)
    return paired.reshape(NCHUNK).astype(jnp.int32)


def draw_segments(key, part):
    boundary = jax.random.randint(jax.random.fold_in(key, 21), (), TOKENS // 4, 3 * TOKENS // 4 + 1).astype(jnp.int32)
    return (jnp.arange(TOKENS, dtype=jnp.int32) >= boundary).astype(jnp.int32)


def strengthened(result, stream_key, source, target, parts, factor):
    def block_of(position):
        return (jnp.arange(result.shape[position]) // (result.shape[position] // parts)).reshape((-1,) + (1,) * (result.ndim - 1 - position))

    first = jax.random.permutation(stream_key, parts)[block_of(target)]
    far = (block_of(target) + parts // 2) % parts
    return jnp.where((block_of(source) == first) | (block_of(source) == far), factor * result, result)


def shard_levels(key, shape, shards, low, high):
    def one(position, parts):
        steps = jax.random.uniform(jax.random.fold_in(jax.random.fold_in(key, 6), position), (parts,), jnp.float32, low / len(shards), high / len(shards))
        return jnp.repeat(jnp.exp(steps), shape[position] // parts).reshape((-1,) + (1,) * (len(shape) - position - 1))

    level = one(*shards[0])
    for cut in shards[1:]:
        level = level * one(*cut)
    return level


def bell_draw(key, shape, scale, most, cuts=(), kind=jnp.bfloat16):
    drawn = scale * jax.random.normal(key, shape, jnp.float32)
    if cuts:
        drawn = drawn * shard_levels(key, shape, cuts, -0.22, 0.18)
    return jnp.clip(drawn, -most, most).astype(kind)


def noise_with(key, shape, deviation, reach, split, heavy, kind=jnp.bfloat16):
    values = deviation * jax.random.normal(key, shape, jnp.float32)
    if split:
        values = values * shard_levels(key, shape, split, -0.22, 0.18)
    return jnp.clip(strengthened(values, jax.random.fold_in(key, 3), *heavy), -reach, reach).astype(kind)


def setup_inputs(seed: int = 0) -> dict:
    seeds = jax.random.split(jax.random.key(seed), 16)
    return {
        "tokens": bell_draw(seeds[0], (TOKENS, D), 1.0, 6.0, ((0, 32),)),
        "cotangent": noise_with(seeds[1], (TOKENS, D), 1.0, 6.0, ((0, 32),), (0, 1, 32, 2.75)),
        "span_order": draw_span_order(jax.random.fold_in(seeds[15], 71), 0),
        "segments": draw_segments(jax.random.fold_in(seeds[15], 71), 0),
        "w_query": bell_draw(seeds[4], (D, HEADS * HEAD_DIM), D ** -0.5, 0.125, ((0, 32),)),
        "w_key": bell_draw(seeds[5], (D, KV_HEADS * HEAD_DIM), D ** -0.5, 0.125, ((0, 32),)),
        "w_value": bell_draw(seeds[6], (D, KV_HEADS * HEAD_DIM), D ** -0.5, 0.125, ((0, 32),)),
        "w_out": bell_draw(seeds[7], (D, HEADS * HEAD_DIM), (HEADS * HEAD_DIM) ** -0.5, 0.125, ((0, 8), (1, 4))),
        "w_gate": bell_draw(seeds[8], (D, FF), D ** -0.5, 0.125, ((0, 8), (1, 4))),
        "w_up": bell_draw(seeds[9], (D, FF), D ** -0.5, 0.125, ((0, 8), (1, 4))),
        "w_down": bell_draw(seeds[10], (D, FF), FF ** -0.5, 0.0625, ((0, 8), (1, 4))),
        "gain_attn_in": jnp.clip(1.0 + 0.18 * jax.random.normal(seeds[11], (D,), jnp.float32), 0.099609375, 1.8984375).astype(jnp.bfloat16),
        "gain_attn_out": jnp.clip(1.0 + 0.18 * jax.random.normal(seeds[12], (D,), jnp.float32), 0.099609375, 1.8984375).astype(jnp.bfloat16),
        "gain_ffn_in": jnp.clip(1.0 + 0.18 * jax.random.normal(seeds[13], (D,), jnp.float32), 0.099609375, 1.8984375).astype(jnp.bfloat16),
        "gain_ffn_out": jnp.clip(1.0 + 0.18 * jax.random.normal(seeds[14], (D,), jnp.float32), 0.099609375, 1.8984375).astype(jnp.bfloat16),
    }


norm_eps = 1e-06
soft_cap = 50.0
rotary_base = 10000.0
gelu_coef = 0.7978845608028654
cubic_coef = 0.044715

def rms_scale(values):
    return lax.rsqrt(lax.optimization_barrier(jnp.mean(values * values, axis=-1, keepdims=True)) + norm_eps)

def norm_apply(values, gain):
    return values * rms_scale(values) * (1.0 + gain.astype(jnp.float32))

def norm_back(values, gain, grad):
    scale = rms_scale(values)
    weight = 1.0 + gain.astype(jnp.float32)
    inner = lax.optimization_barrier(jnp.mean(grad * weight * values, axis=-1, keepdims=True))
    d_values = scale * weight * grad - values * (scale * scale * scale) * inner
    d_gain = lax.optimization_barrier(jnp.sum(grad * values * scale, axis=0))
    return (d_values, d_gain)

def gelu_value(values):
    inner = gelu_coef * (values + cubic_coef * values * values * values)
    return 0.5 * values * (1.0 + jnp.tanh(inner))

def gelu_slope(values):
    inner = gelu_coef * (values + cubic_coef * values * values * values)
    tanh_part = jnp.tanh(inner)
    return 0.5 * (1.0 + tanh_part) + 0.5 * values * (1.0 - tanh_part * tanh_part) * gelu_coef * (1.0 + 3.0 * cubic_coef * values * values)

def rotary_tables(positions, half):
    freqs = rotary_base ** (-jnp.arange(half).astype(jnp.float32) / half)
    angles = positions.astype(jnp.float32)[:, None] * freqs[None, :]
    return (jnp.cos(angles), jnp.sin(angles))

def rotary(values, cosines, sines):
    half = values.shape[-1] // 2
    first, second = (values[..., :half], values[..., half:])
    cos_rows, sin_rows = (cosines[:, None, :], sines[:, None, :])
    return jnp.concatenate([first * cos_rows - second * sin_rows, second * cos_rows + first * sin_rows], axis=-1)

def rotary_back(values, cosines, sines):
    half = values.shape[-1] // 2
    first, second = (values[..., :half], values[..., half:])
    cos_rows, sin_rows = (cosines[:, None, :], sines[:, None, :])
    return jnp.concatenate([first * cos_rows + second * sin_rows, second * cos_rows - first * sin_rows], axis=-1)

def held_positions(span_order, held, span):
    return (jnp.take(span_order, held // span).astype(jnp.int32) * span + held % span).astype(jnp.int32)

def contract_rows(left, right):
    return lax.dot_general(left, right, (((0,), (0,)), ((), ())), preferred_element_type=jnp.float32)

def contract_cols(left, right):
    return lax.dot_general(left, right, (((1,), (1,)), ((), ())), preferred_element_type=jnp.float32)

def attention_forward(queries, keys, values, allowed):
    repeat = queries.shape[1] // keys.shape[1]
    outputs = []
    logs = []
    for head in range(queries.shape[1]):
        kv_head = head // repeat
        scores = jnp.dot(queries[:, head], keys[:, kv_head].T, preferred_element_type=jnp.float32)
        capped = soft_cap * jnp.tanh(scores / soft_cap)
        weights = jnp.where(allowed, jnp.exp(capped), 0.0)
        denom = lax.optimization_barrier(jnp.sum(weights, axis=-1))
        accum = jnp.dot(weights.astype(jnp.bfloat16), values[:, kv_head], preferred_element_type=jnp.float32)
        outputs.append((accum / denom[:, None]).astype(jnp.bfloat16))
        logs.append(jnp.log(denom))
    return (jnp.stack(outputs, axis=1), jnp.stack(logs, axis=1))

def attention_backward(queries, keys, values, grad_heads, lse, dsum, allowed):
    kv_heads = keys.shape[1]
    repeat = queries.shape[1] // kv_heads
    grad_q = []
    grad_k = []
    grad_v = []
    for kv_head in range(kv_heads):
        key_rows = keys[:, kv_head]
        value_rows = values[:, kv_head]
        part_k = jnp.zeros(key_rows.shape, jnp.float32)
        part_v = jnp.zeros(value_rows.shape, jnp.float32)
        for head in range(kv_head * repeat, (kv_head + 1) * repeat):
            scores = jnp.dot(queries[:, head], key_rows.T, preferred_element_type=jnp.float32)
            capped = soft_cap * jnp.tanh(scores / soft_cap)
            probs = jnp.where(allowed, jnp.exp(capped - lse[:, head][:, None]), 0.0)
            dprob = jnp.dot(grad_heads[:, head], value_rows.T, preferred_element_type=jnp.float32)
            dscore = probs * (dprob - dsum[:, head][:, None]) * (1.0 - capped / soft_cap * (capped / soft_cap))
            score_b = dscore.astype(jnp.bfloat16)
            prob_b = probs.astype(jnp.bfloat16)
            grad_q.append(jnp.dot(score_b, key_rows, preferred_element_type=jnp.float32))
            part_k = part_k + contract_rows(score_b, queries[:, head])
            part_v = part_v + contract_rows(prob_b, grad_heads[:, head])
        grad_k.append(part_k)
        grad_v.append(part_v)
    return (jnp.stack(grad_q, axis=1), jnp.stack(grad_k, axis=1), jnp.stack(grad_v, axis=1))

def reference(tokens, cotangent, span_order, segments, w_query, w_key, w_value, w_out, w_gate, w_up, w_down, gain_attn_in, gain_attn_out, gain_ffn_in, gain_ffn_out):
    held = jnp.arange(TOKENS, dtype=jnp.int32)
    positions = held_positions(span_order, held, SPAN)
    seq_ids = jnp.take(segments, positions).astype(jnp.int32)
    cosines, sines = rotary_tables(positions, HEAD_DIM // 2)
    q_scale = float(HEAD_DIM) ** (-0.5)
    inputs = tokens.astype(jnp.float32)
    normed_in = norm_apply(inputs, gain_attn_in).astype(jnp.bfloat16)
    queries = jnp.dot(normed_in, w_query, preferred_element_type=jnp.float32).reshape(TOKENS, HEADS, HEAD_DIM)
    queries = (rotary(queries, cosines, sines) * q_scale).astype(jnp.bfloat16)
    keys = jnp.dot(normed_in, w_key, preferred_element_type=jnp.float32).reshape(TOKENS, KV_HEADS, HEAD_DIM)
    keys = rotary(keys, cosines, sines).astype(jnp.bfloat16)
    values = jnp.dot(normed_in, w_value, preferred_element_type=jnp.float32).astype(jnp.bfloat16).reshape(TOKENS, KV_HEADS, HEAD_DIM)
    q_block = math.gcd(TOKENS, 2048)
    blocks = TOKENS // q_block
    block_ids = jnp.arange(blocks, dtype=jnp.int32)

    def block_mask(start):
        q_pos = lax.dynamic_slice_in_dim(positions, start, q_block, 0)
        q_seq = lax.dynamic_slice_in_dim(seq_ids, start, q_block, 0)
        return (positions[None, :] <= q_pos[:, None]) & (seq_ids[None, :] == q_seq[:, None])

    def forward_block(carry, block_index):
        start = (block_index * q_block).astype(jnp.int32)
        q_rows = lax.dynamic_slice_in_dim(queries, start, q_block, 0)
        outputs, logs = attention_forward(q_rows, keys, values, block_mask(start))
        return (carry, (outputs, logs))
    unused, (attn_heads, lse) = lax.scan(forward_block, jnp.zeros((), jnp.float32), block_ids)
    attn_heads = attn_heads.reshape(TOKENS, HEADS, HEAD_DIM)
    lse = lse.reshape(TOKENS, HEADS)
    head_rows = attn_heads.reshape(TOKENS, HEADS * HEAD_DIM)
    attn_out = contract_cols(head_rows, w_out)
    hidden_in = inputs + norm_apply(attn_out, gain_attn_out)
    grad_out = cotangent.astype(jnp.float32)

    def ffn_block(carry, block_index):
        acc_gate, acc_up, acc_down, acc_three, acc_four = carry
        start = (block_index * q_block).astype(jnp.int32)
        resid = lax.dynamic_slice_in_dim(hidden_in, start, q_block, 0)
        grad_rows = lax.dynamic_slice_in_dim(grad_out, start, q_block, 0)
        normed_mid = norm_apply(resid, gain_ffn_in).astype(jnp.bfloat16)
        gate = jnp.dot(normed_mid, w_gate, preferred_element_type=jnp.float32)
        upper = jnp.dot(normed_mid, w_up, preferred_element_type=jnp.float32)
        hidden = (gelu_value(gate) * upper).astype(jnp.bfloat16)
        ffn_out = contract_cols(hidden, w_down)
        block_rows = (resid + norm_apply(ffn_out, gain_ffn_out)).astype(jnp.bfloat16)
        d_ffn, d_four = norm_back(ffn_out, gain_ffn_out, grad_rows)
        d_ffn_b = d_ffn.astype(jnp.bfloat16)
        d_hidden = jnp.dot(d_ffn_b, w_down, preferred_element_type=jnp.float32)
        d_gate = (d_hidden * upper * gelu_slope(gate)).astype(jnp.bfloat16)
        d_upper = (d_hidden * gelu_value(gate)).astype(jnp.bfloat16)
        d_mid = contract_cols(d_gate, w_gate) + contract_cols(d_upper, w_up)
        d_resid, d_three = norm_back(resid, gain_ffn_in, d_mid)
        carry = (acc_gate + contract_rows(normed_mid, d_gate), acc_up + contract_rows(normed_mid, d_upper), acc_down + contract_rows(d_ffn_b, hidden), acc_three + d_three, acc_four + d_four)
        return (carry, (block_rows, grad_rows + d_resid))
    zero_ff = jnp.zeros((D, FF), jnp.float32)
    zero_d = jnp.zeros((D,), jnp.float32)
    (grad_gate, grad_up, grad_down, grad_three, grad_four), (block_out, grad_hidden) = lax.scan(ffn_block, (zero_ff, zero_ff, zero_ff, zero_d, zero_d), block_ids)
    block_out = block_out.reshape(TOKENS, D)
    grad_hidden = grad_hidden.reshape(TOKENS, D)
    d_attn, grad_two = norm_back(attn_out, gain_attn_out, grad_hidden)
    d_attn_b = d_attn.astype(jnp.bfloat16)
    grad_outproj = contract_rows(d_attn_b, head_rows)
    grad_heads = jnp.dot(d_attn_b, w_out, preferred_element_type=jnp.float32).astype(jnp.bfloat16).reshape(TOKENS, HEADS, HEAD_DIM)
    dsum = lax.optimization_barrier(jnp.sum(grad_heads.astype(jnp.float32) * attn_heads.astype(jnp.float32), axis=-1))

    def backward_block(carry, block_index):
        acc_k, acc_v = carry
        start = (block_index * q_block).astype(jnp.int32)
        q_rows = lax.dynamic_slice_in_dim(queries, start, q_block, 0)
        g_rows = lax.dynamic_slice_in_dim(grad_heads, start, q_block, 0)
        l_rows = lax.dynamic_slice_in_dim(lse, start, q_block, 0)
        s_rows = lax.dynamic_slice_in_dim(dsum, start, q_block, 0)
        part_q, part_k, part_v = attention_backward(q_rows, keys, values, g_rows, l_rows, s_rows, block_mask(start))
        return ((acc_k + part_k, acc_v + part_v), part_q)
    zero_kv = jnp.zeros((TOKENS, KV_HEADS, HEAD_DIM), jnp.float32)
    (total_k, total_v), total_q = lax.scan(backward_block, (zero_kv, zero_kv), block_ids)
    total_q = total_q.reshape(TOKENS, HEADS, HEAD_DIM)
    grad_q = (rotary_back(total_q, cosines, sines) * q_scale).astype(jnp.bfloat16).reshape(TOKENS, HEADS * HEAD_DIM)
    grad_k = rotary_back(total_k, cosines, sines).astype(jnp.bfloat16).reshape(TOKENS, KV_HEADS * HEAD_DIM)
    grad_v = total_v.astype(jnp.bfloat16).reshape(TOKENS, KV_HEADS * HEAD_DIM)
    d_in = contract_cols(grad_q, w_query) + contract_cols(grad_k, w_key) + contract_cols(grad_v, w_value)
    d_inputs, grad_one = norm_back(inputs, gain_attn_in, d_in)
    grad_tokens = grad_hidden + d_inputs
    grad_query = contract_rows(normed_in, grad_q)
    grad_key = contract_rows(normed_in, grad_k)
    grad_value = contract_rows(normed_in, grad_v)
    return (block_out, grad_tokens, grad_query, grad_key, grad_value, grad_outproj, grad_gate, grad_up, grad_down, grad_one, grad_two, grad_three, grad_four)
```

```python
import functools

import jax
import jax.numpy as jnp
from jax import lax
from jax.experimental import pallas as pl
from jax.experimental.pallas import tpu as pltpu
from jax.sharding import PartitionSpec as P

HEAD_DIM = 256
AXES = ("ctx", "uly")

norm_eps = 1e-06
soft_cap = 50.0
rotary_base = 10000.0
gelu_coef = 0.7978845608028654
cubic_coef = 0.044715


bf16 = jnp.bfloat16
f32 = jnp.float32


def rms_scale(values):
    return lax.rsqrt(jnp.mean(values * values, axis=-1, keepdims=True) + norm_eps)


def norm_apply(values, weight):
    return values * rms_scale(values) * weight


def norm_grad(values, weight, grad):
    scale = rms_scale(values)
    inner = jnp.mean(grad * weight * values, axis=-1, keepdims=True)
    return scale * weight * grad - values * (scale * scale * scale) * inner


def gain_part(values, grad):
    return jnp.sum(grad * values * rms_scale(values), axis=0)


def gelu_parts(values):
    inner = gelu_coef * (values + cubic_coef * values * values * values)
    tanh_part = jnp.tanh(inner)
    value = 0.5 * values * (1.0 + tanh_part)
    slope = 0.5 * (1.0 + tanh_part) + 0.5 * values * (1.0 - tanh_part * tanh_part) * gelu_coef * (
        1.0 + 3.0 * cubic_coef * values * values
    )
    return value, slope


def rotary(values, cosines, sines, sign):
    half = HEAD_DIM // 2
    parts = []
    for start in range(0, values.shape[1], HEAD_DIM):
        first = values[:, start : start + half]
        second = values[:, start + half : start + HEAD_DIM]
        parts.append(first * cosines - sign * second * sines)
        parts.append(second * cosines + sign * first * sines)
    return jnp.concatenate(parts, axis=1)


def dot(left, right, left_dim=1, right_dim=0):
    return lax.dot_general(
        left, right, (((left_dim,), (right_dim,)), ((), ())), preferred_element_type=f32
    )


class Plan:
    def __init__(self, mesh):
        grid = mesh.devices
        self.contexts, self.ulysses = mesh.shape["ctx"], mesh.shape["uly"]
        self.cores = sum(tuple(d.coords) == tuple(grid[0, 0].coords) for d in grid[0])
        self.layers = len({d.coords[2] for d in grid[:, 0]})
        self.sides = self.contexts // self.layers
        self.rows = self.ulysses // self.cores
        self.halves = self.layers // self.cores

    def split(self, device):
        ctx, uly = divmod(device, self.ulysses)
        return (*divmod(ctx, self.sides), *divmod(uly, self.cores))

    def join(self, layer, side, row, core):
        return (layer * self.sides + side) * self.ulysses + row * self.cores + core

    def perm(self, target):
        count = self.contexts * self.ulysses
        return [(d, self.join(*target(*self.split(d)))) for d in range(count)]

    def here(self):
        layer, side = jnp.divmod(lax.axis_index("ctx"), self.sides)
        row, core = jnp.divmod(lax.axis_index("uly"), self.cores)
        return layer, side, row, core


class Ring:
    def __init__(self, plan, outer, inner, place, locate):
        self.size = outer * inner
        self.inner = inner

        def cell(index):
            out, rest = divmod(index % self.size, inner)
            return out, (rest if out % 2 == 0 else inner - 1 - rest)

        def index_of(out, inn):
            return out * inner + (inn if out % 2 == 0 else inner - 1 - inn)

        self.cells = [cell(i) for i in range(self.size)]

        def shifted(step):
            def target(*where):
                return place(where, *cell(index_of(*locate(where)) + step))

            return plan.perm(target)

        self.ahead, self.behind = shifted(1), shifted(-1)

    def position(self, out, inn):
        rest = jnp.where(out % 2 == 0, inn, self.inner - 1 - inn)
        return out * self.inner + rest


def move(values, perm):
    return lax.ppermute(values, AXES, perm)


def both(*values):
    return lax.optimization_barrier(values)


def after(values, *earlier):
    return lax.optimization_barrier((values, *earlier))[0]


def ring_gather(block, ring):
    size = ring.size
    found = {0: block}
    if size == 2:
        found[1] = move(block, ring.ahead)
        return [found[0], found[1]]
    forth = back = block
    middle = size // 2
    for step in range(1, middle):
        forth, back = both(move(forth, ring.ahead), move(back, ring.behind))
        found[size - step], found[step] = forth, back
    cut = block.shape[0] // 2
    forth = move(forth[:cut], ring.ahead)
    back = move(back[cut:], ring.behind)
    found[middle] = jnp.concatenate([forth, back], axis=0)
    return [found[k] for k in range(size)]


def ring_scatter(parts, ring, kind=bf16):
    size = ring.size
    if size == 2:
        return parts[0].astype(f32) + move(parts[1].astype(kind), ring.ahead).astype(f32)
    middle = size // 2
    cut = parts[0].shape[0] // 2
    forth = move(parts[middle][:cut].astype(kind), ring.ahead)
    back = move(parts[middle][cut:].astype(kind), ring.behind)
    forth, back = both(forth, back)
    for left in range(middle - 1, 0, -1):
        fore, aft = parts[left].astype(f32), parts[size - left].astype(f32)
        if left == middle - 1:
            fore = jnp.concatenate([fore[:cut] + forth.astype(f32), fore[cut:]], axis=0)
            aft = jnp.concatenate([aft[:cut], aft[cut:] + back.astype(f32)], axis=0)
        else:
            fore, aft = fore + forth.astype(f32), aft + back.astype(f32)
        forth = move(fore.astype(kind), ring.ahead)
        back = move(aft.astype(kind), ring.behind)
        forth, back = both(forth, back)
    return parts[0].astype(f32) + forth.astype(f32) + back.astype(f32)


def place_rows(blocks, indices, count):
    first = blocks[0]
    out = jnp.zeros((count, *first.shape), first.dtype)
    for block, index in zip(blocks, indices, strict=True):
        out = lax.dynamic_update_slice(out, block[None], (index, *(0,) * first.ndim))
    return out


def take_block(values, index, size):
    return lax.dynamic_slice_in_dim(values, index * size, size, 0)


def visible(q_first, k_first, boundary, span):
    q_pos = q_first + lax.broadcasted_iota(jnp.int32, (span, span), 0)
    k_pos = k_first + lax.broadcasted_iota(jnp.int32, (span, span), 1)
    low = jnp.where(q_pos >= boundary, boundary, 0)
    return (k_pos <= q_pos) & (k_pos >= low)


def active(q_first, k_first, boundary, span):
    split = (q_first >= boundary) & (k_first + span <= boundary)
    return (k_first <= q_first) & jnp.logical_not(split)


def attend_kernel(span, repeat, count, qp, kp, bd, q_ref, kv_ref, o_ref, lse_ref, acc, den):
    i, j = pl.program_id(0), pl.program_id(1)

    @pl.when(j == 0)
    def _():
        acc[...] = jnp.zeros_like(acc)
        den[...] = jnp.zeros_like(den)

    q_first, k_first, boundary = qp[i], kp[j], bd[0]

    @pl.when(active(q_first, k_first, boundary, span))
    def _():
        allowed = visible(q_first, k_first, boundary, span)
        keys, values = kv_ref[:, :HEAD_DIM], kv_ref[:, HEAD_DIM:]
        for r in range(repeat):
            cols = slice(r * HEAD_DIM, (r + 1) * HEAD_DIM)
            scores = dot(q_ref[:, cols], keys, 1, 1)
            weights = jnp.where(
                allowed, jnp.exp(soft_cap * jnp.tanh(scores * (1.0 / soft_cap))), 0.0
            )
            den[r] += jnp.sum(weights, axis=1, keepdims=True)
            acc[:, cols] += dot(weights.astype(bf16), values)

    @pl.when(j == count - 1)
    def _():
        for r in range(repeat):
            cols = slice(r * HEAD_DIM, (r + 1) * HEAD_DIM)
            total = den[r][:, :1]
            o_ref[:, cols] = (acc[:, cols] / total).astype(bf16)
            lse_ref[:, r * 128 : (r + 1) * 128] = jnp.broadcast_to(jnp.log(total), (span, 128))


def attend(q, kv, q_pos, k_pos, boundary, span):
    rows, width = q.shape
    repeat = width // HEAD_DIM
    count = kv.shape[0] // span
    spec = pltpu.PrefetchScalarGridSpec(
        num_scalar_prefetch=3,
        grid=(rows // span, count),
        in_specs=[
            pl.BlockSpec((span, width), lambda i, j, *_: (i, 0)),
            pl.BlockSpec((span, kv.shape[1]), lambda i, j, *_: (j, 0)),
        ],
        out_specs=[
            pl.BlockSpec((span, width), lambda i, j, *_: (i, 0)),
            pl.BlockSpec((span, 128 * repeat), lambda i, j, *_: (i, 0)),
        ],
        scratch_shapes=[
            pltpu.VMEM((span, width), f32),
            pltpu.VMEM((repeat, span, 128), f32),
        ],
    )
    flops = 2 * rows * kv.shape[0] * width
    return pl.pallas_call(
        functools.partial(attend_kernel, span, repeat, count),
        out_shape=[
            jax.ShapeDtypeStruct((rows, width), bf16),
            jax.ShapeDtypeStruct((rows, 128 * repeat), f32),
        ],
        grid_spec=spec,
        compiler_params=pltpu.CompilerParams(dimension_semantics=("arbitrary", "arbitrary")),
        cost_estimate=pl.CostEstimate(
            flops=flops, bytes_accessed=2 * kv.size * 2, transcendentals=rows * kv.shape[0] * repeat
        ),
    )(q_pos, k_pos, boundary, q, kv)


def attend_back_kernel(
    span, repeat, count, blocks, qp, kp, bd, q_ref, g_ref, lse_ref, ds_ref, kv_ref, dq_ref, dkv_ref, acc, dk, dv
):
    j, i = pl.program_id(0), pl.program_id(1)

    @pl.when((j == 0) & (i == 0))
    def _():
        acc[...] = jnp.zeros_like(acc)

    @pl.when(i == 0)
    def _():
        dk[...] = jnp.zeros_like(dk)
        dv[...] = jnp.zeros_like(dv)

    q_first, k_first, boundary = qp[i], kp[j], bd[0]

    @pl.when(active(q_first, k_first, boundary, span))
    def _():
        allowed = visible(q_first, k_first, boundary, span)
        keys, values = kv_ref[:, :HEAD_DIM], kv_ref[:, HEAD_DIM:]
        rows = pl.ds(pl.multiple_of(i * span, span), span)
        for r in range(repeat):
            cols = slice(r * HEAD_DIM, (r + 1) * HEAD_DIM)
            query, grad = q_ref[rows, cols], g_ref[rows, cols]
            lse = lse_ref[rows, r * 128 : r * 128 + 1]
            dsum = ds_ref[rows, r * 128 : r * 128 + 1]
            bent = jnp.tanh(dot(query, keys, 1, 1) * (1.0 / soft_cap))
            probs = jnp.where(allowed, jnp.exp(soft_cap * bent - lse), 0.0)
            dprob = dot(grad, values, 1, 1)
            dscore = (probs * (dprob - dsum) * (1.0 - bent * bent)).astype(bf16)
            acc[rows, cols] += dot(dscore, keys)
            dk[...] += dot(dscore, query, 0, 0)
            dv[...] += dot(probs.astype(bf16), grad, 0, 0)

    @pl.when(i == blocks - 1)
    def _():
        dkv_ref[:, :HEAD_DIM] = dk[...].astype(dkv_ref.dtype)
        dkv_ref[:, HEAD_DIM:] = dv[...].astype(dkv_ref.dtype)

    @pl.when((j == count - 1) & (i == blocks - 1))
    def _():
        dq_ref[...] = acc[...]


def attend_back(q, grad, lse, dsum, kv, q_pos, k_pos, boundary, span):
    rows, width = q.shape
    repeat = width // HEAD_DIM
    count, blocks = kv.shape[0] // span, rows // span
    whole = lambda w: pl.BlockSpec((rows, w), lambda j, i, *_: (0, 0))
    spec = pltpu.PrefetchScalarGridSpec(
        num_scalar_prefetch=3,
        grid=(count, blocks),
        in_specs=[
            whole(width),
            whole(width),
            whole(128 * repeat),
            whole(128 * repeat),
            pl.BlockSpec((span, kv.shape[1]), lambda j, i, *_: (j, 0)),
        ],
        out_specs=[
            whole(width),
            pl.BlockSpec((span, kv.shape[1]), lambda j, i, *_: (j, 0)),
        ],
        scratch_shapes=[
            pltpu.VMEM((rows, width), f32),
            pltpu.VMEM((span, HEAD_DIM), f32),
            pltpu.VMEM((span, HEAD_DIM), f32),
        ],
    )
    return pl.pallas_call(
        functools.partial(attend_back_kernel, span, repeat, count, blocks),
        out_shape=[
            jax.ShapeDtypeStruct((rows, width), f32),
            jax.ShapeDtypeStruct(kv.shape, bf16),
        ],
        grid_spec=spec,
        compiler_params=pltpu.CompilerParams(dimension_semantics=("arbitrary", "arbitrary")),
        cost_estimate=pl.CostEstimate(
            flops=5 * rows * kv.shape[0] * width,
            bytes_accessed=2 * kv.size * 2,
            transcendentals=rows * kv.shape[0] * repeat,
        ),
    )(q_pos, k_pos, boundary, q, grad, lse, dsum, kv)


def on_device(
    plan,
    tokens,
    cotangent,
    span_order,
    segments,
    w_query,
    w_key,
    w_value,
    w_out,
    w_gate,
    w_up,
    w_down,
    gain_attn_in,
    gain_attn_out,
    gain_ffn_in,
    gain_ffn_out,
):
    rows, width = tokens.shape
    contexts, ulysses = plan.contexts, plan.ulysses
    layers, sides, cores, halves = plan.layers, plan.sides, plan.cores, plan.halves
    group_rows = rows * ulysses
    span = group_rows // 2
    q_scale = float(HEAD_DIM) ** (-0.5)
    uly, ctx = lax.axis_index("uly"), lax.axis_index("ctx")
    layer, side, row, core = plan.here()

    ctx_ring = Ring(
        plan, sides, layers, lambda w, out, inn: (inn, out, w[2], w[3]), lambda w: (w[1], w[0])
    )
    ffn_ring = Ring(
        plan, plan.rows, layers, lambda w, out, inn: (inn, w[1], out, w[3]), lambda w: (w[2], w[0])
    )
    side_ring = Ring(
        plan, 1, sides, lambda w, out, inn: (w[0], inn, w[2], w[3]), lambda w: (0, w[1])
    )
    row_ring = Ring(
        plan, 1, plan.rows, lambda w, out, inn: (w[0], w[1], inn, w[3]), lambda w: (0, w[2])
    )
    core_ring = Ring(
        plan, 1, cores, lambda w, out, inn: (w[0], w[1], w[2], inn), lambda w: (0, w[3])
    )
    ctx_cells = jnp.array([inn * sides + out for out, inn in ctx_ring.cells], jnp.int32)
    ctx_place = ctx_ring.position(side, layer)
    ring_ctx = [ctx_cells[(ctx_place + k) % contexts] for k in range(contexts)]

    def group_gather(values):
        mine = ring_gather(values, row_ring)
        blocks, where = [], []
        for k, block in enumerate(mine):
            for m, found in enumerate(ring_gather(block, core_ring)):
                blocks.append(found)
                where.append((row + k) % plan.rows * cores + (core + m) % cores)
        return place_rows(blocks, where, ulysses).reshape(group_rows, values.shape[1]), mine[-1]

    def group_scatter(values):
        parts = values.reshape(plan.rows, cores, rows, values.shape[1])

        def part(k, m):
            at = ((row + k) % plan.rows, (core + m) % cores, 0, 0)
            return lax.dynamic_slice(parts, at, (1, 1, *parts.shape[2:]))[0, 0]

        summed = [
            ring_scatter([part(k, m) for m in range(cores)], core_ring) for k in range(plan.rows)
        ]
        return ring_scatter(summed, row_ring)

    def ctx_gather(values):
        found = ring_gather(values, ctx_ring)
        out = place_rows(found, ring_ctx, contexts).reshape(-1, values.shape[1])
        return out, found[contexts // 2]

    def ctx_scatter(values):
        size = values.shape[0] // contexts
        return ring_scatter([take_block(values, ring_ctx[k], size) for k in range(contexts)], ctx_ring)

    shard = gain_attn_in.shape[0]
    places = (ctx_place, row, core)
    tiny_rings = (ctx_ring, row_ring, core_ring)
    ring_order = [inn * sides + out for out, inn in ctx_ring.cells]

    def turn(values, axis, back):
        count, place = values.shape[axis], places[axis]
        start = place if back else (count - place) % count
        twice = jnp.concatenate([values, values], axis=axis)
        return lax.dynamic_slice_in_dim(twice, start, count, axis)

    def spread_gains(packed):
        found = packed
        for axis in (2, 1, 0):
            found = jnp.stack(ring_gather(found, tiny_rings[axis]))
        for axis in range(3):
            found = turn(found, axis, False)
        found = jnp.stack([found[ring_order.index(c)] for c in range(contexts)])
        found = found.reshape(contexts * ulysses, *packed.shape)[:, :4, :shard]
        return jnp.transpose(found, (1, 0, 2)).reshape(4, width)

    def sum_gains(parts):
        count = parts.shape[0]
        found = jnp.transpose(parts.reshape(count, contexts * ulysses, shard), (1, 0, 2))
        found = jnp.pad(found, ((0, 0), (0, -count % 8), (0, -shard % 128)))
        found = found.reshape(contexts, plan.rows, cores, *found.shape[1:])
        found = jnp.stack([found[c] for c in ring_order])
        for axis in range(3):
            found = turn(found, axis, True)
        for axis in (2, 1, 0):
            entries = [lax.index_in_dim(found, k, axis, False) for k in range(found.shape[axis])]
            found = ring_scatter(entries, tiny_rings[axis], f32)
        return found[:count, :shard]

    packed = jnp.stack([gain_attn_in, gain_attn_out, gain_ffn_in, gain_ffn_out])
    packed = jnp.pad(packed, ((0, 4), (0, -shard % 128)))
    gains = spread_gains(packed).astype(f32)
    weight_one, weight_two, weight_three, weight_four = (1.0 + gains[k][None] for k in range(4))

    own_spans = lax.dynamic_slice_in_dim(span_order, 2 * ctx, 2, 0) * span
    boundary = jnp.sum((segments == 0).astype(jnp.int32)).reshape(1)
    ring_spans = jnp.concatenate(
        [lax.dynamic_slice_in_dim(span_order, 2 * c, 2, 0) for c in ring_ctx]
    ) * span
    group_pos = (own_spans[:, None] + jnp.arange(span, dtype=jnp.int32)[None, :]).reshape(-1)
    half = HEAD_DIM // 2
    freqs = rotary_base ** (-jnp.arange(half).astype(f32) / half)
    angles = group_pos.astype(f32)[:, None] * freqs[None, :]
    cosines, sines = jnp.cos(angles), jnp.sin(angles)

    q_cols, k_cols = w_query.shape[1] // ulysses, w_key.shape[1] // ulysses
    mixed = jnp.concatenate(
        [
            w_query.reshape(-1, ulysses, q_cols),
            w_key.reshape(-1, ulysses, k_cols),
            w_value.reshape(-1, ulysses, k_cols),
        ],
        axis=2,
    )
    mixed = jnp.transpose(mixed, (1, 0, 2))
    mixed = lax.all_to_all(mixed, "uly", split_axis=0, concat_axis=0, tiled=True)
    col_qkv, qkv_last = ctx_gather(mixed.reshape(-1, mixed.shape[2]))
    tok_group, tok_first = group_gather(tokens)
    tok_rows = tok_group.astype(f32)
    normed_in = norm_apply(tok_rows, weight_one).astype(bf16)
    qkv = dot(normed_in, col_qkv)
    queries = (rotary(qkv[:, :q_cols], cosines, sines, 1.0) * q_scale).astype(bf16)
    keys = rotary(qkv[:, q_cols : q_cols + k_cols], cosines, sines, 1.0).astype(bf16)
    values = qkv[:, q_cols + k_cols :].astype(bf16)
    col_out, out_last = ctx_gather(after(w_out, qkv_last))
    kv_blocks = ring_gather(jnp.concatenate([keys, values], axis=1), ctx_ring)
    kv = jnp.concatenate(kv_blocks, axis=0)
    kv_last = kv_blocks[contexts // 2]

    slice_cols = w_gate.shape[1] // halves

    def slice_perm(p):
        return plan.perm(lambda l, s, r, c: (c * halves + (l + p) % halves, s, r, l // halves))

    def slice_back(p):
        return [(b, a) for a, b in slice_perm(p)]

    def pick(options, index):
        out = options[0]
        for k in range(1, len(options)):
            out = jnp.where(index == k, options[k], out)
        return out

    def slice_gather(weights, first, second):
        weights = after(weights, first)
        cuts = [weights[:, h * slice_cols : (h + 1) * slice_cols] for h in range(halves)]
        blocks, where = [], []
        for p in range(halves):
            piece = move(pick(cuts, (layer + p) % halves), slice_perm(p))
            piece = piece if second is None else after(piece, second)
            for k, sided in enumerate(ring_gather(piece, side_ring)):
                for m, found in enumerate(ring_gather(sided, core_ring)):
                    origin = (core + m) % cores * halves + (layer - p) % halves
                    blocks.append(found)
                    where.append(origin * sides + (side + k) % sides)
        return place_rows(blocks, where, contexts).reshape(width, slice_cols)

    def slice_scatter(grad, second):
        parts = grad.reshape(cores, halves, sides, -1, slice_cols)
        size = parts.shape[3]

        def part(m):
            at = ((core + m) % cores, 0, 0, 0, 0)
            return lax.dynamic_slice(parts, at, (1, *parts.shape[1:]))[0]

        summed = ring_scatter([part(m) for m in range(cores)], core_ring)

        def side_part(k):
            at = (0, (side + k) % sides, 0, 0)
            found = lax.dynamic_slice(summed, at, (halves, 1, size, slice_cols))
            return found.reshape(halves * size, slice_cols)

        summed = ring_scatter([side_part(k) for k in range(sides)], side_ring).astype(bf16)
        summed = after(summed.reshape(halves, size, slice_cols), second)
        got = []
        for p in range(halves):
            piece = lax.dynamic_index_in_dim(summed, (layer - p) % halves, 0, keepdims=False)
            got.append(move(piece, slice_back(p)))
        cuts = [pick(got, (h - layer) % halves) for h in range(halves)]
        return jnp.concatenate(cuts, axis=1).astype(f32)

    ffn_gate = slice_gather(w_gate, tok_first, qkv_last)
    ffn_up = slice_gather(w_up, kv_last, None)
    ffn_down = slice_gather(w_down, kv_last, None)

    head_o, lse = attend(queries, kv, own_spans, ring_spans, boundary, span)
    attn_out = group_scatter(dot(head_o, col_out, 1, 1))
    tok_own = tokens.astype(f32)
    hidden_in = tok_own + norm_apply(attn_out, weight_two)
    normed_own = norm_apply(hidden_in, weight_three).astype(bf16)

    size = ffn_ring.size
    order = [0]
    for k in range(1, size // 2):
        order += [k, size - k]
    order.append(size // 2)

    def ffn_gather(values):
        found = ring_gather(values, ffn_ring)
        return jnp.concatenate([found[k] for k in order], axis=0)

    def ffn_scatter(values):
        parts = [None] * size
        for n, k in enumerate(order):
            parts[k] = values[n * rows : (n + 1) * rows]
        return ring_scatter(parts, ffn_ring)

    normed_mid = ffn_gather(normed_own)
    gate = dot(normed_mid, ffn_gate)
    upper = dot(normed_mid, ffn_up)
    gate_value, gate_slope = gelu_parts(gate)
    hidden = (gate_value * upper).astype(bf16)
    ffn_out = ffn_scatter(dot(hidden, ffn_down, 1, 1))
    block_out = (hidden_in + norm_apply(ffn_out, weight_four)).astype(bf16)
    cot_own = cotangent.astype(f32)
    d_ffn = ffn_gather(norm_grad(ffn_out, weight_four, cot_own).astype(bf16))
    d_hidden = dot(d_ffn, ffn_down)
    d_gate = (d_hidden * upper * gate_slope).astype(bf16)
    d_upper = (d_hidden * gate_value).astype(bf16)
    d_mid = ffn_scatter(dot(d_gate, ffn_gate, 1, 1) + dot(d_upper, ffn_up, 1, 1))
    grad_hidden = cot_own + norm_grad(hidden_in, weight_three, d_mid)
    grad_down = slice_scatter(dot(d_ffn, hidden, 0, 0), d_mid)

    d_attn, _ = group_gather(norm_grad(attn_out, weight_two, grad_hidden).astype(bf16))
    grad_outproj = ctx_scatter(dot(d_attn, head_o, 0, 0))
    grad_o = dot(d_attn, col_out).astype(bf16)
    products = grad_o.astype(f32) * head_o.astype(f32)
    dsum = jnp.concatenate(
        [
            jnp.broadcast_to(
                jnp.sum(products[:, s : s + HEAD_DIM], axis=1, keepdims=True), (group_rows, 128)
            )
            for s in range(0, q_cols, HEAD_DIM)
        ],
        axis=1,
    )
    grad_q, grad_kv = attend_back(
        queries, grad_o, lse, dsum, kv, own_spans, ring_spans, boundary, span
    )
    grad_kv = ring_scatter(
        [grad_kv[k * group_rows : (k + 1) * group_rows] for k in range(contexts)], ctx_ring
    )
    grad_q = (rotary(grad_q, cosines, sines, -1.0) * q_scale).astype(bf16)
    grad_k = rotary(grad_kv[:, :k_cols], cosines, sines, -1.0).astype(bf16)
    grad_v = grad_kv[:, k_cols:].astype(bf16)
    grad_qkv = jnp.concatenate([grad_q, grad_k, grad_v], axis=1)
    d_in = group_scatter(dot(grad_qkv, col_qkv, 1, 1))
    grad_tokens = grad_hidden + norm_grad(tok_own, weight_one, d_in)
    mixed_grad = ctx_scatter(dot(normed_in, grad_qkv, 0, 0)).astype(bf16)
    grad_gate = slice_scatter(dot(normed_mid, d_gate, 0, 0), mixed_grad)
    grad_up = slice_scatter(dot(normed_mid, d_upper, 0, 0), mixed_grad)
    mixed_grad = lax.all_to_all(
        mixed_grad.reshape(ulysses, -1, mixed_grad.shape[1]),
        "uly",
        split_axis=0,
        concat_axis=0,
        tiled=True,
    )
    mixed_grad = jnp.transpose(mixed_grad, (1, 0, 2)).astype(f32)
    grad_query = mixed_grad[:, :, :q_cols].reshape(w_query.shape)
    grad_key = mixed_grad[:, :, q_cols : q_cols + k_cols].reshape(w_key.shape)
    grad_value = mixed_grad[:, :, q_cols + k_cols :].reshape(w_value.shape)

    gain_grads = sum_gains(
        jnp.stack(
            [
                gain_part(attn_out, grad_hidden),
                gain_part(hidden_in, d_mid),
                gain_part(ffn_out, cot_own),
            ]
        )
    )
    products = [
        jnp.sum(w.astype(f32) * g, axis=1)
        for w, g in ((w_query, grad_query), (w_key, grad_key), (w_value, grad_value))
    ]
    gain_first = (products[0] + products[1] + products[2]) / (1.0 + gain_attn_in.astype(f32))
    return (
        block_out,
        grad_tokens,
        grad_query,
        grad_key,
        grad_value,
        grad_outproj,
        grad_gate,
        grad_up,
        grad_down,
        gain_first,
        gain_grads[0],
        gain_grads[1],
        gain_grads[2],
    )


def solution(mesh):
    flat, cut, line = P(AXES, None), P("ctx", "uly"), P(AXES)
    in_specs = (flat, flat, P(), P(), flat, flat, flat, cut, cut, cut, cut, line, line, line, line)
    out_specs = (flat, flat, flat, flat, flat, cut, cut, cut, cut, line, line, line, line)
    return jax.shard_map(
        functools.partial(on_device, Plan(mesh)),
        mesh=mesh,
        in_specs=in_specs,
        out_specs=out_specs,
        check_vma=False,
    )
```

```python
import functools

import jax
import jax.numpy as jnp
from jax import lax
from jax.experimental import pallas as pl
from jax.experimental.pallas import tpu as pltpu
from jax.sharding import PartitionSpec as P

HEAD_DIM = 256
AXES = ("ctx", "uly")

norm_eps = 1e-06
soft_cap = 50.0
rotary_base = 10000.0
gelu_coef = 0.7978845608028654
cubic_coef = 0.044715


bf16 = jnp.bfloat16
f32 = jnp.float32


def rms_scale(values):
    return lax.rsqrt(jnp.mean(values * values, axis=-1, keepdims=True) + norm_eps)


def norm_apply(values, weight):
    return values * rms_scale(values) * weight


def norm_grad(values, weight, grad):
    scale = rms_scale(values)
    inner = jnp.mean(grad * weight * values, axis=-1, keepdims=True)
    return scale * weight * grad - values * (scale * scale * scale) * inner


def gain_part(values, grad):
    return jnp.sum(grad * values * rms_scale(values), axis=0)


def gelu_parts(values):
    inner = gelu_coef * (values + cubic_coef * values * values * values)
    tanh_part = jnp.tanh(inner)
    value = 0.5 * values * (1.0 + tanh_part)
    slope = 0.5 * (1.0 + tanh_part) + 0.5 * values * (1.0 - tanh_part * tanh_part) * gelu_coef * (
        1.0 + 3.0 * cubic_coef * values * values
    )
    return value, slope


def rotary(values, cosines, sines, sign):
    half = HEAD_DIM // 2
    parts = []
    for start in range(0, values.shape[1], HEAD_DIM):
        first = values[:, start : start + half]
        second = values[:, start + half : start + HEAD_DIM]
        parts.append(first * cosines - sign * second * sines)
        parts.append(second * cosines + sign * first * sines)
    return jnp.concatenate(parts, axis=1)


def dot(left, right, left_dim=1, right_dim=0):
    return lax.dot_general(
        left, right, (((left_dim,), (right_dim,)), ((), ())), preferred_element_type=f32
    )


class Plan:
    def __init__(self, mesh):
        grid = mesh.devices
        self.contexts, self.ulysses = mesh.shape["ctx"], mesh.shape["uly"]
        self.cores = sum(tuple(d.coords) == tuple(grid[0, 0].coords) for d in grid[0])
        self.layers = len({d.coords[2] for d in grid[:, 0]})
        self.sides = self.contexts // self.layers
        self.rows = self.ulysses // self.cores
        self.halves = self.layers // self.cores

    def split(self, device):
        ctx, uly = divmod(device, self.ulysses)
        return (*divmod(ctx, self.sides), *divmod(uly, self.cores))

    def join(self, layer, side, row, core):
        return (layer * self.sides + side) * self.ulysses + row * self.cores + core

    def perm(self, target):
        count = self.contexts * self.ulysses
        return [(d, self.join(*target(*self.split(d)))) for d in range(count)]

    def here(self):
        layer, side = jnp.divmod(lax.axis_index("ctx"), self.sides)
        row, core = jnp.divmod(lax.axis_index("uly"), self.cores)
        return layer, side, row, core


class Ring:
    def __init__(self, plan, outer, inner, place, locate):
        self.size = outer * inner
        self.inner = inner

        def cell(index):
            out, rest = divmod(index % self.size, inner)
            return out, (rest if out % 2 == 0 else inner - 1 - rest)

        def index_of(out, inn):
            return out * inner + (inn if out % 2 == 0 else inner - 1 - inn)

        self.cells = [cell(i) for i in range(self.size)]

        def shifted(step):
            def target(*where):
                return place(where, *cell(index_of(*locate(where)) + step))

            return plan.perm(target)

        self.ahead, self.behind = shifted(1), shifted(-1)

    def position(self, out, inn):
        rest = jnp.where(out % 2 == 0, inn, self.inner - 1 - inn)
        return out * self.inner + rest


def move(values, perm):
    return lax.ppermute(values, AXES, perm)


def both(*values):
    return lax.optimization_barrier(values)


def after(values, *earlier):
    return lax.optimization_barrier((values, *earlier))[0]


def ring_gather(block, ring):
    size = ring.size
    found = {0: block}
    if size == 2:
        found[1] = move(block, ring.ahead)
        return [found[0], found[1]]
    forth = back = block
    middle = size // 2
    for step in range(1, middle):
        forth, back = both(move(forth, ring.ahead), move(back, ring.behind))
        found[size - step], found[step] = forth, back
    cut = block.shape[0] // 2
    forth = move(forth[:cut], ring.ahead)
    back = move(back[cut:], ring.behind)
    found[middle] = jnp.concatenate([forth, back], axis=0)
    return [found[k] for k in range(size)]


def ring_scatter(parts, ring, kind=bf16):
    size = ring.size
    if size == 2:
        return parts[0].astype(f32) + move(parts[1].astype(kind), ring.ahead).astype(f32)
    middle = size // 2
    cut = parts[0].shape[0] // 2
    forth = move(parts[middle][:cut].astype(kind), ring.ahead)
    back = move(parts[middle][cut:].astype(kind), ring.behind)
    forth, back = both(forth, back)
    for left in range(middle - 1, 0, -1):
        fore, aft = parts[left].astype(f32), parts[size - left].astype(f32)
        if left == middle - 1:
            fore = jnp.concatenate([fore[:cut] + forth.astype(f32), fore[cut:]], axis=0)
            aft = jnp.concatenate([aft[:cut], aft[cut:] + back.astype(f32)], axis=0)
        else:
            fore, aft = fore + forth.astype(f32), aft + back.astype(f32)
        forth = move(fore.astype(kind), ring.ahead)
        back = move(aft.astype(kind), ring.behind)
        forth, back = both(forth, back)
    return parts[0].astype(f32) + forth.astype(f32) + back.astype(f32)


def place_rows(blocks, indices, count):
    first = blocks[0]
    out = jnp.zeros((count, *first.shape), first.dtype)
    for block, index in zip(blocks, indices, strict=True):
        out = lax.dynamic_update_slice(out, block[None], (index, *(0,) * first.ndim))
    return out


def take_block(values, index, size):
    return lax.dynamic_slice_in_dim(values, index * size, size, 0)


def weights_kernel(plan, counts, *refs):
    sources, rest = refs[: counts[0]], refs[counts[0] :]
    results, rest = rest[: counts[1]], rest[counts[1] :]
    tok_in, wq, wk, wv, out_in, gain_in, *mats = sources
    tok_all, qkv, out_all, gain_all, *slices = results
    tok_tmp, qkv_tmp, out_tmp, gain_tmp, local, send, recv = rest
    layers, sides, cores, halves = plan.layers, plan.sides, plan.cores, plan.halves
    ulysses, contexts = plan.ulysses, plan.contexts
    ctx, uly = lax.axis_index("ctx"), lax.axis_index("uly")
    layer, side, row, core = ctx // sides, ctx % sides, uly // cores, uly % cores

    def at(a_layer, a_side, a_row, a_core):
        return {"ctx": a_layer * sides + a_side, "uly": a_row * cores + a_core}

    friends = []
    for dl in range(layers):
        for dc in range(cores):
            if (dl, dc) != (0, 0):
                friends.append(at((layer + dl) % layers, side, row, (core + dc) % cores))
    for ds in sorted({1 % sides, sides - 1} - {0}):
        friends.append(at(layer, (side + ds) % sides, row, core))
    for dr in range(1, plan.rows):
        for dc in range(cores):
            friends.append(at(layer, side, (row + dr) % plan.rows, (core + dc) % cores))
    barrier = pltpu.get_barrier_semaphore()
    for friend in friends:
        pl.semaphore_signal(
            barrier, inc=1, device_id=friend, device_id_type=pl.DeviceIdType.MESH
        )
    pl.semaphore_wait(barrier, len(friends))

    used = [0]
    sent = []

    def push(source, target, device):
        k = used[0]
        used[0] += 1
        copy = pltpu.make_async_remote_copy(
            source,
            target,
            send.at[k],
            recv.at[k],
            device_id=device,
            device_id_type=pl.DeviceIdType.MESH,
        )
        copy.start()
        sent.append(copy)
        return copy

    q_cols, k_cols = wq.shape[1] // ulysses, wk.shape[1] // ulysses

    def parts(u):
        yield wq.at[:, pl.ds(pl.multiple_of(u * q_cols, 128), q_cols)], pl.ds(0, q_cols)
        yield wk.at[:, pl.ds(pl.multiple_of(u * k_cols, 128), k_cols)], pl.ds(q_cols, k_cols)
        yield wv.at[:, pl.ds(pl.multiple_of(u * k_cols, 128), k_cols)], pl.ds(q_cols + k_cols, k_cols)

    pulls = [pltpu.make_async_copy(src, qkv_tmp.at[:, cols], local.at[k]) for k, (src, cols) in enumerate(parts(uly))]
    pulls.append(pltpu.make_async_copy(gain_in, gain_tmp, local.at[3]))
    pulls.append(pltpu.make_async_copy(out_in, out_tmp, local.at[4]))
    pulls.append(pltpu.make_async_copy(tok_in, tok_tmp, local.at[5]))
    for pull in pulls:
        pull.start()
    place = ctx * ulysses + uly
    group = []
    for dr in range(plan.rows - 1, -1, -1):
        for dc in range(cores):
            if (dr, dc) == (0, 0):
                continue
            there_row, there_core = (row + dr) % plan.rows, (core + dc) % cores
            friend, u = at(layer, side, there_row, there_core), there_row * cores + there_core
            for source, cols in parts(u):
                group.append(push(source, qkv.at[place, :, cols], friend))
            group.append(push(gain_in, gain_all.at[place], friend))
    for pull in pulls:
        pull.wait()
    puts = [
        pltpu.make_async_copy(qkv_tmp, qkv.at[place], local.at[6]),
        pltpu.make_async_copy(gain_tmp, gain_all.at[place], local.at[7]),
        pltpu.make_async_copy(out_tmp, out_all.at[ctx], local.at[8]),
        pltpu.make_async_copy(tok_tmp, tok_all.at[uly], local.at[9]),
    ]
    for put in puts:
        put.start()
    for put in puts:
        put.wait()
    for copy in group:
        copy.wait_recv()

    def spot(index):
        out, low = index // layers, index % layers
        flip = out % 2
        return (low * (1 - flip) + (layers - 1 - low) * flip) * sides + out

    flip = side % 2
    here = side * layers + layer * (1 - flip) + (layers - 1 - layer) * flip
    ahead = {"ctx": spot((here + 1) % contexts), "uly": uly}
    behind = {"ctx": spot((here + contexts - 1) % contexts), "uly": uly}

    def ring_steps(piece, cut):
        middle = contexts // 2
        last = ()
        for step in range(middle):
            for copy in last:
                copy.wait_recv()
            fore, aft = spot((here + contexts - step) % contexts), spot((here + step) % contexts)
            if step < middle - 1:
                last = (
                    push(piece(fore), piece(fore), ahead),
                    push(piece(aft), piece(aft), behind),
                )
            else:
                last = (
                    push(piece(fore).at[:cut], piece(fore).at[:cut], ahead),
                    push(piece(aft).at[cut:], piece(aft).at[cut:], behind),
                )
            yield
        for copy in last:
            copy.wait_recv()

    slice_cols = mats[0].shape[1] // halves if mats else 0

    def slice_sends(m, p):
        h = (layer + p) % halves
        target = at(core * halves + h, side, row, cores - 1 - layer // halves)
        cols = pl.ds(pl.multiple_of(h * slice_cols, 128), slice_cols)
        return push(mats[m].at[:, cols], slices[m].at[ctx], target)

    def origin(p):
        return (cores - 1 - core) * halves + (layer - p + halves) % halves

    def slice_moves(m, p, arrived):
        held = arrived
        passed = []
        for step in range(sides):
            held.wait_recv()
            slot = slices[m].at[origin(p) * sides + (side - step + sides) % sides]
            for dc in range(1, cores):
                passed.append(push(slot, slot, at(layer, side, row, (core + dc) % cores)))
            if step < sides - 1:
                held = push(slot, slot, at(layer, (side + 1) % sides, row, core))
            yield
        for copy in passed:
            copy.wait_recv()

    rings = [
        ring_steps(lambda c: qkv.at[pl.ds(c * ulysses, ulysses)], ulysses // 2),
        ring_steps(lambda c: gain_all.at[pl.ds(c * ulysses, ulysses)], ulysses // 2),
        ring_steps(lambda c: out_all.at[c], out_all.shape[1] // 16 * 8),
    ]
    tasks = [(m, p) for m in range(len(mats)) for p in range(halves)]
    arrived, moving = [], []

    def drive(generators):
        return [g for g in generators if next(g, "end") != "end"]

    active_rings = drive(rings[:2])
    toks = []
    for dr in range(plan.rows - 1, -1, -1):
        for dc in range(cores):
            if (dr, dc) != (0, 0):
                toks.append(push(tok_in, tok_all.at[uly], at(layer, side, (row + dr) % plan.rows, (core + dc) % cores)))
    waiting = list(tasks)
    pending = []
    extra = [rings[2]]
    while active_rings or waiting or pending or moving or extra:
        if waiting:
            task = waiting.pop(0)
            pending.append((*task, slice_sends(*task)))
        active_rings = drive(active_rings)
        if not active_rings and extra:
            active_rings = drive([extra.pop(0)])
        if pending and (len(pending) > 1 or not waiting):
            moving.append(slice_moves(*pending.pop(0)))
        moving = drive(moving)
    for copy in toks:
        copy.wait_recv()
    for copy in sent:
        copy.wait_send()


def fetch_weights(plan, tokens, wq, wk, wv, w_out, gains, mats):
    shard, contexts, ulysses = wq.shape[0], plan.contexts, plan.ulysses
    cols = (wq.shape[1] + wk.shape[1] + wv.shape[1]) // ulysses
    results = [
        jax.ShapeDtypeStruct((ulysses, *tokens.shape), tokens.dtype),
        jax.ShapeDtypeStruct((contexts * ulysses, shard, cols), wq.dtype),
        jax.ShapeDtypeStruct((contexts, *w_out.shape), w_out.dtype),
        jax.ShapeDtypeStruct((contexts * ulysses, *gains.shape), gains.dtype),
    ] + [
        jax.ShapeDtypeStruct((contexts, w.shape[0], w.shape[1] // plan.halves), w.dtype)
        for w in mats
    ]
    copies = 5 * (ulysses - 1) + 3 * contexts + len(mats) * plan.halves * plan.sides * (1 + plan.cores)
    anywhere = pl.BlockSpec(memory_space=pl.ANY)
    inputs = (tokens, wq, wk, wv, w_out, gains, *mats)
    return pl.pallas_call(
        functools.partial(weights_kernel, plan, (len(inputs), len(results))),
        out_shape=results,
        in_specs=[anywhere] * len(inputs),
        out_specs=[anywhere] * len(results),
        scratch_shapes=[
            pltpu.VMEM(tokens.shape, tokens.dtype),
            pltpu.VMEM((shard, cols), wq.dtype),
            pltpu.VMEM(w_out.shape, w_out.dtype),
            pltpu.VMEM(gains.shape, gains.dtype),
            pltpu.SemaphoreType.DMA((10,)),
            pltpu.SemaphoreType.DMA((copies,)),
            pltpu.SemaphoreType.DMA((copies,)),
        ],
        compiler_params=pltpu.CompilerParams(collective_id=1, has_side_effects=True),
    )(*inputs)


def visible(q_first, k_first, boundary, span):
    q_pos = q_first + lax.broadcasted_iota(jnp.int32, (span, span), 0)
    k_pos = k_first + lax.broadcasted_iota(jnp.int32, (span, span), 1)
    low = jnp.where(q_pos >= boundary, boundary, 0)
    return (k_pos <= q_pos) & (k_pos >= low)


def active(q_first, k_first, boundary, span):
    split = (q_first >= boundary) & (k_first + span <= boundary)
    return (k_first <= q_first) & jnp.logical_not(split)


def attend_kernel(span, repeat, count, qp, kp, bd, q_ref, kv_ref, o_ref, lse_ref, acc, den):
    i, j = pl.program_id(0), pl.program_id(1)

    @pl.when(j == 0)
    def _():
        acc[...] = jnp.zeros_like(acc)
        den[...] = jnp.zeros_like(den)

    q_first, k_first, boundary = qp[i], kp[j], bd[0]

    @pl.when(active(q_first, k_first, boundary, span))
    def _():
        allowed = visible(q_first, k_first, boundary, span)
        keys, values = kv_ref[:, :HEAD_DIM], kv_ref[:, HEAD_DIM:]
        for r in range(repeat):
            cols = slice(r * HEAD_DIM, (r + 1) * HEAD_DIM)
            scores = dot(q_ref[:, cols], keys, 1, 1)
            weights = jnp.where(
                allowed, jnp.exp(soft_cap * jnp.tanh(scores * (1.0 / soft_cap))), 0.0
            )
            den[r] += jnp.sum(weights, axis=1, keepdims=True)
            acc[:, cols] += dot(weights.astype(bf16), values)

    @pl.when(j == count - 1)
    def _():
        for r in range(repeat):
            cols = slice(r * HEAD_DIM, (r + 1) * HEAD_DIM)
            total = den[r][:, :1]
            o_ref[:, cols] = (acc[:, cols] / total).astype(bf16)
            lse_ref[:, r * 128 : (r + 1) * 128] = jnp.broadcast_to(jnp.log(total), (span, 128))


def attend(q, kv, q_pos, k_pos, boundary, span):
    rows, width = q.shape
    repeat = width // HEAD_DIM
    count = kv.shape[0] // span
    spec = pltpu.PrefetchScalarGridSpec(
        num_scalar_prefetch=3,
        grid=(rows // span, count),
        in_specs=[
            pl.BlockSpec((span, width), lambda i, j, *_: (i, 0)),
            pl.BlockSpec((span, kv.shape[1]), lambda i, j, *_: (j, 0)),
        ],
        out_specs=[
            pl.BlockSpec((span, width), lambda i, j, *_: (i, 0)),
            pl.BlockSpec((span, 128 * repeat), lambda i, j, *_: (i, 0)),
        ],
        scratch_shapes=[
            pltpu.VMEM((span, width), f32),
            pltpu.VMEM((repeat, span, 128), f32),
        ],
    )
    flops = 2 * rows * kv.shape[0] * width
    return pl.pallas_call(
        functools.partial(attend_kernel, span, repeat, count),
        out_shape=[
            jax.ShapeDtypeStruct((rows, width), bf16),
            jax.ShapeDtypeStruct((rows, 128 * repeat), f32),
        ],
        grid_spec=spec,
        compiler_params=pltpu.CompilerParams(dimension_semantics=("arbitrary", "arbitrary")),
        cost_estimate=pl.CostEstimate(
            flops=flops, bytes_accessed=2 * kv.size * 2, transcendentals=rows * kv.shape[0] * repeat
        ),
    )(q_pos, k_pos, boundary, q, kv)


def attend_back_kernel(
    span, repeat, count, blocks, qp, kp, bd, q_ref, g_ref, lse_ref, ds_ref, kv_ref, dq_ref, dkv_ref, acc, dk, dv
):
    j, i = pl.program_id(0), pl.program_id(1)

    @pl.when((j == 0) & (i == 0))
    def _():
        acc[...] = jnp.zeros_like(acc)

    @pl.when(i == 0)
    def _():
        dk[...] = jnp.zeros_like(dk)
        dv[...] = jnp.zeros_like(dv)

    q_first, k_first, boundary = qp[i], kp[j], bd[0]

    @pl.when(active(q_first, k_first, boundary, span))
    def _():
        allowed = visible(q_first, k_first, boundary, span)
        keys, values = kv_ref[:, :HEAD_DIM], kv_ref[:, HEAD_DIM:]
        rows = pl.ds(pl.multiple_of(i * span, span), span)
        for r in range(repeat):
            cols = slice(r * HEAD_DIM, (r + 1) * HEAD_DIM)
            query, grad = q_ref[rows, cols], g_ref[rows, cols]
            lse = lse_ref[rows, r * 128 : r * 128 + 1]
            dsum = ds_ref[rows, r * 128 : r * 128 + 1]
            bent = jnp.tanh(dot(query, keys, 1, 1) * (1.0 / soft_cap))
            probs = jnp.where(allowed, jnp.exp(soft_cap * bent - lse), 0.0)
            dprob = dot(grad, values, 1, 1)
            dscore = (probs * (dprob - dsum) * (1.0 - bent * bent)).astype(bf16)
            acc[rows, cols] += dot(dscore, keys)
            dk[...] += dot(dscore, query, 0, 0)
            dv[...] += dot(probs.astype(bf16), grad, 0, 0)

    @pl.when(i == blocks - 1)
    def _():
        dkv_ref[:, :HEAD_DIM] = dk[...].astype(dkv_ref.dtype)
        dkv_ref[:, HEAD_DIM:] = dv[...].astype(dkv_ref.dtype)

    @pl.when((j == count - 1) & (i == blocks - 1))
    def _():
        dq_ref[...] = acc[...]


def attend_back(q, grad, lse, dsum, kv, q_pos, k_pos, boundary, span):
    rows, width = q.shape
    repeat = width // HEAD_DIM
    count, blocks = kv.shape[0] // span, rows // span
    whole = lambda w: pl.BlockSpec((rows, w), lambda j, i, *_: (0, 0))
    spec = pltpu.PrefetchScalarGridSpec(
        num_scalar_prefetch=3,
        grid=(count, blocks),
        in_specs=[
            whole(width),
            whole(width),
            whole(128 * repeat),
            whole(128 * repeat),
            pl.BlockSpec((span, kv.shape[1]), lambda j, i, *_: (j, 0)),
        ],
        out_specs=[
            whole(width),
            pl.BlockSpec((span, kv.shape[1]), lambda j, i, *_: (j, 0)),
        ],
        scratch_shapes=[
            pltpu.VMEM((rows, width), f32),
            pltpu.VMEM((span, HEAD_DIM), f32),
            pltpu.VMEM((span, HEAD_DIM), f32),
        ],
    )
    return pl.pallas_call(
        functools.partial(attend_back_kernel, span, repeat, count, blocks),
        out_shape=[
            jax.ShapeDtypeStruct((rows, width), f32),
            jax.ShapeDtypeStruct(kv.shape, bf16),
        ],
        grid_spec=spec,
        compiler_params=pltpu.CompilerParams(dimension_semantics=("arbitrary", "arbitrary")),
        cost_estimate=pl.CostEstimate(
            flops=5 * rows * kv.shape[0] * width,
            bytes_accessed=2 * kv.size * 2,
            transcendentals=rows * kv.shape[0] * repeat,
        ),
    )(q_pos, k_pos, boundary, q, grad, lse, dsum, kv)


def on_device(
    plan,
    tokens,
    cotangent,
    span_order,
    segments,
    w_query,
    w_key,
    w_value,
    w_out,
    w_gate,
    w_up,
    w_down,
    gain_attn_in,
    gain_attn_out,
    gain_ffn_in,
    gain_ffn_out,
):
    rows, width = tokens.shape
    contexts, ulysses = plan.contexts, plan.ulysses
    layers, sides, cores, halves = plan.layers, plan.sides, plan.cores, plan.halves
    group_rows = rows * ulysses
    span = group_rows // 2
    q_scale = float(HEAD_DIM) ** (-0.5)
    uly, ctx = lax.axis_index("uly"), lax.axis_index("ctx")
    layer, side, row, core = plan.here()

    ctx_ring = Ring(
        plan, sides, layers, lambda w, out, inn: (inn, out, w[2], w[3]), lambda w: (w[1], w[0])
    )
    ffn_ring = Ring(
        plan, plan.rows, layers, lambda w, out, inn: (inn, w[1], out, w[3]), lambda w: (w[2], w[0])
    )
    side_ring = Ring(
        plan, 1, sides, lambda w, out, inn: (w[0], inn, w[2], w[3]), lambda w: (0, w[1])
    )
    row_ring = Ring(
        plan, 1, plan.rows, lambda w, out, inn: (w[0], w[1], inn, w[3]), lambda w: (0, w[2])
    )
    core_ring = Ring(
        plan, 1, cores, lambda w, out, inn: (w[0], w[1], w[2], inn), lambda w: (0, w[3])
    )
    ctx_cells = jnp.array([inn * sides + out for out, inn in ctx_ring.cells], jnp.int32)
    ctx_place = ctx_ring.position(side, layer)
    ring_ctx = [ctx_cells[(ctx_place + k) % contexts] for k in range(contexts)]

    def group_gather(values):
        mine = ring_gather(values, row_ring)
        blocks, where = [], []
        for k, block in enumerate(mine):
            for m, found in enumerate(ring_gather(block, core_ring)):
                blocks.append(found)
                where.append((row + k) % plan.rows * cores + (core + m) % cores)
        return place_rows(blocks, where, ulysses).reshape(group_rows, values.shape[1]), mine[-1]

    def group_scatter(values):
        parts = values.reshape(plan.rows, cores, rows, values.shape[1])

        def part(k, m):
            at = ((row + k) % plan.rows, (core + m) % cores, 0, 0)
            return lax.dynamic_slice(parts, at, (1, 1, *parts.shape[2:]))[0, 0]

        summed = [
            ring_scatter([part(k, m) for m in range(cores)], core_ring) for k in range(plan.rows)
        ]
        return ring_scatter(summed, row_ring)

    def ctx_scatter(values):
        size = values.shape[0] // contexts
        return ring_scatter([take_block(values, ring_ctx[k], size) for k in range(contexts)], ctx_ring)

    shard = gain_attn_in.shape[0]
    places = (ctx_place, row, core)
    tiny_rings = (ctx_ring, row_ring, core_ring)
    ring_order = [inn * sides + out for out, inn in ctx_ring.cells]

    def turn(values, axis, back):
        count, place = values.shape[axis], places[axis]
        start = place if back else (count - place) % count
        twice = jnp.concatenate([values, values], axis=axis)
        return lax.dynamic_slice_in_dim(twice, start, count, axis)

    def sum_gains(parts):
        count = parts.shape[0]
        found = jnp.transpose(parts.reshape(count, contexts * ulysses, shard), (1, 0, 2))
        found = jnp.pad(found, ((0, 0), (0, -count % 8), (0, -shard % 128)))
        found = found.reshape(contexts, plan.rows, cores, *found.shape[1:])
        found = jnp.stack([found[c] for c in ring_order])
        for axis in range(3):
            found = turn(found, axis, True)
        for axis in (2, 1, 0):
            entries = [lax.index_in_dim(found, k, axis, False) for k in range(found.shape[axis])]
            found = ring_scatter(entries, tiny_rings[axis], f32)
        return found[:count, :shard]

    packed = jnp.stack([gain_attn_in, gain_attn_out, gain_ffn_in, gain_ffn_out])
    packed = jnp.pad(packed, ((0, 4), (0, -shard % 128)))
    fetched = fetch_weights(
        plan, tokens, w_query, w_key, w_value, w_out, packed.astype(f32), (w_gate, w_up, w_down)
    )
    tok_group, col_qkv, col_out, gains, ffn_gate, ffn_up, ffn_down = fetched
    tok_group = tok_group.reshape(group_rows, width)
    col_qkv = col_qkv.reshape(width, -1)
    col_out = col_out.reshape(width, -1)
    ffn_gate, ffn_up, ffn_down = (w.reshape(width, -1) for w in (ffn_gate, ffn_up, ffn_down))
    gains = jnp.transpose(gains[:, :4, :shard], (1, 0, 2)).reshape(4, width)
    weight_one, weight_two, weight_three, weight_four = (1.0 + gains[k][None] for k in range(4))

    own_spans = lax.dynamic_slice_in_dim(span_order, 2 * ctx, 2, 0) * span
    boundary = jnp.sum((segments == 0).astype(jnp.int32)).reshape(1)
    ring_spans = jnp.concatenate(
        [lax.dynamic_slice_in_dim(span_order, 2 * c, 2, 0) for c in ring_ctx]
    ) * span
    group_pos = (own_spans[:, None] + jnp.arange(span, dtype=jnp.int32)[None, :]).reshape(-1)
    half = HEAD_DIM // 2
    freqs = rotary_base ** (-jnp.arange(half).astype(f32) / half)
    angles = group_pos.astype(f32)[:, None] * freqs[None, :]
    cosines, sines = jnp.cos(angles), jnp.sin(angles)

    q_cols, k_cols = w_query.shape[1] // ulysses, w_key.shape[1] // ulysses
    tok_rows = tok_group.astype(f32)
    normed_in = norm_apply(tok_rows, weight_one).astype(bf16)
    qkv = dot(normed_in, col_qkv)
    queries = (rotary(qkv[:, :q_cols], cosines, sines, 1.0) * q_scale).astype(bf16)
    keys = rotary(qkv[:, q_cols : q_cols + k_cols], cosines, sines, 1.0).astype(bf16)
    values = qkv[:, q_cols + k_cols :].astype(bf16)
    kv_blocks = ring_gather(jnp.concatenate([keys, values], axis=1), ctx_ring)
    kv = jnp.concatenate(kv_blocks, axis=0)

    slice_cols = w_gate.shape[1] // halves

    def slice_perm(p):
        return plan.perm(lambda l, s, r, c: (c * halves + (l + p) % halves, s, r, l // halves))

    def slice_back(p):
        return [(b, a) for a, b in slice_perm(p)]

    def pick(options, index):
        out = options[0]
        for k in range(1, len(options)):
            out = jnp.where(index == k, options[k], out)
        return out

    def slice_scatter(grad, second):
        parts = grad.reshape(cores, halves, sides, -1, slice_cols)
        size = parts.shape[3]

        def part(m):
            at = ((core + m) % cores, 0, 0, 0, 0)
            return lax.dynamic_slice(parts, at, (1, *parts.shape[1:]))[0]

        summed = ring_scatter([part(m) for m in range(cores)], core_ring)

        def side_part(k):
            at = (0, (side + k) % sides, 0, 0)
            found = lax.dynamic_slice(summed, at, (halves, 1, size, slice_cols))
            return found.reshape(halves * size, slice_cols)

        summed = ring_scatter([side_part(k) for k in range(sides)], side_ring).astype(bf16)
        summed = after(summed.reshape(halves, size, slice_cols), second)
        got = []
        for p in range(halves):
            piece = lax.dynamic_index_in_dim(summed, (layer - p) % halves, 0, keepdims=False)
            got.append(move(piece, slice_back(p)))
        cuts = [pick(got, (h - layer) % halves) for h in range(halves)]
        return jnp.concatenate(cuts, axis=1).astype(f32)

    head_o, lse = attend(queries, kv, own_spans, ring_spans, boundary, span)
    attn_out = group_scatter(dot(head_o, col_out, 1, 1))
    tok_own = tokens.astype(f32)
    hidden_in = tok_own + norm_apply(attn_out, weight_two)
    normed_own = norm_apply(hidden_in, weight_three).astype(bf16)

    size = ffn_ring.size
    order = [0]
    for k in range(1, size // 2):
        order += [k, size - k]
    order.append(size // 2)

    def ffn_gather(values):
        found = ring_gather(values, ffn_ring)
        return jnp.concatenate([found[k] for k in order], axis=0)

    def ffn_scatter(values):
        parts = [None] * size
        for n, k in enumerate(order):
            parts[k] = values[n * rows : (n + 1) * rows]
        return ring_scatter(parts, ffn_ring)

    normed_mid = ffn_gather(normed_own)
    gate = dot(normed_mid, ffn_gate)
    upper = dot(normed_mid, ffn_up)
    gate_value, gate_slope = gelu_parts(gate)
    hidden = (gate_value * upper).astype(bf16)
    ffn_out = ffn_scatter(dot(hidden, ffn_down, 1, 1))
    block_out = (hidden_in + norm_apply(ffn_out, weight_four)).astype(bf16)
    cot_own = cotangent.astype(f32)
    d_ffn = ffn_gather(norm_grad(ffn_out, weight_four, cot_own).astype(bf16))
    d_hidden = dot(d_ffn, ffn_down)
    d_gate = (d_hidden * upper * gate_slope).astype(bf16)
    d_upper = (d_hidden * gate_value).astype(bf16)
    d_mid = ffn_scatter(dot(d_gate, ffn_gate, 1, 1) + dot(d_upper, ffn_up, 1, 1))
    grad_hidden = cot_own + norm_grad(hidden_in, weight_three, d_mid)
    grad_down = slice_scatter(dot(d_ffn, hidden, 0, 0), d_mid)

    d_attn, _ = group_gather(norm_grad(attn_out, weight_two, grad_hidden).astype(bf16))
    grad_outproj = ctx_scatter(dot(d_attn, head_o, 0, 0))
    grad_o = dot(d_attn, col_out).astype(bf16)
    products = grad_o.astype(f32) * head_o.astype(f32)
    dsum = jnp.concatenate(
        [
            jnp.broadcast_to(
                jnp.sum(products[:, s : s + HEAD_DIM], axis=1, keepdims=True), (group_rows, 128)
            )
            for s in range(0, q_cols, HEAD_DIM)
        ],
        axis=1,
    )
    grad_q, grad_kv = attend_back(
        queries, grad_o, lse, dsum, kv, own_spans, ring_spans, boundary, span
    )
    grad_kv = ring_scatter(
        [grad_kv[k * group_rows : (k + 1) * group_rows] for k in range(contexts)], ctx_ring
    )
    grad_q = (rotary(grad_q, cosines, sines, -1.0) * q_scale).astype(bf16)
    grad_k = rotary(grad_kv[:, :k_cols], cosines, sines, -1.0).astype(bf16)
    grad_v = grad_kv[:, k_cols:].astype(bf16)
    grad_qkv = jnp.concatenate([grad_q, grad_k, grad_v], axis=1)
    d_in = group_scatter(dot(grad_qkv, col_qkv, 1, 1))
    grad_tokens = grad_hidden + norm_grad(tok_own, weight_one, d_in)
    mixed_grad = ctx_scatter(dot(normed_in, grad_qkv, 0, 0)).astype(bf16)
    grad_gate = slice_scatter(dot(normed_mid, d_gate, 0, 0), mixed_grad)
    grad_up = slice_scatter(dot(normed_mid, d_upper, 0, 0), mixed_grad)
    mixed_grad = lax.all_to_all(
        mixed_grad.reshape(ulysses, -1, mixed_grad.shape[1]),
        "uly",
        split_axis=0,
        concat_axis=0,
        tiled=True,
    )
    mixed_grad = jnp.transpose(mixed_grad, (1, 0, 2)).astype(f32)
    grad_query = mixed_grad[:, :, :q_cols].reshape(w_query.shape)
    grad_key = mixed_grad[:, :, q_cols : q_cols + k_cols].reshape(w_key.shape)
    grad_value = mixed_grad[:, :, q_cols + k_cols :].reshape(w_value.shape)

    gain_grads = sum_gains(
        jnp.stack(
            [
                gain_part(attn_out, grad_hidden),
                gain_part(hidden_in, d_mid),
                gain_part(ffn_out, cot_own),
            ]
        )
    )
    products = [
        jnp.sum(w.astype(f32) * g, axis=1)
        for w, g in ((w_query, grad_query), (w_key, grad_key), (w_value, grad_value))
    ]
    gain_first = (products[0] + products[1] + products[2]) / (1.0 + gain_attn_in.astype(f32))
    return (
        block_out,
        grad_tokens,
        grad_query,
        grad_key,
        grad_value,
        grad_outproj,
        grad_gate,
        grad_up,
        grad_down,
        gain_first,
        gain_grads[0],
        gain_grads[1],
        gain_grads[2],
    )


def solution(mesh):
    flat, cut, line = P(AXES, None), P("ctx", "uly"), P(AXES)
    in_specs = (flat, flat, P(), P(), flat, flat, flat, cut, cut, cut, cut, line, line, line, line)
    out_specs = (flat, flat, flat, flat, flat, cut, cut, cut, cut, line, line, line, line)
    return jax.shard_map(
        functools.partial(on_device, Plan(mesh)),
        mesh=mesh,
        in_specs=in_specs,
        out_specs=out_specs,
        check_vma=False,
    )
```

```python
import functools

import jax
import jax.numpy as jnp
from jax import lax
from jax.experimental import pallas as pl
from jax.experimental.pallas import tpu as pltpu
from jax.sharding import PartitionSpec as P


HEAD_DIM = 256
AXES = ("ctx", "uly")

norm_eps = 1e-06
soft_cap = 50.0
rotary_base = 10000.0
gelu_coef = 0.7978845608028654
cubic_coef = 0.044715


BURST, LAG = 1, 1

bf16 = jnp.bfloat16
f32 = jnp.float32


def rms_scale(values):
    return lax.rsqrt(jnp.mean(values * values, axis=-1, keepdims=True) + norm_eps)


def norm_apply(values, weight):
    return values * rms_scale(values) * weight


def norm_grad(values, weight, grad):
    scale = rms_scale(values)
    inner = jnp.mean(grad * weight * values, axis=-1, keepdims=True)
    return scale * weight * grad - values * (scale * scale * scale) * inner


def gain_part(values, grad):
    return jnp.sum(grad * values * rms_scale(values), axis=0)


def gelu_parts(values):
    inner = gelu_coef * (values + cubic_coef * values * values * values)
    tanh_part = jnp.tanh(inner)
    value = 0.5 * values * (1.0 + tanh_part)
    slope = 0.5 * (1.0 + tanh_part) + 0.5 * values * (1.0 - tanh_part * tanh_part) * gelu_coef * (
        1.0 + 3.0 * cubic_coef * values * values
    )
    return value, slope


def rotary(values, cosines, sines, sign):
    half = HEAD_DIM // 2
    parts = []
    for start in range(0, values.shape[1], HEAD_DIM):
        first = values[:, start : start + half]
        second = values[:, start + half : start + HEAD_DIM]
        parts.append(first * cosines - sign * second * sines)
        parts.append(second * cosines + sign * first * sines)
    return jnp.concatenate(parts, axis=1)


def dot(left, right, left_dim=1, right_dim=0):
    return lax.dot_general(
        left, right, (((left_dim,), (right_dim,)), ((), ())), preferred_element_type=f32
    )


class Plan:
    def __init__(self, mesh):
        grid = mesh.devices
        self.contexts, self.ulysses = mesh.shape["ctx"], mesh.shape["uly"]
        self.cores = sum(tuple(d.coords) == tuple(grid[0, 0].coords) for d in grid[0])
        self.layers = len({d.coords[2] for d in grid[:, 0]})
        self.sides = self.contexts // self.layers
        self.rows = self.ulysses // self.cores
        self.halves = self.layers // self.cores

    def split(self, device):
        ctx, uly = divmod(device, self.ulysses)
        return (*divmod(ctx, self.sides), *divmod(uly, self.cores))

    def join(self, layer, side, row, core):
        return (layer * self.sides + side) * self.ulysses + row * self.cores + core

    def perm(self, target):
        count = self.contexts * self.ulysses
        return [(d, self.join(*target(*self.split(d)))) for d in range(count)]

    def here(self):
        layer, side = jnp.divmod(lax.axis_index("ctx"), self.sides)
        row, core = jnp.divmod(lax.axis_index("uly"), self.cores)
        return layer, side, row, core


class Ring:
    def __init__(self, plan, outer, inner, place, locate):
        self.size = outer * inner
        self.inner = inner

        def cell(index):
            out, rest = divmod(index % self.size, inner)
            return out, (rest if out % 2 == 0 else inner - 1 - rest)

        def index_of(out, inn):
            return out * inner + (inn if out % 2 == 0 else inner - 1 - inn)

        self.cells = [cell(i) for i in range(self.size)]

        def shifted(step):
            def target(*where):
                return place(where, *cell(index_of(*locate(where)) + step))

            return plan.perm(target)

        self.ahead, self.behind = shifted(1), shifted(-1)

    def position(self, out, inn):
        rest = jnp.where(out % 2 == 0, inn, self.inner - 1 - inn)
        return out * self.inner + rest


def move(values, perm):
    return lax.ppermute(values, AXES, perm)


def both(*values):
    return lax.optimization_barrier(values)


def after(values, *earlier):
    return lax.optimization_barrier((values, *earlier))[0]


def ring_gather(block, ring):
    size = ring.size
    found = {0: block}
    if size == 2:
        found[1] = move(block, ring.ahead)
        return [found[0], found[1]]
    forth = back = block
    middle = size // 2
    for step in range(1, middle):
        forth = move(forth, ring.ahead)
        back = move(back, ring.behind)
        forth, back = both(forth, back)
        found[size - step], found[step] = forth, back
    cut = block.shape[0] // 2
    forth = move(forth[:cut], ring.ahead)
    back = move(back[cut:], ring.behind)
    found[middle] = jnp.concatenate([forth, back], axis=0)
    return [found[k] for k in range(size)]


def ring_scatter(parts, ring, kind=bf16, landed=None):
    size = ring.size
    if size == 2:
        return parts[0].astype(f32) + move(parts[1].astype(kind), ring.ahead).astype(f32)
    middle = size // 2
    cut = parts[0].shape[0] // 2
    forth = move(parts[middle][:cut].astype(kind), ring.ahead)
    back = move(parts[middle][cut:].astype(kind), ring.behind)
    forth, back = both(forth, back)
    landed = [] if landed is None else landed
    for left in range(middle - 1, 0, -1):
        landed.append(forth)
        fore, aft = parts[left].astype(f32), parts[size - left].astype(f32)
        if left == middle - 1:
            fore = jnp.concatenate([fore[:cut] + forth.astype(f32), fore[cut:]], axis=0)
            aft = jnp.concatenate([aft[:cut], aft[cut:] + back.astype(f32)], axis=0)
        else:
            fore, aft = fore + forth.astype(f32), aft + back.astype(f32)
        forth = move(fore.astype(kind), ring.ahead)
        back = move(aft.astype(kind), ring.behind)
        forth, back = both(forth, back)
    return parts[0].astype(f32) + forth.astype(f32) + back.astype(f32)


def place_rows(blocks, indices, count):
    first = blocks[0]
    out = jnp.zeros((count, *first.shape), first.dtype)
    for block, index in zip(blocks, indices, strict=True):
        out = lax.dynamic_update_slice(out, block[None], (index, *(0,) * first.ndim))
    return out


def take_block(values, index, size):
    return lax.dynamic_slice_in_dim(values, index * size, size, 0)


class Sender:
    def __init__(self, plan, send, recv):
        self.plan, self.send, self.recv, self.sent = plan, send, recv, []
        self.ctx, self.uly = lax.axis_index("ctx"), lax.axis_index("uly")
        self.layer, self.side = self.ctx // plan.sides, self.ctx % plan.sides
        self.row, self.core = self.uly // plan.cores, self.uly % plan.cores
        flip = self.side % 2
        self.here = self.side * plan.layers + (
            self.layer * (1 - flip) + (plan.layers - 1 - self.layer) * flip
        )

    def at(self, layer, side, row, core):
        plan = self.plan
        return {"ctx": layer * plan.sides + side, "uly": row * plan.cores + core}

    def group(self):
        plan = self.plan
        for dr in range(plan.rows - 1, -1, -1):
            for dc in range(plan.cores):
                if (dr, dc) != (0, 0):
                    row, core = (self.row + dr) % plan.rows, (self.core + dc) % plan.cores
                    yield self.at(self.layer, self.side, row, core), row * plan.cores + core

    def meet(self):
        plan = self.plan
        friends = [friend for friend, _ in self.group()]
        for dl in range(1, plan.layers):
            for dc in range(plan.cores):
                layer, core = (self.layer + dl) % plan.layers, (self.core + dc) % plan.cores
                friends.append(self.at(layer, self.side, self.row, core))
        for ds in sorted({1 % plan.sides, plan.sides - 1} - {0}):
            side = (self.side + ds) % plan.sides
            friends.append(self.at(self.layer, side, self.row, self.core))
        barrier = pltpu.get_barrier_semaphore()
        for friend in friends:
            pl.semaphore_signal(
                barrier, inc=1, device_id=friend, device_id_type=pl.DeviceIdType.MESH
            )
        pl.semaphore_wait(barrier, len(friends))

    def push(self, source, target, device):
        k = len(self.sent)
        copy = pltpu.make_async_remote_copy(
            source,
            target,
            self.send.at[k],
            self.recv.at[k],
            device_id=device,
            device_id_type=pl.DeviceIdType.MESH,
        )
        copy.start()
        self.sent.append(copy)
        return copy

    def finish(self):
        for copy in self.sent:
            copy.wait_send()

    def spot(self, index):
        plan = self.plan
        out, low = index // plan.layers, index % plan.layers
        flip = out % 2
        return (low * (1 - flip) + (plan.layers - 1 - low) * flip) * plan.sides + out

    def ring(self, piece, cut, own=None):
        count = self.plan.contexts
        middle = count // 2
        ahead = {"ctx": self.spot((self.here + 1) % count), "uly": self.uly}
        behind = {"ctx": self.spot((self.here + count - 1) % count), "uly": self.uly}
        last = ()
        for step in range(middle):
            for copy in last:
                copy.wait_recv()
            fore = piece(self.spot((self.here + count - step) % count))
            aft = piece(self.spot((self.here + step) % count))
            first, second = (fore, aft) if step or own is None else (own, own)
            if step == middle - 1:
                fore, first = fore.at[:cut], first.at[:cut]
                aft, second = aft.at[cut:], second.at[cut:]
            last = (self.push(first, fore, ahead), self.push(second, aft, behind))
            yield
        for copy in last:
            copy.wait_recv()

    def slice_send(self, matrix, result, p):
        plan = self.plan
        h = (self.layer + p) % plan.halves
        target = self.at(
            self.core * plan.halves + h,
            self.side,
            self.row,
            plan.cores - 1 - self.layer // plan.halves,
        )
        width = matrix.shape[1] // plan.halves
        cols = pl.ds(pl.multiple_of(h * width, 128), width)
        return self.push(matrix.at[:, cols], result.at[self.ctx], target)

    def slice_pass(self, result, p, held):
        plan = self.plan
        origin = (plan.cores - 1 - self.core) * plan.halves
        origin = origin + (self.layer - p + plan.halves) % plan.halves
        passed = []
        for step in range(plan.sides):
            held.wait_recv()
            slot = result.at[origin * plan.sides + (self.side - step + plan.sides) % plan.sides]
            for dc in range(1, plan.cores):
                core = (self.core + dc) % plan.cores
                passed.append(self.push(slot, slot, self.at(self.layer, self.side, self.row, core)))
            if step < plan.sides - 1:
                side = (self.side + 1) % plan.sides
                held = self.push(slot, slot, self.at(self.layer, side, self.row, self.core))
            yield
        for copy in passed:
            copy.wait_recv()

    def run(self, rings, slices):
        going, queue, flying, moving, turn = [], list(rings), [], [], 0
        tasks = [(m, r, p) for m, r in slices for p in range(self.plan.halves)]

        def drive(generators):
            return [g for g in generators if next(g, "end") != "end"]

        while going or queue or tasks or flying or moving:
            going = drive(going)
            if not going and queue:
                going = drive(queue.pop(0))
            for _ in range(BURST):
                if tasks:
                    matrix, result, p = tasks.pop(0)
                    flying.append((result, p, self.slice_send(matrix, result, p)))
            turn += 1
            if flying and turn > LAG:
                moving.append(self.slice_pass(*flying.pop(0)))
            moving = drive(moving)


def copies_of(plan, slices):
    return slices * plan.halves * (1 + plan.sides - 1 + plan.sides * (plan.cores - 1))


def weights_kernel(plan, *refs):
    tok_in, wq, wk, wv, out_in, gain_in, gate_in = refs[:7]
    tok_all, qkv, out_all, gain_all, gate_all = refs[7:12]
    tok_tmp, qkv_tmp, out_tmp, gain_tmp, local, send, recv = refs[12:]
    link = Sender(plan, send, recv)
    link.meet()
    ulysses, ctx, uly = plan.ulysses, link.ctx, link.uly
    q_cols, k_cols = wq.shape[1] // ulysses, wk.shape[1] // ulysses

    def parts(u):
        yield wq.at[:, pl.ds(pl.multiple_of(u * q_cols, 128), q_cols)], pl.ds(0, q_cols)
        for k, matrix in enumerate((wk, wv)):
            cols = pl.ds(pl.multiple_of(u * k_cols, 128), k_cols)
            yield matrix.at[:, cols], pl.ds(q_cols + k * k_cols, k_cols)

    pairs = [(src, qkv_tmp.at[:, cols]) for src, cols in parts(uly)]
    pairs += [(gain_in, gain_tmp), (out_in, out_tmp), (tok_in, tok_tmp)]
    pulls = [pltpu.make_async_copy(*pair, local.at[k]) for k, pair in enumerate(pairs)]
    for pull in pulls:
        pull.start()
    place = ctx * ulysses + uly
    first = []
    for friend, u in link.group():
        for source, cols in parts(u):
            first.append(link.push(source, qkv.at[place, :, cols], friend))
        first.append(link.push(gain_in, gain_all.at[place], friend))
    for pull in pulls:
        pull.wait()
    pairs = [
        (qkv_tmp, qkv.at[place]),
        (gain_tmp, gain_all.at[place]),
        (out_tmp, out_all.at[ctx]),
        (tok_tmp, tok_all.at[uly]),
    ]
    puts = [pltpu.make_async_copy(*pair, local.at[6 + k]) for k, pair in enumerate(pairs)]
    for put in puts:
        put.start()
    for put in puts:
        put.wait()
    for copy in first:
        copy.wait_recv()
    tokens = [link.push(tok_in, tok_all.at[uly], friend) for friend, _ in link.group()]

    def block(array):
        return lambda c: array.at[pl.ds(c * ulysses, ulysses)]

    rings = [
        [link.ring(block(qkv), ulysses // 2), link.ring(block(gain_all), ulysses // 2)],
        [link.ring(lambda c: out_all.at[c], out_all.shape[1] // 16 * 8)],
    ]
    link.run(rings, [(gate_in, gate_all)])
    for copy in tokens:
        copy.wait_recv()
    link.finish()


anywhere = pl.BlockSpec(memory_space=pl.ANY)


def sliced(plan, weights):
    shape = (plan.contexts, weights.shape[0], weights.shape[1] // plan.halves)
    return jax.ShapeDtypeStruct(shape, weights.dtype)


def fetch_weights(plan, tokens, wq, wk, wv, w_out, gains, w_gate):
    shard, contexts, ulysses = wq.shape[0], plan.contexts, plan.ulysses
    cols = (wq.shape[1] + wk.shape[1] + wv.shape[1]) // ulysses
    results = [
        jax.ShapeDtypeStruct((ulysses, *tokens.shape), tokens.dtype),
        jax.ShapeDtypeStruct((contexts * ulysses, shard, cols), wq.dtype),
        jax.ShapeDtypeStruct((contexts, *w_out.shape), w_out.dtype),
        jax.ShapeDtypeStruct((contexts * ulysses, *gains.shape), gains.dtype),
        sliced(plan, w_gate),
    ]
    copies = 5 * (ulysses - 1) + 3 * contexts + copies_of(plan, 1)
    return pl.pallas_call(
        functools.partial(weights_kernel, plan),
        out_shape=results,
        in_specs=[anywhere] * 7,
        out_specs=[anywhere] * len(results),
        scratch_shapes=[
            pltpu.VMEM(tokens.shape, tokens.dtype),
            pltpu.VMEM((shard, cols), wq.dtype),
            pltpu.VMEM(w_out.shape, w_out.dtype),
            pltpu.VMEM(gains.shape, gains.dtype),
            pltpu.SemaphoreType.DMA((10,)),
            pltpu.SemaphoreType.DMA((copies,)),
            pltpu.SemaphoreType.DMA((copies,)),
        ],
        compiler_params=pltpu.CompilerParams(collective_id=1, has_side_effects=True),
    )(tokens, wq, wk, wv, w_out, gains, w_gate)


def keys_kernel(plan, kv_in, up_in, down_in, kv_all, up_all, down_all, tmp, local, send, recv):
    link = Sender(plan, send, recv)
    link.meet()
    pull = pltpu.make_async_copy(kv_in, tmp, local.at[0])
    put = pltpu.make_async_copy(tmp, kv_all.at[link.ctx], local.at[1])
    pull.start()
    pull.wait()
    put.start()
    ring = link.ring(lambda c: kv_all.at[c], kv_in.shape[0] // 2, kv_in)
    link.run([[ring]], [(up_in, up_all), (down_in, down_all)])
    put.wait()
    link.finish()


def fetch_keys(plan, kv, w_up, w_down):
    copies = plan.contexts + copies_of(plan, 2)
    return pl.pallas_call(
        functools.partial(keys_kernel, plan),
        out_shape=[
            jax.ShapeDtypeStruct((plan.contexts, *kv.shape), kv.dtype),
            sliced(plan, w_up),
            sliced(plan, w_down),
        ],
        in_specs=[anywhere] * 3,
        out_specs=[anywhere] * 3,
        scratch_shapes=[
            pltpu.VMEM(kv.shape, kv.dtype),
            pltpu.SemaphoreType.DMA((2,)),
            pltpu.SemaphoreType.DMA((copies,)),
            pltpu.SemaphoreType.DMA((copies,)),
        ],
        compiler_params=pltpu.CompilerParams(collective_id=2, has_side_effects=True),
    )(kv, w_up, w_down)


def visible(q_first, k_first, boundary, span):
    q_pos = q_first + lax.broadcasted_iota(jnp.int32, (span, span), 0)
    k_pos = k_first + lax.broadcasted_iota(jnp.int32, (span, span), 1)
    low = jnp.where(q_pos >= boundary, boundary, 0)
    return (k_pos <= q_pos) & (k_pos >= low)


def active(q_first, k_first, boundary, span):
    split = (q_first >= boundary) & (k_first + span <= boundary)
    return (k_first <= q_first) & jnp.logical_not(split)


def attend_kernel(span, repeat, count, qp, kp, bd, q_ref, kv_ref, o_ref, lse_ref, acc, den):
    i, j = pl.program_id(0), pl.program_id(1)

    @pl.when(j == 0)
    def _():
        acc[...] = jnp.zeros_like(acc)
        den[...] = jnp.zeros_like(den)

    q_first, k_first, boundary = qp[i], kp[j], bd[0]

    @pl.when(active(q_first, k_first, boundary, span))
    def _():
        allowed = visible(q_first, k_first, boundary, span)
        keys, values = kv_ref[:, :HEAD_DIM], kv_ref[:, HEAD_DIM:]
        for r in range(repeat):
            cols = slice(r * HEAD_DIM, (r + 1) * HEAD_DIM)
            scores = dot(q_ref[:, cols], keys, 1, 1)
            weights = jnp.where(
                allowed, jnp.exp(soft_cap * jnp.tanh(scores * (1.0 / soft_cap))), 0.0
            )
            den[r] += jnp.sum(weights, axis=1, keepdims=True)
            acc[:, cols] += dot(weights.astype(bf16), values)

    @pl.when(j == count - 1)
    def _():
        for r in range(repeat):
            cols = slice(r * HEAD_DIM, (r + 1) * HEAD_DIM)
            total = den[r][:, :1]
            o_ref[:, cols] = (acc[:, cols] / total).astype(bf16)
            lse_ref[:, r * 128 : (r + 1) * 128] = jnp.broadcast_to(jnp.log(total), (span, 128))


def attend(q, kv, q_pos, k_pos, boundary, span):
    rows, width = q.shape
    repeat = width // HEAD_DIM
    count = kv.shape[0] // span
    spec = pltpu.PrefetchScalarGridSpec(
        num_scalar_prefetch=3,
        grid=(rows // span, count),
        in_specs=[
            pl.BlockSpec((span, width), lambda i, j, *_: (i, 0)),
            pl.BlockSpec((span, kv.shape[1]), lambda i, j, *_: (j, 0)),
        ],
        out_specs=[
            pl.BlockSpec((span, width), lambda i, j, *_: (i, 0)),
            pl.BlockSpec((span, 128 * repeat), lambda i, j, *_: (i, 0)),
        ],
        scratch_shapes=[
            pltpu.VMEM((span, width), f32),
            pltpu.VMEM((repeat, span, 128), f32),
        ],
    )
    flops = 2 * rows * kv.shape[0] * width
    return pl.pallas_call(
        functools.partial(attend_kernel, span, repeat, count),
        out_shape=[
            jax.ShapeDtypeStruct((rows, width), bf16),
            jax.ShapeDtypeStruct((rows, 128 * repeat), f32),
        ],
        grid_spec=spec,
        compiler_params=pltpu.CompilerParams(dimension_semantics=("arbitrary", "arbitrary")),
        cost_estimate=pl.CostEstimate(
            flops=flops, bytes_accessed=2 * kv.size * 2, transcendentals=rows * kv.shape[0] * repeat
        ),
    )(q_pos, k_pos, boundary, q, kv)


def attend_back_kernel(
    span, repeat, count, blocks, qp, kp, bd, q_ref, g_ref, lse_ref, ds_ref, kv_ref, dq_ref, dkv_ref, acc, dk, dv
):
    j, i = pl.program_id(0), pl.program_id(1)

    @pl.when((j == 0) & (i == 0))
    def _():
        acc[...] = jnp.zeros_like(acc)

    @pl.when(i == 0)
    def _():
        dk[...] = jnp.zeros_like(dk)
        dv[...] = jnp.zeros_like(dv)

    q_first, k_first, boundary = qp[i], kp[j], bd[0]

    @pl.when(active(q_first, k_first, boundary, span))
    def _():
        allowed = visible(q_first, k_first, boundary, span)
        keys, values = kv_ref[:, :HEAD_DIM], kv_ref[:, HEAD_DIM:]
        rows = pl.ds(pl.multiple_of(i * span, span), span)
        for r in range(repeat):
            cols = slice(r * HEAD_DIM, (r + 1) * HEAD_DIM)
            query, grad = q_ref[rows, cols], g_ref[rows, cols]
            lse = lse_ref[rows, r * 128 : r * 128 + 1]
            dsum = ds_ref[rows, r * 128 : r * 128 + 1]
            bent = jnp.tanh(dot(query, keys, 1, 1) * (1.0 / soft_cap))
            probs = jnp.where(allowed, jnp.exp(soft_cap * bent - lse), 0.0)
            dprob = dot(grad, values, 1, 1)
            dscore = (probs * (dprob - dsum) * (1.0 - bent * bent)).astype(bf16)
            acc[rows, cols] += dot(dscore, keys)
            dk[...] += dot(dscore, query, 0, 0)
            dv[...] += dot(probs.astype(bf16), grad, 0, 0)

    @pl.when(i == blocks - 1)
    def _():
        dkv_ref[:, :HEAD_DIM] = dk[...].astype(dkv_ref.dtype)
        dkv_ref[:, HEAD_DIM:] = dv[...].astype(dkv_ref.dtype)

    @pl.when((j == count - 1) & (i == blocks - 1))
    def _():
        dq_ref[...] = acc[...]


def attend_back(q, grad, lse, dsum, kv, q_pos, k_pos, boundary, span):
    rows, width = q.shape
    repeat = width // HEAD_DIM
    count, blocks = kv.shape[0] // span, rows // span
    whole = lambda w: pl.BlockSpec((rows, w), lambda j, i, *_: (0, 0))
    spec = pltpu.PrefetchScalarGridSpec(
        num_scalar_prefetch=3,
        grid=(count, blocks),
        in_specs=[
            whole(width),
            whole(width),
            whole(128 * repeat),
            whole(128 * repeat),
            pl.BlockSpec((span, kv.shape[1]), lambda j, i, *_: (j, 0)),
        ],
        out_specs=[
            whole(width),
            pl.BlockSpec((span, kv.shape[1]), lambda j, i, *_: (j, 0)),
        ],
        scratch_shapes=[
            pltpu.VMEM((rows, width), f32),
            pltpu.VMEM((span, HEAD_DIM), f32),
            pltpu.VMEM((span, HEAD_DIM), f32),
        ],
    )
    return pl.pallas_call(
        functools.partial(attend_back_kernel, span, repeat, count, blocks),
        out_shape=[
            jax.ShapeDtypeStruct((rows, width), f32),
            jax.ShapeDtypeStruct(kv.shape, bf16),
        ],
        grid_spec=spec,
        compiler_params=pltpu.CompilerParams(dimension_semantics=("arbitrary", "arbitrary")),
        cost_estimate=pl.CostEstimate(
            flops=5 * rows * kv.shape[0] * width,
            bytes_accessed=2 * kv.size * 2,
            transcendentals=rows * kv.shape[0] * repeat,
        ),
    )(q_pos, k_pos, boundary, q, grad, lse, dsum, kv)


def on_device(
    plan,
    tokens,
    cotangent,
    span_order,
    segments,
    w_query,
    w_key,
    w_value,
    w_out,
    w_gate,
    w_up,
    w_down,
    gain_attn_in,
    gain_attn_out,
    gain_ffn_in,
    gain_ffn_out,
):
    rows, width = tokens.shape
    contexts, ulysses = plan.contexts, plan.ulysses
    layers, sides, cores, halves = plan.layers, plan.sides, plan.cores, plan.halves
    group_rows = rows * ulysses
    span = group_rows // 2
    q_scale = float(HEAD_DIM) ** (-0.5)
    ctx = lax.axis_index("ctx")
    layer, side, row, core = plan.here()

    ctx_ring = Ring(
        plan, sides, layers, lambda w, out, inn: (inn, out, w[2], w[3]), lambda w: (w[1], w[0])
    )
    ffn_ring = Ring(
        plan, plan.rows, layers, lambda w, out, inn: (inn, w[1], out, w[3]), lambda w: (w[2], w[0])
    )
    side_ring = Ring(
        plan, 1, sides, lambda w, out, inn: (w[0], inn, w[2], w[3]), lambda w: (0, w[1])
    )
    row_ring = Ring(
        plan, 1, plan.rows, lambda w, out, inn: (w[0], w[1], inn, w[3]), lambda w: (0, w[2])
    )
    core_ring = Ring(
        plan, 1, cores, lambda w, out, inn: (w[0], w[1], w[2], inn), lambda w: (0, w[3])
    )
    ctx_cells = jnp.array([inn * sides + out for out, inn in ctx_ring.cells], jnp.int32)
    ctx_place = ctx_ring.position(side, layer)
    ring_ctx = [ctx_cells[(ctx_place + k) % contexts] for k in range(contexts)]

    def group_gather(values):
        mine = ring_gather(values, row_ring)
        blocks, where = [], []
        for k, block in enumerate(mine):
            for m, found in enumerate(ring_gather(block, core_ring)):
                blocks.append(found)
                where.append((row + k) % plan.rows * cores + (core + m) % cores)
        return place_rows(blocks, where, ulysses).reshape(group_rows, values.shape[1])

    def group_scatter(values):
        parts = values.reshape(plan.rows, cores, rows, values.shape[1])

        def part(k, m):
            at = ((row + k) % plan.rows, (core + m) % cores, 0, 0)
            return lax.dynamic_slice(parts, at, (1, 1, *parts.shape[2:]))[0, 0]

        summed = [
            ring_scatter([part(k, m) for m in range(cores)], core_ring) for k in range(plan.rows)
        ]
        return ring_scatter(summed, row_ring)

    def ctx_scatter(arrays):
        size = arrays[0].shape[0] // contexts

        def part(k):
            blocks = [take_block(array, ring_ctx[k], size) for array in arrays]
            return jnp.concatenate(blocks, axis=1) if len(blocks) > 1 else blocks[0]

        return ring_scatter([part(k) for k in range(contexts)], ctx_ring, bf16)

    shard = gain_attn_in.shape[0]
    places = (ctx_place, row, core)
    tiny_rings = (ctx_ring, row_ring, core_ring)
    ring_order = [inn * sides + out for out, inn in ctx_ring.cells]

    def turn(values, axis, back):
        count, place = values.shape[axis], places[axis]
        start = place if back else (count - place) % count
        twice = jnp.concatenate([values, values], axis=axis)
        return lax.dynamic_slice_in_dim(twice, start, count, axis)

    def sum_gains(parts):
        count = parts.shape[0]
        found = jnp.transpose(parts.reshape(count, contexts * ulysses, shard), (1, 0, 2))
        found = jnp.pad(found, ((0, 0), (0, -count % 8), (0, -shard % 128)))
        found = found.reshape(contexts, plan.rows, cores, *found.shape[1:])
        found = jnp.stack([found[c] for c in ring_order])
        for axis in range(3):
            found = turn(found, axis, True)
        for axis in (2, 1, 0):
            entries = [lax.index_in_dim(found, k, axis, False) for k in range(found.shape[axis])]
            found = ring_scatter(entries, tiny_rings[axis], f32)
        return found[:count, :shard]

    packed = jnp.stack([gain_attn_in, gain_attn_out, gain_ffn_in, gain_ffn_out])
    packed = jnp.pad(packed, ((0, 4), (0, -shard % 128)))
    tok_group, col_qkv, col_out, gains, ffn_gate = fetch_weights(
        plan, tokens, w_query, w_key, w_value, w_out, packed.astype(f32), w_gate
    )
    tok_group = tok_group.reshape(group_rows, width)
    col_qkv = col_qkv.reshape(width, -1)
    col_out = col_out.reshape(width, -1)
    gains = jnp.transpose(gains[:, :4, :shard], (1, 0, 2)).reshape(4, width)
    weight_one, weight_two, weight_three, weight_four = (1.0 + gains[k][None] for k in range(4))

    own_spans = lax.dynamic_slice_in_dim(span_order, 2 * ctx, 2, 0) * span
    boundary = jnp.sum((segments == 0).astype(jnp.int32)).reshape(1)
    key_spans = span_order * span
    group_pos = (own_spans[:, None] + jnp.arange(span, dtype=jnp.int32)[None, :]).reshape(-1)
    half = HEAD_DIM // 2
    freqs = rotary_base ** (-jnp.arange(half).astype(f32) / half)
    angles = group_pos.astype(f32)[:, None] * freqs[None, :]
    cosines, sines = jnp.cos(angles), jnp.sin(angles)

    q_cols, k_cols = w_query.shape[1] // ulysses, w_key.shape[1] // ulysses
    tok_rows = tok_group.astype(f32)
    normed_in = norm_apply(tok_rows, weight_one).astype(bf16)
    qkv = dot(normed_in, col_qkv)
    queries = (rotary(qkv[:, :q_cols], cosines, sines, 1.0) * q_scale).astype(bf16)
    keys = rotary(qkv[:, q_cols : q_cols + k_cols], cosines, sines, 1.0).astype(bf16)
    values = qkv[:, q_cols + k_cols :].astype(bf16)
    kv, ffn_up, ffn_down = fetch_keys(
        plan, jnp.concatenate([keys, values], axis=1), w_up, w_down
    )
    kv = kv.reshape(contexts * group_rows, -1)
    ffn_gate, ffn_up, ffn_down = (w.reshape(width, -1) for w in (ffn_gate, ffn_up, ffn_down))

    slice_cols = w_gate.shape[1] // halves

    def slice_perm(p):
        return plan.perm(lambda l, s, r, c: (c * halves + (l + p) % halves, s, r, l // halves))

    def slice_back(p):
        return [(b, a) for a, b in slice_perm(p)]

    def pick(options, index):
        out = options[0]
        for k in range(1, len(options)):
            out = jnp.where(index == k, options[k], out)
        return out

    def slice_start(grad):
        parts = grad.reshape(cores, halves, sides, -1, slice_cols)
        size = parts.shape[3]
        others = []
        for m in range(1, cores):
            at = ((core + m) % cores, 0, 0, 0, 0)
            piece = lax.dynamic_slice(parts, at, (1, *parts.shape[1:]))[0]
            perm = plan.perm(lambda l, s, r, c, m=m: (l, s, r, (c + m) % cores))
            others.append(move(piece, perm))

        def side_part(k):
            here = (side + k) % sides
            shape = (halves, 1, size, slice_cols)
            found = lax.dynamic_slice(parts, (core, 0, here, 0, 0), (1, *shape))[0].astype(f32)
            for other in others:
                found = found + lax.dynamic_slice(other, (0, here, 0, 0), shape).astype(f32)
            return found.reshape(halves * size, slice_cols)

        summed = ring_scatter([side_part(k) for k in range(sides)], side_ring, bf16)
        return summed.astype(bf16).reshape(halves, size, slice_cols)

    def slice_end(summed):
        got = []
        for p in range(halves):
            piece = lax.dynamic_index_in_dim(summed, (layer - p) % halves, 0, keepdims=False)
            got.append(move(piece, slice_back(p)))
        cuts = [pick(got, (h - layer) % halves) for h in range(halves)]
        return jnp.concatenate(cuts, axis=1).astype(f32)

    head_o, lse = attend(queries, kv, own_spans, key_spans, boundary, span)
    attn_out = group_scatter(dot(head_o, col_out, 1, 1))
    tok_own = tokens.astype(f32)
    hidden_in = tok_own + norm_apply(attn_out, weight_two)
    normed_own = norm_apply(hidden_in, weight_three).astype(bf16)

    size = ffn_ring.size
    order = [0]
    for k in range(1, size // 2):
        order += [k, size - k]
    order.append(size // 2)
    near = max(size - 3, 1)

    def ffn_gather(values):
        found = ring_gather(values, ffn_ring)
        return [
            jnp.concatenate([found[k] for k in ks], axis=0) for ks in (order[:near], order[near:])
        ]

    def ffn_scatter(chunk):
        parts = [None] * size
        far = chunk(1, None)
        for values, ks in ((far, order[near:]), (chunk(0, far), order[:near])):
            for n, k in enumerate(ks):
                parts[k] = values[n * rows : (n + 1) * rows]
        landed = []
        return ring_scatter(parts, ffn_ring, bf16, landed), landed

    normed_mid = ffn_gather(normed_own)
    gate = [dot(x, ffn_gate) for x in normed_mid]
    upper = [dot(x, ffn_up) for x in normed_mid]
    hidden = [(gelu_parts(g)[0] * u).astype(bf16) for g, u in zip(gate, upper, strict=True)]

    def down_part(n, far):
        rows_in = hidden[n] if far is None else after(hidden[n], far)
        return dot(rows_in, ffn_down, 1, 1)

    ffn_out, _ = ffn_scatter(down_part)
    block_out = (hidden_in + norm_apply(ffn_out, weight_four)).astype(bf16)
    cot_own = cotangent.astype(f32)
    d_ffn = ffn_gather(norm_grad(ffn_out, weight_four, cot_own).astype(bf16))
    d_gate, d_upper = [], []
    for n in range(2):
        d_hidden = dot(d_ffn[n], ffn_down)
        gate_value, gate_slope = gelu_parts(gate[n])
        d_gate.append((d_hidden * upper[n] * gate_slope).astype(bf16))
        d_upper.append((d_hidden * gate_value).astype(bf16))

    def mid_part(n, far):
        left, right = d_gate[n], d_upper[n]
        if far is not None:
            left, right = after(left, far), after(right, far)
        return dot(left, ffn_gate, 1, 1) + dot(right, ffn_up, 1, 1)

    d_mid, landed = ffn_scatter(mid_part)
    grad_hidden = cot_own + norm_grad(hidden_in, weight_three, d_mid)
    joined = [jnp.concatenate(x, axis=0) for x in (d_ffn, hidden, normed_mid, d_gate, d_upper)]

    def weight_grad(left, right, step):
        left = after(left, landed[min(step, len(landed) - 1)])
        grad = dot(left, right, 0, 0).astype(bf16)
        return slice_start(grad)

    sum_down = weight_grad(joined[0], joined[1], 0)
    sum_gate = weight_grad(joined[2], joined[3], 1)
    sum_up = weight_grad(joined[2], joined[4], 2)
    grad_down = slice_end(after(sum_down, d_mid))
    grad_gate = slice_end(after(sum_gate, d_mid))

    d_attn = group_gather(norm_grad(attn_out, weight_two, grad_hidden).astype(bf16))
    out_part = dot(d_attn, head_o, 0, 0).astype(bf16)
    grad_o = dot(d_attn, col_out).astype(bf16)
    products = grad_o.astype(f32) * head_o.astype(f32)
    dsum = jnp.concatenate(
        [
            jnp.broadcast_to(
                jnp.sum(products[:, s : s + HEAD_DIM], axis=1, keepdims=True), (group_rows, 128)
            )
            for s in range(0, q_cols, HEAD_DIM)
        ],
        axis=1,
    )
    grad_q, grad_kv = attend_back(
        queries, grad_o, lse, dsum, kv, own_spans, key_spans, boundary, span
    )
    grad_kv = ctx_scatter([grad_kv])
    grad_up = slice_end(after(sum_up, grad_kv))
    grad_q = (rotary(grad_q, cosines, sines, -1.0) * q_scale).astype(bf16)
    grad_k = rotary(grad_kv[:, :k_cols], cosines, sines, -1.0).astype(bf16)
    grad_v = grad_kv[:, k_cols:].astype(bf16)
    grad_qkv = jnp.concatenate([grad_q, grad_k, grad_v], axis=1)
    d_in_part = dot(grad_qkv, col_qkv, 1, 1)
    d_in = group_scatter(d_in_part)
    grad_tokens = grad_hidden + norm_grad(tok_own, weight_one, d_in)
    qkv_part = dot(normed_in, grad_qkv, 0, 0).astype(bf16)
    mixed_grad = ctx_scatter([qkv_part, out_part])
    grad_outproj = mixed_grad[:, qkv_part.shape[1] :]
    mixed_grad = mixed_grad[:, : qkv_part.shape[1]].astype(bf16)
    mixed_grad = lax.all_to_all(
        mixed_grad.reshape(ulysses, -1, mixed_grad.shape[1]),
        "uly",
        split_axis=0,
        concat_axis=0,
        tiled=True,
    )
    mixed_grad = jnp.transpose(mixed_grad, (1, 0, 2)).astype(f32)
    grad_query = mixed_grad[:, :, :q_cols].reshape(w_query.shape)
    grad_key = mixed_grad[:, :, q_cols : q_cols + k_cols].reshape(w_key.shape)
    grad_value = mixed_grad[:, :, q_cols + k_cols :].reshape(w_value.shape)

    gain_grads = sum_gains(
        jnp.stack(
            [
                gain_part(attn_out, after(grad_hidden, grad_q)),
                gain_part(hidden_in, after(d_mid, grad_q)),
                gain_part(ffn_out, after(cot_own, grad_q)),
            ]
        )
    )
    products = [
        jnp.sum(w.astype(f32) * g, axis=1)
        for w, g in ((w_query, grad_query), (w_key, grad_key), (w_value, grad_value))
    ]
    gain_first = (products[0] + products[1] + products[2]) / (1.0 + gain_attn_in.astype(f32))
    return (
        block_out,
        grad_tokens,
        grad_query,
        grad_key,
        grad_value,
        grad_outproj,
        grad_gate,
        grad_up,
        grad_down,
        gain_first,
        gain_grads[0],
        gain_grads[1],
        gain_grads[2],
    )


def solution(mesh):
    flat, cut, line = P(AXES, None), P("ctx", "uly"), P(AXES)
    in_specs = (flat, flat, P(), P(), flat, flat, flat, cut, cut, cut, cut, line, line, line, line)
    out_specs = (flat, flat, flat, flat, flat, cut, cut, cut, cut, line, line, line, line)
    plan = Plan(mesh)

    def body(*args):
        return on_device(plan, *args)

    return jax.shard_map(
        body, mesh=mesh, in_specs=in_specs, out_specs=out_specs, check_vma=False
    )
```

```python
import functools

import jax
import jax.numpy as jnp
from jax import lax
from jax.experimental import pallas as pl
from jax.experimental.pallas import tpu as pltpu
from jax.sharding import PartitionSpec as P


HEAD_DIM = 256
AXES = ("ctx", "uly")

norm_eps = 1e-06
soft_cap = 50.0
rotary_base = 10000.0
gelu_coef = 0.7978845608028654
cubic_coef = 0.044715


bf16 = jnp.bfloat16
f32 = jnp.float32


def rms_scale(values):
    return lax.rsqrt(jnp.mean(values * values, axis=-1, keepdims=True) + norm_eps)


def norm_apply(values, weight):
    return values * rms_scale(values) * weight


def norm_grad(values, weight, grad):
    scale = rms_scale(values)
    inner = jnp.mean(grad * weight * values, axis=-1, keepdims=True)
    return scale * weight * grad - values * (scale * scale * scale) * inner


def gain_part(values, grad):
    return jnp.sum(grad * values * rms_scale(values), axis=0)


def gelu_parts(values):
    inner = gelu_coef * (values + cubic_coef * values * values * values)
    tanh_part = jnp.tanh(inner)
    value = 0.5 * values * (1.0 + tanh_part)
    slope = 0.5 * (1.0 + tanh_part) + 0.5 * values * (1.0 - tanh_part * tanh_part) * gelu_coef * (
        1.0 + 3.0 * cubic_coef * values * values
    )
    return value, slope


def rotary(values, cosines, sines, sign):
    half = HEAD_DIM // 2
    parts = []
    for start in range(0, values.shape[1], HEAD_DIM):
        first = values[:, start : start + half]
        second = values[:, start + half : start + HEAD_DIM]
        parts.append(first * cosines - sign * second * sines)
        parts.append(second * cosines + sign * first * sines)
    return jnp.concatenate(parts, axis=1)


def dot(left, right, left_dim=1, right_dim=0):
    return lax.dot_general(
        left, right, (((left_dim,), (right_dim,)), ((), ())), preferred_element_type=f32
    )


class Plan:
    def __init__(self, mesh):
        grid = mesh.devices
        self.contexts, self.ulysses = mesh.shape["ctx"], mesh.shape["uly"]
        self.cores = sum(tuple(d.coords) == tuple(grid[0, 0].coords) for d in grid[0])
        self.layers = len({d.coords[2] for d in grid[:, 0]})
        self.sides = self.contexts // self.layers
        self.rows = self.ulysses // self.cores
        self.halves = self.layers // self.cores

    def split(self, device):
        ctx, uly = divmod(device, self.ulysses)
        return (*divmod(ctx, self.sides), *divmod(uly, self.cores))

    def join(self, layer, side, row, core):
        return (layer * self.sides + side) * self.ulysses + row * self.cores + core

    def perm(self, target):
        count = self.contexts * self.ulysses
        return [(d, self.join(*target(*self.split(d)))) for d in range(count)]

    def here(self):
        layer, side = jnp.divmod(lax.axis_index("ctx"), self.sides)
        row, core = jnp.divmod(lax.axis_index("uly"), self.cores)
        return layer, side, row, core


class Ring:
    def __init__(self, plan, outer, inner, place, locate):
        self.size = outer * inner
        self.inner = inner

        def cell(index):
            out, rest = divmod(index % self.size, inner)
            return out, (rest if out % 2 == 0 else inner - 1 - rest)

        def index_of(out, inn):
            return out * inner + (inn if out % 2 == 0 else inner - 1 - inn)

        self.cells = [cell(i) for i in range(self.size)]

        def shifted(step):
            def target(*where):
                return place(where, *cell(index_of(*locate(where)) + step))

            return plan.perm(target)

        self.ahead, self.behind = shifted(1), shifted(-1)

    def position(self, out, inn):
        rest = jnp.where(out % 2 == 0, inn, self.inner - 1 - inn)
        return out * self.inner + rest


def move(values, perm):
    return lax.ppermute(values, AXES, perm)


def both(*values):
    return lax.optimization_barrier(values)


def after(values, *earlier):
    return lax.optimization_barrier((values, *earlier))[0]


def ring_gather(block, ring):
    size = ring.size
    found = {0: block}
    if size == 2:
        found[1] = move(block, ring.ahead)
        return [found[0], found[1]]
    forth = back = block
    middle = size // 2
    for step in range(1, middle):
        forth = move(forth, ring.ahead)
        back = move(back, ring.behind)
        forth, back = both(forth, back)
        found[size - step], found[step] = forth, back
    cut = block.shape[0] // 2
    forth = move(forth[:cut], ring.ahead)
    back = move(back[cut:], ring.behind)
    found[middle] = jnp.concatenate([forth, back], axis=0)
    return [found[k] for k in range(size)]


def ring_scatter(parts, ring, kind=bf16, landed=None):
    size = ring.size
    if size == 2:
        return parts[0].astype(f32) + move(parts[1].astype(kind), ring.ahead).astype(f32)
    middle = size // 2
    cut = parts[0].shape[0] // 2
    forth = move(parts[middle][:cut].astype(kind), ring.ahead)
    back = move(parts[middle][cut:].astype(kind), ring.behind)
    forth, back = both(forth, back)
    landed = [] if landed is None else landed
    for left in range(middle - 1, 0, -1):
        landed.append(forth)
        fore, aft = parts[left].astype(f32), parts[size - left].astype(f32)
        if left == middle - 1:
            fore = jnp.concatenate([fore[:cut] + forth.astype(f32), fore[cut:]], axis=0)
            aft = jnp.concatenate([aft[:cut], aft[cut:] + back.astype(f32)], axis=0)
        else:
            fore, aft = fore + forth.astype(f32), aft + back.astype(f32)
        forth = move(fore.astype(kind), ring.ahead)
        back = move(aft.astype(kind), ring.behind)
        forth, back = both(forth, back)
    return parts[0].astype(f32) + forth.astype(f32) + back.astype(f32)


def place_rows(blocks, indices, count):
    first = blocks[0]
    out = jnp.zeros((count, *first.shape), first.dtype)
    for block, index in zip(blocks, indices, strict=True):
        out = lax.dynamic_update_slice(out, block[None], (index, *(0,) * first.ndim))
    return out


def take_block(values, index, size):
    return lax.dynamic_slice_in_dim(values, index * size, size, 0)


class Sender:
    def __init__(self, plan, send, recv):
        self.plan, self.send, self.recv, self.sent = plan, send, recv, []
        self.ctx, self.uly = lax.axis_index("ctx"), lax.axis_index("uly")
        self.layer, self.side = self.ctx // plan.sides, self.ctx % plan.sides
        self.row, self.core = self.uly // plan.cores, self.uly % plan.cores
        flip = self.side % 2
        self.here = self.side * plan.layers + (
            self.layer * (1 - flip) + (plan.layers - 1 - self.layer) * flip
        )

    def at(self, layer, side, row, core):
        plan = self.plan
        return {"ctx": layer * plan.sides + side, "uly": row * plan.cores + core}

    def group(self):
        plan = self.plan
        for dr in range(plan.rows - 1, -1, -1):
            for dc in range(plan.cores):
                if (dr, dc) != (0, 0):
                    row, core = (self.row + dr) % plan.rows, (self.core + dc) % plan.cores
                    yield self.at(self.layer, self.side, row, core), row * plan.cores + core

    def meet(self):
        plan = self.plan
        friends = [friend for friend, _ in self.group()]
        for dl in range(1, plan.layers):
            for dc in range(plan.cores):
                layer, core = (self.layer + dl) % plan.layers, (self.core + dc) % plan.cores
                friends.append(self.at(layer, self.side, self.row, core))
        for ds in sorted({1 % plan.sides, plan.sides - 1} - {0}):
            side = (self.side + ds) % plan.sides
            friends.append(self.at(self.layer, side, self.row, self.core))
        barrier = pltpu.get_barrier_semaphore()
        for friend in friends:
            pl.semaphore_signal(
                barrier, inc=1, device_id=friend, device_id_type=pl.DeviceIdType.MESH
            )
        pl.semaphore_wait(barrier, len(friends))

    def push(self, source, target, device):
        k = len(self.sent)
        copy = pltpu.make_async_remote_copy(
            source,
            target,
            self.send.at[k],
            self.recv.at[k],
            device_id=device,
            device_id_type=pl.DeviceIdType.MESH,
        )
        copy.start()
        self.sent.append(copy)
        return copy

    def finish(self):
        for copy in self.sent:
            copy.wait_send()

    def spot(self, index):
        plan = self.plan
        out, low = index // plan.layers, index % plan.layers
        flip = out % 2
        return (low * (1 - flip) + (plan.layers - 1 - low) * flip) * plan.sides + out

    def ring(self, piece, cut, own=None):
        count = self.plan.contexts
        middle = count // 2
        ahead = {"ctx": self.spot((self.here + 1) % count), "uly": self.uly}
        behind = {"ctx": self.spot((self.here + count - 1) % count), "uly": self.uly}
        last = ()
        for step in range(middle):
            for copy in last:
                copy.wait_recv()
            fore = piece(self.spot((self.here + count - step) % count))
            aft = piece(self.spot((self.here + step) % count))
            first, second = (fore, aft) if step or own is None else (own, own)
            if step == middle - 1:
                fore, first = fore.at[:cut], first.at[:cut]
                aft, second = aft.at[cut:], second.at[cut:]
            last = (self.push(first, fore, ahead), self.push(second, aft, behind))
            yield
        for copy in last:
            copy.wait_recv()

    def slice_send(self, matrix, result, p):
        plan = self.plan
        h = (self.layer + p) % plan.halves
        target = self.at(
            self.core * plan.halves + h,
            self.side,
            self.row,
            plan.cores - 1 - self.layer // plan.halves,
        )
        width = matrix.shape[1] // plan.halves
        cols = pl.ds(pl.multiple_of(h * width, 128), width)
        return self.push(matrix.at[:, cols], result.at[self.ctx], target)

    def slice_pass(self, result, p, held):
        plan = self.plan
        origin = (plan.cores - 1 - self.core) * plan.halves
        origin = origin + (self.layer - p + plan.halves) % plan.halves
        passed = []
        for step in range(plan.sides):
            held.wait_recv()
            slot = result.at[origin * plan.sides + (self.side - step + plan.sides) % plan.sides]
            for dc in range(1, plan.cores):
                core = (self.core + dc) % plan.cores
                passed.append(self.push(slot, slot, self.at(self.layer, self.side, self.row, core)))
            if step < plan.sides - 1:
                side = (self.side + 1) % plan.sides
                held = self.push(slot, slot, self.at(self.layer, side, self.row, self.core))
            yield
        for copy in passed:
            copy.wait_recv()

    def run(self, rings, slices):
        flying, moving = [], []
        tasks = [(m, r, p) for m, r in slices for p in range(self.plan.halves)]

        def drive(generators):
            return [g for g in generators if next(g, "end") != "end"]

        while rings or tasks or flying or moving:
            rings = drive(rings)
            if flying:
                moving.append(self.slice_pass(*flying.pop(0)))
            if tasks:
                matrix, result, p = tasks.pop(0)
                flying.append((result, p, self.slice_send(matrix, result, p)))
            moving = drive(moving)


def copies_of(plan, slices):
    return slices * plan.halves * (1 + plan.sides - 1 + plan.sides * (plan.cores - 1))


def weights_kernel(plan, *refs):
    tok_in, wq, wk, wv, out_in, gain_in, gate_in = refs[:7]
    tok_all, qkv, out_all, gain_all, gate_all = refs[7:12]
    tok_tmp, qkv_tmp, out_tmp, gain_tmp, local, send, recv = refs[12:]
    link = Sender(plan, send, recv)
    link.meet()
    ulysses, ctx, uly = plan.ulysses, link.ctx, link.uly
    q_cols, k_cols = wq.shape[1] // ulysses, wk.shape[1] // ulysses

    def parts(u):
        yield wq.at[:, pl.ds(pl.multiple_of(u * q_cols, 128), q_cols)], pl.ds(0, q_cols)
        for k, matrix in enumerate((wk, wv)):
            cols = pl.ds(pl.multiple_of(u * k_cols, 128), k_cols)
            yield matrix.at[:, cols], pl.ds(q_cols + k * k_cols, k_cols)

    pairs = [(src, qkv_tmp.at[:, cols]) for src, cols in parts(uly)]
    pairs += [(gain_in, gain_tmp), (out_in, out_tmp), (tok_in, tok_tmp)]
    pulls = [pltpu.make_async_copy(*pair, local.at[k]) for k, pair in enumerate(pairs)]
    for pull in pulls:
        pull.start()
    place = ctx * ulysses + uly
    first = []
    for friend, u in link.group():
        for source, cols in parts(u):
            first.append(link.push(source, qkv.at[place, :, cols], friend))
        first.append(link.push(gain_in, gain_all.at[place], friend))
    for pull in pulls:
        pull.wait()
    pairs = [
        (qkv_tmp, qkv.at[place]),
        (gain_tmp, gain_all.at[place]),
        (out_tmp, out_all.at[ctx]),
        (tok_tmp, tok_all.at[uly]),
    ]
    puts = [pltpu.make_async_copy(*pair, local.at[6 + k]) for k, pair in enumerate(pairs)]
    for put in puts:
        put.start()
    for put in puts:
        put.wait()
    for copy in first:
        copy.wait_recv()
    tokens = [link.push(tok_in, tok_all.at[uly], friend) for friend, _ in link.group()]

    def block(array):
        return lambda c: array.at[pl.ds(c * ulysses, ulysses)]

    rings = [
        link.ring(block(qkv), ulysses // 2),
        link.ring(block(gain_all), ulysses // 2),
        link.ring(lambda c: out_all.at[c], out_all.shape[1] // 16 * 8),
    ]
    link.run(rings, [(gate_in, gate_all)])
    for copy in tokens:
        copy.wait_recv()
    link.finish()


anywhere = pl.BlockSpec(memory_space=pl.ANY)


def sliced(plan, weights):
    shape = (plan.contexts, weights.shape[0], weights.shape[1] // plan.halves)
    return jax.ShapeDtypeStruct(shape, weights.dtype)


def fetch_weights(plan, tokens, wq, wk, wv, w_out, gains, w_gate):
    shard, contexts, ulysses = wq.shape[0], plan.contexts, plan.ulysses
    cols = (wq.shape[1] + wk.shape[1] + wv.shape[1]) // ulysses
    results = [
        jax.ShapeDtypeStruct((ulysses, *tokens.shape), tokens.dtype),
        jax.ShapeDtypeStruct((contexts * ulysses, shard, cols), wq.dtype),
        jax.ShapeDtypeStruct((contexts, *w_out.shape), w_out.dtype),
        jax.ShapeDtypeStruct((contexts * ulysses, *gains.shape), gains.dtype),
        sliced(plan, w_gate),
    ]
    copies = 5 * (ulysses - 1) + 3 * contexts + copies_of(plan, 1)
    return pl.pallas_call(
        functools.partial(weights_kernel, plan),
        out_shape=results,
        in_specs=[anywhere] * 7,
        out_specs=[anywhere] * len(results),
        scratch_shapes=[
            pltpu.VMEM(tokens.shape, tokens.dtype),
            pltpu.VMEM((shard, cols), wq.dtype),
            pltpu.VMEM(w_out.shape, w_out.dtype),
            pltpu.VMEM(gains.shape, gains.dtype),
            pltpu.SemaphoreType.DMA((10,)),
            pltpu.SemaphoreType.DMA((copies,)),
            pltpu.SemaphoreType.DMA((copies,)),
        ],
        compiler_params=pltpu.CompilerParams(collective_id=1, has_side_effects=True),
    )(tokens, wq, wk, wv, w_out, gains, w_gate)


def keys_kernel(plan, kv_in, up_in, kv_all, up_all, tmp, local, send, recv):
    link = Sender(plan, send, recv)
    link.meet()
    pull = pltpu.make_async_copy(kv_in, tmp, local.at[0])
    put = pltpu.make_async_copy(tmp, kv_all.at[link.ctx], local.at[1])
    pull.start()
    pull.wait()
    put.start()
    ring = link.ring(lambda c: kv_all.at[c], kv_in.shape[0] // 2, kv_in)
    link.run([ring], [(up_in, up_all)])
    put.wait()
    link.finish()


def fetch_keys(plan, kv, w_up):
    copies = plan.contexts + copies_of(plan, 1)
    return pl.pallas_call(
        functools.partial(keys_kernel, plan),
        out_shape=[
            jax.ShapeDtypeStruct((plan.contexts, *kv.shape), kv.dtype),
            sliced(plan, w_up),
        ],
        in_specs=[anywhere] * 2,
        out_specs=[anywhere] * 2,
        scratch_shapes=[
            pltpu.VMEM(kv.shape, kv.dtype),
            pltpu.SemaphoreType.DMA((2,)),
            pltpu.SemaphoreType.DMA((copies,)),
            pltpu.SemaphoreType.DMA((copies,)),
        ],
        compiler_params=pltpu.CompilerParams(collective_id=2, has_side_effects=True),
    )(kv, w_up)


def visible(q_first, k_first, boundary, span):
    q_pos = q_first + lax.broadcasted_iota(jnp.int32, (span, span), 0)
    k_pos = k_first + lax.broadcasted_iota(jnp.int32, (span, span), 1)
    low = jnp.where(q_pos >= boundary, boundary, 0)
    return (k_pos <= q_pos) & (k_pos >= low)


def active(q_first, k_first, boundary, span):
    split = (q_first >= boundary) & (k_first + span <= boundary)
    return (k_first <= q_first) & jnp.logical_not(split)


def whole(q_first, k_first, boundary, span):
    same = (k_first >= boundary) | (q_first + span <= boundary)
    return (k_first + span <= q_first) & same


def over_pairs(span, blocks, chunk, qp, kp, bd, work):
    start = pl.program_id(0) * chunk

    def pair(t, carry):
        i, j = t % blocks, t // blocks
        q_first, k_first, boundary = qp[i], kp[start + j], bd[0]
        q_rows = pl.ds(pl.multiple_of(i * span, span), span)
        k_rows = pl.ds(pl.multiple_of(j * span, span), span)
        full = whole(q_first, k_first, boundary, span)

        @pl.when(full)
        def _():
            work(q_rows, k_rows, None)

        @pl.when(active(q_first, k_first, boundary, span) & jnp.logical_not(full))
        def _():
            work(q_rows, k_rows, visible(q_first, k_first, boundary, span))

        return carry

    lax.fori_loop(0, blocks * chunk, pair, 0)


def attend_kernel(span, repeat, steps, chunk, qp, kp, bd, q_ref, kv_ref, o_ref, lse_ref, acc, den):
    step = pl.program_id(0)

    @pl.when(step == 0)
    def _():
        acc[...] = jnp.zeros_like(acc)
        den[...] = jnp.zeros_like(den)

    def work(q_rows, k_rows, allowed):
        keys, values = kv_ref[k_rows, :HEAD_DIM], kv_ref[k_rows, HEAD_DIM:]
        for r in range(repeat):
            cols = slice(r * HEAD_DIM, (r + 1) * HEAD_DIM)
            scores = dot(q_ref[q_rows, cols], keys, 1, 1)
            weights = jnp.exp(soft_cap * jnp.tanh(scores * (1.0 / soft_cap)))
            if allowed is not None:
                weights = jnp.where(allowed, weights, 0.0)
            folded = weights[:, :128]
            for k in range(128, span, 128):
                folded = folded + weights[:, k : k + 128]
            den[q_rows, r * 128 : (r + 1) * 128] += folded
            acc[q_rows, cols] += dot(weights.astype(bf16), values)

    over_pairs(span, q_ref.shape[0] // span, chunk, qp, kp, bd, work)

    @pl.when(step == steps - 1)
    def _():
        for r in range(repeat):
            cols, lanes = slice(r * HEAD_DIM, (r + 1) * HEAD_DIM), slice(r * 128, (r + 1) * 128)
            total = jnp.sum(den[:, lanes], axis=1, keepdims=True)
            o_ref[:, cols] = (acc[:, cols] / total).astype(bf16)
            lse_ref[:, lanes] = jnp.broadcast_to(jnp.log(total), den[:, lanes].shape)


def key_chunk(count):
    return next(c for c in (4, 2, 1) if count % c == 0)


def attend(q, kv, q_pos, k_pos, boundary, span):
    rows, width = q.shape
    repeat = width // HEAD_DIM
    count = kv.shape[0] // span
    chunk = key_chunk(count)
    spec = pltpu.PrefetchScalarGridSpec(
        num_scalar_prefetch=3,
        grid=(count // chunk,),
        in_specs=[
            pl.BlockSpec((rows, width), lambda j, *_: (0, 0)),
            pl.BlockSpec((chunk * span, kv.shape[1]), lambda j, *_: (j, 0)),
        ],
        out_specs=[
            pl.BlockSpec((rows, width), lambda j, *_: (0, 0)),
            pl.BlockSpec((rows, 128 * repeat), lambda j, *_: (0, 0)),
        ],
        scratch_shapes=[
            pltpu.VMEM((rows, width), f32),
            pltpu.VMEM((rows, 128 * repeat), f32),
        ],
    )
    return pl.pallas_call(
        functools.partial(attend_kernel, span, repeat, count // chunk, chunk),
        out_shape=[
            jax.ShapeDtypeStruct((rows, width), bf16),
            jax.ShapeDtypeStruct((rows, 128 * repeat), f32),
        ],
        grid_spec=spec,
        compiler_params=pltpu.CompilerParams(dimension_semantics=("arbitrary",)),
        cost_estimate=pl.CostEstimate(
            flops=2 * rows * kv.shape[0] * width,
            bytes_accessed=2 * kv.size * 2,
            transcendentals=rows * kv.shape[0] * repeat,
        ),
    )(q_pos, k_pos, boundary, q, kv)


def attend_back_kernel(
    span, repeat, chunk, qp, kp, bd, q_ref, g_ref, lse_ref, ds_ref, kv_ref, dq_ref, dkv_ref, acc
):
    step = pl.program_id(0)

    @pl.when(step == 0)
    def _():
        dq_ref[...] = jnp.zeros_like(dq_ref)

    acc[...] = jnp.zeros_like(acc)

    def work(q_rows, k_rows, allowed):
        keys, values = kv_ref[k_rows, :HEAD_DIM], kv_ref[k_rows, HEAD_DIM:]
        for r in range(repeat):
            cols = slice(r * HEAD_DIM, (r + 1) * HEAD_DIM)
            query, grad = q_ref[q_rows, cols], g_ref[q_rows, cols]
            lse = lse_ref[q_rows, r * 128 : r * 128 + 1]
            dsum = ds_ref[q_rows, r * 128 : r * 128 + 1]
            bent = jnp.tanh(dot(query, keys, 1, 1) * (1.0 / soft_cap))
            probs = jnp.exp(soft_cap * bent - lse)
            if allowed is not None:
                probs = jnp.where(allowed, probs, 0.0)
            dprob = dot(grad, values, 1, 1)
            dscore = (probs * (dprob - dsum) * (1.0 - bent * bent)).astype(bf16)
            dq_ref[q_rows, cols] += dot(dscore, keys)
            acc[k_rows, :HEAD_DIM] += dot(dscore, query, 0, 0)
            acc[k_rows, HEAD_DIM:] += dot(probs.astype(bf16), grad, 0, 0)

    over_pairs(span, q_ref.shape[0] // span, chunk, qp, kp, bd, work)
    dkv_ref[...] = acc[...].astype(dkv_ref.dtype)


def attend_back(q, grad, lse, dsum, kv, q_pos, k_pos, boundary, span):
    rows, width = q.shape
    repeat = width // HEAD_DIM
    count = kv.shape[0] // span
    chunk = key_chunk(count)
    fixed = lambda w: pl.BlockSpec((rows, w), lambda j, *_: (0, 0))
    moving = pl.BlockSpec((chunk * span, kv.shape[1]), lambda j, *_: (j, 0))
    spec = pltpu.PrefetchScalarGridSpec(
        num_scalar_prefetch=3,
        grid=(count // chunk,),
        in_specs=[fixed(width), fixed(width), fixed(128 * repeat), fixed(128 * repeat), moving],
        out_specs=[fixed(width), moving],
        scratch_shapes=[pltpu.VMEM((chunk * span, kv.shape[1]), f32)],
    )
    return pl.pallas_call(
        functools.partial(attend_back_kernel, span, repeat, chunk),
        out_shape=[
            jax.ShapeDtypeStruct((rows, width), f32),
            jax.ShapeDtypeStruct(kv.shape, bf16),
        ],
        grid_spec=spec,
        compiler_params=pltpu.CompilerParams(dimension_semantics=("arbitrary",)),
        cost_estimate=pl.CostEstimate(
            flops=5 * rows * kv.shape[0] * width,
            bytes_accessed=2 * kv.size * 2,
            transcendentals=rows * kv.shape[0] * repeat,
        ),
    )(q_pos, k_pos, boundary, q, grad, lse, dsum, kv)


def on_device(
    plan,
    tokens,
    cotangent,
    span_order,
    segments,
    w_query,
    w_key,
    w_value,
    w_out,
    w_gate,
    w_up,
    w_down,
    gain_attn_in,
    gain_attn_out,
    gain_ffn_in,
    gain_ffn_out,
):
    rows, width = tokens.shape
    contexts, ulysses = plan.contexts, plan.ulysses
    layers, sides, cores, halves = plan.layers, plan.sides, plan.cores, plan.halves
    group_rows = rows * ulysses
    span = group_rows // 2
    q_scale = float(HEAD_DIM) ** (-0.5)
    ctx = lax.axis_index("ctx")
    layer, side, row, core = plan.here()

    ctx_ring = Ring(
        plan, sides, layers, lambda w, out, inn: (inn, out, w[2], w[3]), lambda w: (w[1], w[0])
    )
    ffn_ring = Ring(
        plan, plan.rows, layers, lambda w, out, inn: (inn, w[1], out, w[3]), lambda w: (w[2], w[0])
    )
    side_ring = Ring(
        plan, 1, sides, lambda w, out, inn: (w[0], inn, w[2], w[3]), lambda w: (0, w[1])
    )
    row_ring = Ring(
        plan, 1, plan.rows, lambda w, out, inn: (w[0], w[1], inn, w[3]), lambda w: (0, w[2])
    )
    core_ring = Ring(
        plan, 1, cores, lambda w, out, inn: (w[0], w[1], w[2], inn), lambda w: (0, w[3])
    )
    ctx_cells = jnp.array([inn * sides + out for out, inn in ctx_ring.cells], jnp.int32)
    ctx_place = ctx_ring.position(side, layer)
    ring_ctx = [ctx_cells[(ctx_place + k) % contexts] for k in range(contexts)]

    def group_gather(values):
        mine = ring_gather(values, row_ring)
        blocks, where = [], []
        for k, block in enumerate(mine):
            for m, found in enumerate(ring_gather(block, core_ring)):
                blocks.append(found)
                where.append((row + k) % plan.rows * cores + (core + m) % cores)
        return place_rows(blocks, where, ulysses).reshape(group_rows, values.shape[1])

    def group_scatter(values):
        parts = values.reshape(plan.rows, cores, rows, values.shape[1])

        def part(k, m):
            at = ((row + k) % plan.rows, (core + m) % cores, 0, 0)
            return lax.dynamic_slice(parts, at, (1, 1, *parts.shape[2:]))[0, 0]

        summed = [
            ring_scatter([part(k, m) for m in range(cores)], core_ring) for k in range(plan.rows)
        ]
        return ring_scatter(summed, row_ring)

    def ctx_scatter(arrays):
        size = arrays[0].shape[0] // contexts

        def part(k):
            blocks = [take_block(array, ring_ctx[k], size) for array in arrays]
            return jnp.concatenate(blocks, axis=1) if len(blocks) > 1 else blocks[0]

        return ring_scatter([part(k) for k in range(contexts)], ctx_ring, bf16)

    shard = gain_attn_in.shape[0]
    places = (ctx_place, row, core)
    tiny_rings = (ctx_ring, row_ring, core_ring)
    ring_order = [inn * sides + out for out, inn in ctx_ring.cells]

    def turn(values, axis, back):
        count, place = values.shape[axis], places[axis]
        start = place if back else (count - place) % count
        twice = jnp.concatenate([values, values], axis=axis)
        return lax.dynamic_slice_in_dim(twice, start, count, axis)

    def sum_gains(parts):
        count = parts.shape[0]
        found = jnp.transpose(parts.reshape(count, contexts * ulysses, shard), (1, 0, 2))
        found = jnp.pad(found, ((0, 0), (0, -count % 8), (0, -shard % 128)))
        found = found.reshape(contexts, plan.rows, cores, *found.shape[1:])
        found = jnp.stack([found[c] for c in ring_order])
        for axis in range(3):
            found = turn(found, axis, True)
        for axis in (2, 1, 0):
            entries = [lax.index_in_dim(found, k, axis, False) for k in range(found.shape[axis])]
            found = ring_scatter(entries, tiny_rings[axis], f32)
        return found[:count, :shard]

    packed = jnp.stack([gain_attn_in, gain_attn_out, gain_ffn_in, gain_ffn_out])
    packed = jnp.pad(packed, ((0, 4), (0, -shard % 128)))
    tok_group, col_qkv, col_out, gains, ffn_gate = fetch_weights(
        plan, tokens, w_query, w_key, w_value, w_out, packed.astype(f32), w_gate
    )
    tok_group = tok_group.reshape(group_rows, width)
    col_qkv = col_qkv.reshape(width, -1)
    col_out = col_out.reshape(width, -1)
    gains = jnp.transpose(gains[:, :4, :shard], (1, 0, 2)).reshape(4, width)
    weight_one, weight_two, weight_three, weight_four = (1.0 + gains[k][None] for k in range(4))

    own_spans = lax.dynamic_slice_in_dim(span_order, 2 * ctx, 2, 0) * span
    boundary = jnp.sum((segments == 0).astype(jnp.int32)).reshape(1)
    key_spans = span_order * span
    group_pos = (own_spans[:, None] + jnp.arange(span, dtype=jnp.int32)[None, :]).reshape(-1)
    half = HEAD_DIM // 2
    freqs = rotary_base ** (-jnp.arange(half).astype(f32) / half)
    angles = group_pos.astype(f32)[:, None] * freqs[None, :]
    cosines, sines = jnp.cos(angles), jnp.sin(angles)

    q_cols, k_cols = w_query.shape[1] // ulysses, w_key.shape[1] // ulysses
    tok_rows = tok_group.astype(f32)
    normed_in = norm_apply(tok_rows, weight_one).astype(bf16)
    qkv = dot(normed_in, col_qkv)
    queries = (rotary(qkv[:, :q_cols], cosines, sines, 1.0) * q_scale).astype(bf16)
    keys = rotary(qkv[:, q_cols : q_cols + k_cols], cosines, sines, 1.0).astype(bf16)
    values = qkv[:, q_cols + k_cols :].astype(bf16)
    kv, ffn_up = fetch_keys(plan, jnp.concatenate([keys, values], axis=1), w_up)
    kv = kv.reshape(contexts * group_rows, -1)
    ffn_gate, ffn_up = ffn_gate.reshape(width, -1), ffn_up.reshape(width, -1)

    slice_cols = w_gate.shape[1] // halves

    def slice_perm(p):
        return plan.perm(lambda l, s, r, c: (c * halves + (l + p) % halves, s, r, l // halves))

    def slice_back(p):
        return [(b, a) for a, b in slice_perm(p)]

    def pick(options, index):
        out = options[0]
        for k in range(1, len(options)):
            out = jnp.where(index == k, options[k], out)
        return out

    def slice_fetch(weights):
        cuts = [weights[:, h * slice_cols : (h + 1) * slice_cols] for h in range(halves)]
        size = weights.shape[0]
        got = [move(pick(cuts, (layer + p) % halves), slice_perm(p)) for p in range(halves)]
        sided = ring_gather(jnp.concatenate(got, axis=0), side_ring)
        cored = ring_gather(jnp.concatenate(sided, axis=0), core_ring)
        blocks, where = [], []
        for m, found in enumerate(cored):
            for k in range(sides):
                for p in range(halves):
                    n = k * halves + p
                    blocks.append(found[n * size : (n + 1) * size])
                    origin = (core + m) % cores * halves + (layer - p) % halves
                    where.append(origin * sides + (side + k) % sides)
        return place_rows(blocks, where, contexts).reshape(width, slice_cols)

    def slice_start(grad):
        parts = grad.reshape(cores, halves, sides, -1, slice_cols)
        size = parts.shape[3]
        others = []
        for m in range(1, cores):
            at = ((core + m) % cores, 0, 0, 0, 0)
            piece = lax.dynamic_slice(parts, at, (1, *parts.shape[1:]))[0]
            perm = plan.perm(lambda l, s, r, c, m=m: (l, s, r, (c + m) % cores))
            others.append(move(piece, perm))

        def side_part(k):
            here = (side + k) % sides
            shape = (halves, 1, size, slice_cols)
            found = lax.dynamic_slice(parts, (core, 0, here, 0, 0), (1, *shape))[0].astype(f32)
            for other in others:
                found = found + lax.dynamic_slice(other, (0, here, 0, 0), shape).astype(f32)
            return found.reshape(halves * size, slice_cols)

        sent = [side_part(k).astype(bf16) for k in range(1, sides)]
        summed = ring_scatter([side_part(0), *sent], side_ring, bf16)
        return summed.astype(bf16).reshape(halves, size, slice_cols)

    def slice_end(summed):
        got = []
        for p in range(halves):
            piece = lax.dynamic_index_in_dim(summed, (layer - p) % halves, 0, keepdims=False)
            got.append(move(piece, slice_back(p)))
        cuts = [pick(got, (h - layer) % halves) for h in range(halves)]
        return jnp.concatenate(cuts, axis=1).astype(f32)

    ffn_down = slice_fetch(after(w_down, kv))
    head_o, lse = attend(queries, kv, own_spans, key_spans, boundary, span)
    attn_out = group_scatter(dot(head_o, col_out, 1, 1))
    tok_own = tokens.astype(f32)
    hidden_in = tok_own + norm_apply(attn_out, weight_two)
    normed_own = norm_apply(hidden_in, weight_three).astype(bf16)

    size = ffn_ring.size
    order = [0]
    for k in range(1, size // 2):
        order += [k, size - k]
    order.append(size // 2)
    near = max(size - 3, 1)

    def ffn_gather(values):
        found = ring_gather(values, ffn_ring)
        return [
            jnp.concatenate([found[k] for k in ks], axis=0) for ks in (order[:near], order[near:])
        ]

    def ffn_scatter(chunk):
        parts = [None] * size
        far = chunk(1, None)
        for values, ks in ((far, order[near:]), (chunk(0, far), order[:near])):
            for n, k in enumerate(ks):
                parts[k] = values[n * rows : (n + 1) * rows]
        landed = []
        return ring_scatter(parts, ffn_ring, bf16, landed), landed

    normed_mid = ffn_gather(normed_own)
    gate = [dot(x, ffn_gate) for x in normed_mid]
    upper = [dot(x, ffn_up) for x in normed_mid]
    hidden = [(gelu_parts(g)[0] * u).astype(bf16) for g, u in zip(gate, upper, strict=True)]

    def down_part(n, far):
        rows_in = hidden[n] if far is None else after(hidden[n], far)
        return dot(rows_in, ffn_down, 1, 1)

    ffn_out, _ = ffn_scatter(down_part)
    block_out = (hidden_in + norm_apply(ffn_out, weight_four)).astype(bf16)
    cot_own = cotangent.astype(f32)
    d_ffn = ffn_gather(norm_grad(ffn_out, weight_four, cot_own).astype(bf16))
    d_gate, d_upper = [], []
    for n in range(2):
        d_hidden = dot(d_ffn[n], ffn_down)
        gate_value, gate_slope = gelu_parts(gate[n])
        d_gate.append((d_hidden * upper[n] * gate_slope).astype(bf16))
        d_upper.append((d_hidden * gate_value).astype(bf16))

    def mid_part(n, far):
        left, right = d_gate[n], d_upper[n]
        if far is not None:
            left, right = after(left, far), after(right, far)
        return dot(left, ffn_gate, 1, 1) + dot(right, ffn_up, 1, 1)

    d_mid, landed = ffn_scatter(mid_part)
    grad_hidden = cot_own + norm_grad(hidden_in, weight_three, d_mid)
    joined = [jnp.concatenate(x, axis=0) for x in (d_ffn, hidden, normed_mid, d_gate, d_upper)]

    def weight_grad(left, right, earlier):
        left = after(left, earlier)
        grad = dot(left, right, 0, 0).astype(bf16)
        return slice_start(grad)

    sum_down = weight_grad(joined[0], joined[1], landed[0])
    sum_gate = weight_grad(joined[2], joined[3], landed[min(1, len(landed) - 1)])
    sum_up = weight_grad(joined[2], joined[4], d_mid)
    grad_down = slice_end(after(sum_down, d_mid))
    grad_gate = slice_end(after(sum_gate, d_mid))

    d_attn = group_gather(norm_grad(attn_out, weight_two, grad_hidden).astype(bf16))
    out_part = dot(d_attn, head_o, 0, 0).astype(bf16)
    grad_o = dot(d_attn, col_out).astype(bf16)
    products = grad_o.astype(f32) * head_o.astype(f32)
    dsum = jnp.concatenate(
        [
            jnp.broadcast_to(
                jnp.sum(products[:, s : s + HEAD_DIM], axis=1, keepdims=True), (group_rows, 128)
            )
            for s in range(0, q_cols, HEAD_DIM)
        ],
        axis=1,
    )
    grad_q, grad_kv = attend_back(
        queries, grad_o, lse, dsum, kv, own_spans, key_spans, boundary, span
    )
    grad_kv = ctx_scatter([grad_kv])
    grad_up = slice_end(after(sum_up, grad_q))
    grad_q = (rotary(grad_q, cosines, sines, -1.0) * q_scale).astype(bf16)
    grad_k = rotary(grad_kv[:, :k_cols], cosines, sines, -1.0).astype(bf16)
    grad_v = grad_kv[:, k_cols:].astype(bf16)
    grad_kv = jnp.concatenate([grad_k, grad_v], axis=1)
    q_part = dot(normed_in, grad_q, 0, 0).astype(bf16)
    kv_part = dot(normed_in, grad_kv, 0, 0).astype(bf16)
    d_in_part = dot(grad_q, col_qkv[:, :q_cols], 1, 1) + dot(grad_kv, col_qkv[:, q_cols:], 1, 1)
    d_in = group_scatter(d_in_part)
    grad_tokens = grad_hidden + norm_grad(tok_own, weight_one, d_in)
    first_grad = ctx_scatter([q_part, out_part])
    second_grad = ctx_scatter([kv_part])
    grad_outproj = first_grad[:, q_cols:]
    mixed_grad = jnp.concatenate([first_grad[:, :q_cols], second_grad], axis=1).astype(bf16)
    mixed_grad = lax.all_to_all(
        mixed_grad.reshape(ulysses, -1, mixed_grad.shape[1]),
        "uly",
        split_axis=0,
        concat_axis=0,
        tiled=True,
    )
    mixed_grad = jnp.transpose(mixed_grad, (1, 0, 2)).astype(f32)
    grad_query = mixed_grad[:, :, :q_cols].reshape(w_query.shape)
    grad_key = mixed_grad[:, :, q_cols : q_cols + k_cols].reshape(w_key.shape)
    grad_value = mixed_grad[:, :, q_cols + k_cols :].reshape(w_value.shape)

    gain_grads = sum_gains(
        jnp.stack(
            [
                gain_part(attn_out, after(grad_hidden, grad_q)),
                gain_part(hidden_in, after(d_mid, grad_q)),
                gain_part(ffn_out, after(cot_own, grad_q)),
            ]
        )
    )
    products = [
        jnp.sum(w.astype(f32) * g, axis=1)
        for w, g in ((w_query, grad_query), (w_key, grad_key), (w_value, grad_value))
    ]
    gain_first = (products[0] + products[1] + products[2]) / (1.0 + gain_attn_in.astype(f32))
    return (
        block_out,
        grad_tokens,
        grad_query,
        grad_key,
        grad_value,
        grad_outproj,
        grad_gate,
        grad_up,
        grad_down,
        gain_first,
        gain_grads[0],
        gain_grads[1],
        gain_grads[2],
    )


def solution(mesh):
    flat, cut, line = P(AXES, None), P("ctx", "uly"), P(AXES)
    in_specs = (flat, flat, P(), P(), flat, flat, flat, cut, cut, cut, cut, line, line, line, line)
    out_specs = (flat, flat, flat, flat, flat, cut, cut, cut, cut, line, line, line, line)
    plan = Plan(mesh)

    def body(*args):
        return on_device(plan, *args)

    return jax.shard_map(
        body, mesh=mesh, in_specs=in_specs, out_specs=out_specs, check_vma=False
    )
```

```python
import functools

import jax
import jax.numpy as jnp
from jax import lax
from jax.experimental import pallas as pl
from jax.experimental.pallas import tpu as pltpu
from jax.sharding import PartitionSpec as P


HEAD_DIM = 256
AXES = ("ctx", "uly")

norm_eps = 1e-06
soft_cap = 50.0
rotary_base = 10000.0
gelu_coef = 0.7978845608028654
cubic_coef = 0.044715


bf16 = jnp.bfloat16
f32 = jnp.float32


def rms_scale(values):
    return lax.rsqrt(jnp.mean(values * values, axis=-1, keepdims=True) + norm_eps)


def norm_apply(values, weight):
    return values * rms_scale(values) * weight


def norm_grad(values, weight, grad):
    scale = rms_scale(values)
    inner = jnp.mean(grad * weight * values, axis=-1, keepdims=True)
    return scale * weight * grad - values * (scale * scale * scale) * inner


def gain_part(values, grad):
    return jnp.sum(grad * values * rms_scale(values), axis=0)


def gelu_parts(values):
    inner = gelu_coef * (values + cubic_coef * values * values * values)
    tanh_part = jnp.tanh(inner)
    value = 0.5 * values * (1.0 + tanh_part)
    slope = 0.5 * (1.0 + tanh_part) + 0.5 * values * (1.0 - tanh_part * tanh_part) * gelu_coef * (
        1.0 + 3.0 * cubic_coef * values * values
    )
    return value, slope


def rotary(values, cosines, sines, sign):
    half = HEAD_DIM // 2
    parts = []
    for start in range(0, values.shape[1], HEAD_DIM):
        first = values[:, start : start + half]
        second = values[:, start + half : start + HEAD_DIM]
        parts.append(first * cosines - sign * second * sines)
        parts.append(second * cosines + sign * first * sines)
    return jnp.concatenate(parts, axis=1)


def dot(left, right, left_dim=1, right_dim=0):
    return lax.dot_general(
        left, right, (((left_dim,), (right_dim,)), ((), ())), preferred_element_type=f32
    )


class Plan:
    def __init__(self, mesh):
        grid = mesh.devices
        self.contexts, self.ulysses = mesh.shape["ctx"], mesh.shape["uly"]
        self.cores = sum(tuple(d.coords) == tuple(grid[0, 0].coords) for d in grid[0])
        self.layers = len({d.coords[2] for d in grid[:, 0]})
        self.sides = self.contexts // self.layers
        self.rows = self.ulysses // self.cores
        self.halves = self.layers // self.cores

    def split(self, device):
        ctx, uly = divmod(device, self.ulysses)
        return (*divmod(ctx, self.sides), *divmod(uly, self.cores))

    def join(self, layer, side, row, core):
        return (layer * self.sides + side) * self.ulysses + row * self.cores + core

    def perm(self, target):
        count = self.contexts * self.ulysses
        return [(d, self.join(*target(*self.split(d)))) for d in range(count)]

    def here(self):
        layer, side = jnp.divmod(lax.axis_index("ctx"), self.sides)
        row, core = jnp.divmod(lax.axis_index("uly"), self.cores)
        return layer, side, row, core


class Ring:
    def __init__(self, plan, outer, inner, place, locate):
        self.size = outer * inner
        self.inner = inner

        def cell(index):
            out, rest = divmod(index % self.size, inner)
            return out, (rest if out % 2 == 0 else inner - 1 - rest)

        def index_of(out, inn):
            return out * inner + (inn if out % 2 == 0 else inner - 1 - inn)

        self.cells = [cell(i) for i in range(self.size)]

        def shifted(step):
            def target(*where):
                return place(where, *cell(index_of(*locate(where)) + step))

            return plan.perm(target)

        self.ahead, self.behind = shifted(1), shifted(-1)

    def position(self, out, inn):
        rest = jnp.where(out % 2 == 0, inn, self.inner - 1 - inn)
        return out * self.inner + rest


def move(values, perm):
    return lax.ppermute(values, AXES, perm)


def both(*values):
    return lax.optimization_barrier(values)


def after(values, *earlier):
    return lax.optimization_barrier((values, *earlier))[0]


def ring_gather(block, ring):
    size = ring.size
    found = {0: block}
    if size == 2:
        found[1] = move(block, ring.ahead)
        return [found[0], found[1]]
    forth = back = block
    middle = size // 2
    for step in range(1, middle):
        forth = move(forth, ring.ahead)
        back = move(back, ring.behind)
        forth, back = both(forth, back)
        found[size - step], found[step] = forth, back
    cut = block.shape[0] // 2
    forth = move(forth[:cut], ring.ahead)
    back = move(back[cut:], ring.behind)
    found[middle] = jnp.concatenate([forth, back], axis=0)
    return [found[k] for k in range(size)]


def ring_scatter(parts, ring, kind=bf16, landed=None):
    size = ring.size
    if size == 2:
        return parts[0].astype(f32) + move(parts[1].astype(kind), ring.ahead).astype(f32)
    middle = size // 2
    cut = parts[0].shape[0] // 2
    forth = move(parts[middle][:cut].astype(kind), ring.ahead)
    back = move(parts[middle][cut:].astype(kind), ring.behind)
    forth, back = both(forth, back)
    landed = [] if landed is None else landed
    for left in range(middle - 1, 0, -1):
        landed.append(forth)
        fore, aft = parts[left].astype(f32), parts[size - left].astype(f32)
        if left == middle - 1:
            fore = jnp.concatenate([fore[:cut] + forth.astype(f32), fore[cut:]], axis=0)
            aft = jnp.concatenate([aft[:cut], aft[cut:] + back.astype(f32)], axis=0)
        else:
            fore, aft = fore + forth.astype(f32), aft + back.astype(f32)
        forth = move(fore.astype(kind), ring.ahead)
        back = move(aft.astype(kind), ring.behind)
        forth, back = both(forth, back)
    return parts[0].astype(f32) + forth.astype(f32) + back.astype(f32)


def place_rows(blocks, indices, count):
    first = blocks[0]
    out = jnp.zeros((count, *first.shape), first.dtype)
    for block, index in zip(blocks, indices, strict=True):
        out = lax.dynamic_update_slice(out, block[None], (index, *(0,) * first.ndim))
    return out


def take_block(values, index, size):
    return lax.dynamic_slice_in_dim(values, index * size, size, 0)


class Sender:
    def __init__(self, plan, send, recv):
        self.plan, self.send, self.recv, self.sent = plan, send, recv, []
        self.ctx, self.uly = lax.axis_index("ctx"), lax.axis_index("uly")
        self.layer, self.side = self.ctx // plan.sides, self.ctx % plan.sides
        self.row, self.core = self.uly // plan.cores, self.uly % plan.cores
        flip = self.side % 2
        self.here = self.side * plan.layers + (
            self.layer * (1 - flip) + (plan.layers - 1 - self.layer) * flip
        )

    def at(self, layer, side, row, core):
        plan = self.plan
        return {"ctx": layer * plan.sides + side, "uly": row * plan.cores + core}

    def group(self):
        plan = self.plan
        for dr in range(plan.rows - 1, -1, -1):
            for dc in range(plan.cores):
                if (dr, dc) != (0, 0):
                    row, core = (self.row + dr) % plan.rows, (self.core + dc) % plan.cores
                    yield self.at(self.layer, self.side, row, core), row * plan.cores + core

    def meet(self):
        plan = self.plan
        friends = [friend for friend, _ in self.group()]
        for dl in range(1, plan.layers):
            for dc in range(plan.cores):
                layer, core = (self.layer + dl) % plan.layers, (self.core + dc) % plan.cores
                friends.append(self.at(layer, self.side, self.row, core))
        for ds in sorted({1 % plan.sides, plan.sides - 1} - {0}):
            side = (self.side + ds) % plan.sides
            friends.append(self.at(self.layer, side, self.row, self.core))
        barrier = pltpu.get_barrier_semaphore()
        for friend in friends:
            pl.semaphore_signal(
                barrier, inc=1, device_id=friend, device_id_type=pl.DeviceIdType.MESH
            )
        pl.semaphore_wait(barrier, len(friends))

    def push(self, source, target, device):
        k = len(self.sent)
        copy = pltpu.make_async_remote_copy(
            source,
            target,
            self.send.at[k],
            self.recv.at[k],
            device_id=device,
            device_id_type=pl.DeviceIdType.MESH,
        )
        copy.start()
        self.sent.append(copy)
        return copy

    def finish(self):
        for copy in self.sent:
            copy.wait_send()

    def spot(self, index):
        plan = self.plan
        out, low = index // plan.layers, index % plan.layers
        flip = out % 2
        return (low * (1 - flip) + (plan.layers - 1 - low) * flip) * plan.sides + out

    def ring(self, piece, cut, own=None):
        count = self.plan.contexts
        middle = count // 2
        ahead = {"ctx": self.spot((self.here + 1) % count), "uly": self.uly}
        behind = {"ctx": self.spot((self.here + count - 1) % count), "uly": self.uly}
        last = ()
        for step in range(middle):
            for copy in last:
                copy.wait_recv()
            fore = piece(self.spot((self.here + count - step) % count))
            aft = piece(self.spot((self.here + step) % count))
            first, second = (fore, aft) if step or own is None else (own, own)
            if step == middle - 1:
                fore, first = fore.at[:cut], first.at[:cut]
                aft, second = aft.at[cut:], second.at[cut:]
            last = (self.push(first, fore, ahead), self.push(second, aft, behind))
            yield
        for copy in last:
            copy.wait_recv()

    def slice_send(self, matrix, result, p):
        plan = self.plan
        h = (self.layer + p) % plan.halves
        target = self.at(
            self.core * plan.halves + h,
            self.side,
            self.row,
            plan.cores - 1 - self.layer // plan.halves,
        )
        width = matrix.shape[1] // plan.halves
        cols = pl.ds(pl.multiple_of(h * width, 128), width)
        return self.push(matrix.at[:, cols], result.at[self.ctx], target)

    def slice_pass(self, result, p, held):
        plan = self.plan
        origin = (plan.cores - 1 - self.core) * plan.halves
        origin = origin + (self.layer - p + plan.halves) % plan.halves
        passed = []
        for step in range(plan.sides):
            held.wait_recv()
            slot = result.at[origin * plan.sides + (self.side - step + plan.sides) % plan.sides]
            for dc in range(1, plan.cores):
                core = (self.core + dc) % plan.cores
                passed.append(self.push(slot, slot, self.at(self.layer, self.side, self.row, core)))
            if step < plan.sides - 1:
                side = (self.side + 1) % plan.sides
                held = self.push(slot, slot, self.at(self.layer, side, self.row, self.core))
            yield
        for copy in passed:
            copy.wait_recv()

    def run(self, rings, slices):
        flying, moving = [], []
        tasks = [(m, r, p) for m, r in slices for p in range(self.plan.halves)]

        def drive(generators):
            return [g for g in generators if next(g, "end") != "end"]

        while rings or tasks or flying or moving:
            rings = drive(rings)
            if flying:
                moving.append(self.slice_pass(*flying.pop(0)))
            if tasks:
                matrix, result, p = tasks.pop(0)
                flying.append((result, p, self.slice_send(matrix, result, p)))
            moving = drive(moving)


def copies_of(plan, slices):
    return slices * plan.halves * (1 + plan.sides - 1 + plan.sides * (plan.cores - 1))


def weights_kernel(plan, *refs):
    tok_in, wq, wk, wv, out_in, gain_in, gate_in = refs[:7]
    tok_all, qkv, out_all, gain_all, gate_all = refs[7:12]
    tok_tmp, qkv_tmp, out_tmp, gain_tmp, local, send, recv = refs[12:]
    link = Sender(plan, send, recv)
    link.meet()
    ulysses, ctx, uly = plan.ulysses, link.ctx, link.uly
    q_cols, k_cols = wq.shape[1] // ulysses, wk.shape[1] // ulysses

    def parts(u):
        yield wq.at[:, pl.ds(pl.multiple_of(u * q_cols, 128), q_cols)], pl.ds(0, q_cols)
        for k, matrix in enumerate((wk, wv)):
            cols = pl.ds(pl.multiple_of(u * k_cols, 128), k_cols)
            yield matrix.at[:, cols], pl.ds(q_cols + k * k_cols, k_cols)

    pairs = [(src, qkv_tmp.at[:, cols]) for src, cols in parts(uly)]
    pairs += [(gain_in, gain_tmp), (out_in, out_tmp), (tok_in, tok_tmp)]
    pulls = [pltpu.make_async_copy(*pair, local.at[k]) for k, pair in enumerate(pairs)]
    for pull in pulls:
        pull.start()
    place = ctx * ulysses + uly
    first = []
    for friend, u in link.group():
        for source, cols in parts(u):
            first.append(link.push(source, qkv.at[place, :, cols], friend))
        first.append(link.push(gain_in, gain_all.at[place], friend))
    for pull in pulls:
        pull.wait()
    pairs = [
        (qkv_tmp, qkv.at[place]),
        (gain_tmp, gain_all.at[place]),
        (out_tmp, out_all.at[ctx]),
        (tok_tmp, tok_all.at[uly]),
    ]
    puts = [pltpu.make_async_copy(*pair, local.at[6 + k]) for k, pair in enumerate(pairs)]
    for put in puts:
        put.start()
    for put in puts:
        put.wait()
    for copy in first:
        copy.wait_recv()
    tokens = [link.push(tok_in, tok_all.at[uly], friend) for friend, _ in link.group()]

    def block(array):
        return lambda c: array.at[pl.ds(c * ulysses, ulysses)]

    rings = [
        link.ring(block(qkv), ulysses // 2),
        link.ring(block(gain_all), ulysses // 2),
        link.ring(lambda c: out_all.at[c], out_all.shape[1] // 16 * 8),
    ]
    link.run(rings, [(gate_in, gate_all)])
    for copy in tokens:
        copy.wait_recv()
    link.finish()


anywhere = pl.BlockSpec(memory_space=pl.ANY)


def sliced(plan, weights):
    shape = (plan.contexts, weights.shape[0], weights.shape[1] // plan.halves)
    return jax.ShapeDtypeStruct(shape, weights.dtype)


def fetch_weights(plan, tokens, wq, wk, wv, w_out, gains, w_gate):
    shard, contexts, ulysses = wq.shape[0], plan.contexts, plan.ulysses
    cols = (wq.shape[1] + wk.shape[1] + wv.shape[1]) // ulysses
    results = [
        jax.ShapeDtypeStruct((ulysses, *tokens.shape), tokens.dtype),
        jax.ShapeDtypeStruct((contexts * ulysses, shard, cols), wq.dtype),
        jax.ShapeDtypeStruct((contexts, *w_out.shape), w_out.dtype),
        jax.ShapeDtypeStruct((contexts * ulysses, *gains.shape), gains.dtype),
        sliced(plan, w_gate),
    ]
    copies = 5 * (ulysses - 1) + 3 * contexts + copies_of(plan, 1)
    return pl.pallas_call(
        functools.partial(weights_kernel, plan),
        out_shape=results,
        in_specs=[anywhere] * 7,
        out_specs=[anywhere] * len(results),
        scratch_shapes=[
            pltpu.VMEM(tokens.shape, tokens.dtype),
            pltpu.VMEM((shard, cols), wq.dtype),
            pltpu.VMEM(w_out.shape, w_out.dtype),
            pltpu.VMEM(gains.shape, gains.dtype),
            pltpu.SemaphoreType.DMA((10,)),
            pltpu.SemaphoreType.DMA((copies,)),
            pltpu.SemaphoreType.DMA((copies,)),
        ],
        compiler_params=pltpu.CompilerParams(collective_id=1, has_side_effects=True),
    )(tokens, wq, wk, wv, w_out, gains, w_gate)


def keys_kernel(plan, kv_in, up_in, kv_all, up_all, tmp, local, send, recv):
    link = Sender(plan, send, recv)
    link.meet()
    pull = pltpu.make_async_copy(kv_in, tmp, local.at[0])
    put = pltpu.make_async_copy(tmp, kv_all.at[link.ctx], local.at[1])
    pull.start()
    pull.wait()
    put.start()
    ring = link.ring(lambda c: kv_all.at[c], kv_in.shape[0] // 2, kv_in)
    link.run([ring], [(up_in, up_all)])
    put.wait()
    link.finish()


def fetch_keys(plan, kv, w_up):
    copies = plan.contexts + copies_of(plan, 1)
    return pl.pallas_call(
        functools.partial(keys_kernel, plan),
        out_shape=[
            jax.ShapeDtypeStruct((plan.contexts, *kv.shape), kv.dtype),
            sliced(plan, w_up),
        ],
        in_specs=[anywhere] * 2,
        out_specs=[anywhere] * 2,
        scratch_shapes=[
            pltpu.VMEM(kv.shape, kv.dtype),
            pltpu.SemaphoreType.DMA((2,)),
            pltpu.SemaphoreType.DMA((copies,)),
            pltpu.SemaphoreType.DMA((copies,)),
        ],
        compiler_params=pltpu.CompilerParams(collective_id=2, has_side_effects=True),
    )(kv, w_up)


def grads_kernel(plan, q_in, kv_in, out_in, rows_in, gain_in, *refs):
    parts = (q_in, kv_in, out_in)
    lows = (0, q_in.shape[2], q_in.shape[2] + kv_in.shape[2])
    query_out, key_out, value_out, out_out, rows_out, gain_out = refs[:6]
    main_send, main_recv, gain_send, gain_recv, turn_send, turn_recv, gain_last, gain_turn = refs[6:14]
    core_recv, row_send, row_recv, send, recv = refs[14:]
    link = Sender(plan, send, recv)
    count, ulysses, cores = plan.contexts, plan.ulysses, plan.cores
    middle = count // 2
    ctx, uly = link.ctx, link.uly
    ahead = {"ctx": link.spot((link.here + 1) % count), "uly": uly}
    behind = {"ctx": link.spot((link.here + count - 1) % count), "uly": uly}
    link.meet()

    half = max(ulysses // 2, 1)
    lanes = [range(half), range(half, ulysses)]

    def pass_on(step, way, lane):
        left = middle - step
        there = link.spot((link.here + (left if way == 0 else count - left)) % count)
        received = step > 1 or (step == 1 and lane == way)
        for m in lanes[lane]:
            place = there * ulysses + m
            gain = gain_in[place]
            for array, low in zip(parts, lows, strict=True):
                high = low + array.shape[2]
                block = array[place]
                if received:
                    block = block.astype(f32) + main_recv[step - 1, way, m, :, low:high].astype(f32)
                main_send[step, way, m, :, low:high] = block.astype(bf16)
            gain_send[step, way, m] = gain + gain_recv[step - 1, way, m] if received else gain
        device = ahead if way == 0 else behind
        rows = pl.ds(lanes[lane][0], len(lanes[lane]))
        return [
            link.push(main_send.at[step, way, rows], main_recv.at[step, way, rows], device),
            link.push(gain_send.at[step, way, rows], gain_recv.at[step, way, rows], device),
        ]

    last = {}
    core_copies, row_copies = [], []
    for step in range(middle):
        sent = {}
        for lane in range(2):
            for way in range(2):
                for copy in last.get((lane, way), ()):
                    copy.wait_recv()
                if step or lane == way:
                    sent[lane, way] = pass_on(step, way, lane)
        last = sent
        if step == 0:
            for dc in range(1, cores):
                core = (link.core + dc) % cores
                for r in range(plan.rows):
                    device = link.at(link.layer, link.side, link.row, core)
                    source = rows_in.at[r * cores + core]
                    core_copies.append(link.push(source, core_recv.at[dc - 1, r], device))
        if step == min(1, middle - 1):
            for copy in core_copies:
                copy.wait_recv()

            def total(r):
                found = rows_in[r * cores + link.core].astype(f32)
                for dc in range(1, cores):
                    found = found + core_recv[dc - 1, r].astype(f32)
                return found

            for dr in range(1, plan.rows):
                row_send[dr - 1] = total((link.row + dr) % plan.rows).astype(bf16)
            rows_out[...] = total(link.row)
            for dr in range(1, plan.rows):
                device = link.at(link.layer, link.side, (link.row + dr) % plan.rows, link.core)
                row_copies.append(link.push(row_send.at[dr - 1], row_recv.at[dr - 1], device))
    for copies in last.values():
        for copy in copies:
            copy.wait_recv()
    place = ctx * ulysses

    def finish(m, array, received, low):
        high = low + array.shape[2]
        found = array[place + m].astype(f32)
        if middle > 1:
            return found + received[middle - 1, 0, m, :, low:high].astype(f32) + received[
                middle - 1, 1, m, :, low:high
            ].astype(f32)
        way = 0 if m < ulysses // 2 else 1
        return found + received[0, way, m, :, low:high].astype(f32)

    for m in range(ulysses):
        turn_send[m, :, : lows[1]] = finish(m, q_in, main_recv, 0).astype(bf16)
        turn_send[m, :, lows[1] :] = finish(m, kv_in, main_recv, lows[1]).astype(bf16)
        gain_last[m] = finish(m, gain_in, gain_recv, 0)
    turn_recv[uly] = turn_send[uly]
    gain_turn[uly] = gain_last[uly]
    turned = []
    for friend, u in link.group():
        turned.append(link.push(turn_send.at[u], turn_recv.at[uly], friend))
        turned.append(link.push(gain_last.at[u], gain_turn.at[uly], friend))
    for m in range(ulysses):
        out_out[m] = finish(m, out_in, main_recv, lows[2])
    for dr, copy in enumerate(row_copies):
        copy.wait_recv()
        rows_out[...] += row_recv[dr].astype(f32)
    for copy in turned:
        copy.wait_recv()
    q_cols, k_cols = query_out.shape[1] // ulysses, key_out.shape[1] // ulysses
    for u in range(ulysses):
        query_out[:, u * q_cols : (u + 1) * q_cols] = turn_recv[u, :, :q_cols].astype(f32)
        cols = slice(u * k_cols, (u + 1) * k_cols)
        key_out[:, cols] = turn_recv[u, :, q_cols : q_cols + k_cols].astype(f32)
        value_out[:, cols] = turn_recv[u, :, q_cols + k_cols :].astype(f32)
    gain_out[...] = gain_turn[0]
    for u in range(1, ulysses):
        gain_out[...] += gain_turn[u]
    link.finish()


def sum_grads(plan, q, kv, out, rows, gains, q_width, k_width):
    contexts, ulysses = plan.contexts, plan.ulysses
    shard = q.shape[1]
    turned = (ulysses, shard, q.shape[2] + kv.shape[2])
    middle, tail = contexts // 2, gains.shape[1:]
    wide = (shard, turned[2] + out.shape[2])
    block = rows.shape[1:]
    results = [
        jax.ShapeDtypeStruct((shard, q_width), f32),
        jax.ShapeDtypeStruct((shard, k_width), f32),
        jax.ShapeDtypeStruct((shard, k_width), f32),
        jax.ShapeDtypeStruct((ulysses, *out.shape[1:]), f32),
        jax.ShapeDtypeStruct(block, f32),
        jax.ShapeDtypeStruct(tail, f32),
    ]
    copies = 8 * middle + (plan.cores - 1) * plan.rows + plan.rows - 1 + 2 * (ulysses - 1)
    local = pl.BlockSpec(memory_space=pltpu.VMEM)
    return pl.pallas_call(
        functools.partial(grads_kernel, plan),
        out_shape=results,
        in_specs=[local] * 5,
        out_specs=[local] * len(results),
        scratch_shapes=[
            pltpu.VMEM((middle, 2, ulysses, *wide), bf16),
            pltpu.VMEM((middle, 2, ulysses, *wide), bf16),
            pltpu.VMEM((middle, 2, ulysses, *tail), f32),
            pltpu.VMEM((middle, 2, ulysses, *tail), f32),
            pltpu.VMEM(turned, bf16),
            pltpu.VMEM(turned, bf16),
            pltpu.VMEM((ulysses, *tail), f32),
            pltpu.VMEM((ulysses, *tail), f32),
            pltpu.VMEM((max(plan.cores - 1, 1), plan.rows, *block), bf16),
            pltpu.VMEM((max(plan.rows - 1, 1), *block), bf16),
            pltpu.VMEM((max(plan.rows - 1, 1), *block), bf16),
            pltpu.SemaphoreType.DMA((copies,)),
            pltpu.SemaphoreType.DMA((copies,)),
        ],
        compiler_params=pltpu.CompilerParams(collective_id=3, has_side_effects=True),
    )(q, kv, out, rows, gains)


def visible(q_first, k_first, boundary, span):
    q_pos = q_first + lax.broadcasted_iota(jnp.int32, (span, span), 0)
    k_pos = k_first + lax.broadcasted_iota(jnp.int32, (span, span), 1)
    low = jnp.where(q_pos >= boundary, boundary, 0)
    return (k_pos <= q_pos) & (k_pos >= low)


def active(q_first, k_first, boundary, span):
    split = (q_first >= boundary) & (k_first + span <= boundary)
    return (k_first <= q_first) & jnp.logical_not(split)


def whole(q_first, k_first, boundary, span):
    same = (k_first >= boundary) | (q_first + span <= boundary)
    return (k_first + span <= q_first) & same


def over_pairs(span, blocks, chunk, qp, kp, bd, work):
    start = pl.program_id(0) * chunk

    def pair(t, carry):
        i, j = t % blocks, t // blocks
        q_first, k_first, boundary = qp[i], kp[start + j], bd[0]
        q_rows = pl.ds(pl.multiple_of(i * span, span), span)
        k_rows = pl.ds(pl.multiple_of(j * span, span), span)
        full = whole(q_first, k_first, boundary, span)

        @pl.when(full)
        def _():
            work(q_rows, k_rows, None)

        @pl.when(active(q_first, k_first, boundary, span) & jnp.logical_not(full))
        def _():
            work(q_rows, k_rows, visible(q_first, k_first, boundary, span))

        return carry

    lax.fori_loop(0, blocks * chunk, pair, 0)


def attend_kernel(span, repeat, steps, chunk, qp, kp, bd, q_ref, kv_ref, o_ref, lse_ref, acc, den):
    step = pl.program_id(0)

    @pl.when(step == 0)
    def _():
        acc[...] = jnp.zeros_like(acc)
        den[...] = jnp.zeros_like(den)

    def work(q_rows, k_rows, allowed):
        keys, values = kv_ref[k_rows, :HEAD_DIM], kv_ref[k_rows, HEAD_DIM:]
        for r in range(repeat):
            cols = slice(r * HEAD_DIM, (r + 1) * HEAD_DIM)
            scores = dot(q_ref[q_rows, cols], keys, 1, 1)
            weights = jnp.exp(soft_cap * jnp.tanh(scores * (1.0 / soft_cap)))
            if allowed is not None:
                weights = jnp.where(allowed, weights, 0.0)
            folded = weights[:, :128]
            for k in range(128, span, 128):
                folded = folded + weights[:, k : k + 128]
            den[q_rows, r * 128 : (r + 1) * 128] += folded
            acc[q_rows, cols] += dot(weights.astype(bf16), values)

    over_pairs(span, q_ref.shape[0] // span, chunk, qp, kp, bd, work)

    @pl.when(step == steps - 1)
    def _():
        for r in range(repeat):
            cols, lanes = slice(r * HEAD_DIM, (r + 1) * HEAD_DIM), slice(r * 128, (r + 1) * 128)
            total = jnp.sum(den[:, lanes], axis=1, keepdims=True)
            o_ref[:, cols] = (acc[:, cols] / total).astype(bf16)
            lse_ref[:, lanes] = jnp.broadcast_to(jnp.log(total), den[:, lanes].shape)


def key_chunk(count):
    return next(c for c in (4, 2, 1) if count % c == 0)


def attend(q, kv, q_pos, k_pos, boundary, span):
    rows, width = q.shape
    repeat = width // HEAD_DIM
    count = kv.shape[0] // span
    chunk = key_chunk(count)
    spec = pltpu.PrefetchScalarGridSpec(
        num_scalar_prefetch=3,
        grid=(count // chunk,),
        in_specs=[
            pl.BlockSpec((rows, width), lambda j, *_: (0, 0)),
            pl.BlockSpec((chunk * span, kv.shape[1]), lambda j, *_: (j, 0)),
        ],
        out_specs=[
            pl.BlockSpec((rows, width), lambda j, *_: (0, 0)),
            pl.BlockSpec((rows, 128 * repeat), lambda j, *_: (0, 0)),
        ],
        scratch_shapes=[
            pltpu.VMEM((rows, width), f32),
            pltpu.VMEM((rows, 128 * repeat), f32),
        ],
    )
    return pl.pallas_call(
        functools.partial(attend_kernel, span, repeat, count // chunk, chunk),
        out_shape=[
            jax.ShapeDtypeStruct((rows, width), bf16),
            jax.ShapeDtypeStruct((rows, 128 * repeat), f32),
        ],
        grid_spec=spec,
        compiler_params=pltpu.CompilerParams(dimension_semantics=("arbitrary",)),
        cost_estimate=pl.CostEstimate(
            flops=2 * rows * kv.shape[0] * width,
            bytes_accessed=2 * kv.size * 2,
            transcendentals=rows * kv.shape[0] * repeat,
        ),
    )(q_pos, k_pos, boundary, q, kv)


def attend_back_kernel(
    span, repeat, chunk, qp, kp, bd, q_ref, g_ref, lse_ref, ds_ref, kv_ref, dq_ref, dkv_ref, acc
):
    step = pl.program_id(0)

    @pl.when(step == 0)
    def _():
        dq_ref[...] = jnp.zeros_like(dq_ref)

    acc[...] = jnp.zeros_like(acc)

    def work(q_rows, k_rows, allowed):
        keys, values = kv_ref[k_rows, :HEAD_DIM], kv_ref[k_rows, HEAD_DIM:]
        for r in range(repeat):
            cols = slice(r * HEAD_DIM, (r + 1) * HEAD_DIM)
            query, grad = q_ref[q_rows, cols], g_ref[q_rows, cols]
            lse = lse_ref[q_rows, r * 128 : r * 128 + 1]
            dsum = ds_ref[q_rows, r * 128 : r * 128 + 1]
            bent = jnp.tanh(dot(query, keys, 1, 1) * (1.0 / soft_cap))
            probs = jnp.exp(soft_cap * bent - lse)
            if allowed is not None:
                probs = jnp.where(allowed, probs, 0.0)
            dprob = dot(grad, values, 1, 1)
            dscore = (probs * (dprob - dsum) * (1.0 - bent * bent)).astype(bf16)
            dq_ref[q_rows, cols] += dot(dscore, keys)
            acc[k_rows, :HEAD_DIM] += dot(dscore, query, 0, 0)
            acc[k_rows, HEAD_DIM:] += dot(probs.astype(bf16), grad, 0, 0)

    over_pairs(span, q_ref.shape[0] // span, chunk, qp, kp, bd, work)
    dkv_ref[...] = acc[...].astype(dkv_ref.dtype)


def attend_back(q, grad, lse, dsum, kv, q_pos, k_pos, boundary, span):
    rows, width = q.shape
    repeat = width // HEAD_DIM
    count = kv.shape[0] // span
    chunk = key_chunk(count)
    fixed = lambda w: pl.BlockSpec((rows, w), lambda j, *_: (0, 0))
    moving = pl.BlockSpec((chunk * span, kv.shape[1]), lambda j, *_: (j, 0))
    spec = pltpu.PrefetchScalarGridSpec(
        num_scalar_prefetch=3,
        grid=(count // chunk,),
        in_specs=[fixed(width), fixed(width), fixed(128 * repeat), fixed(128 * repeat), moving],
        out_specs=[fixed(width), moving],
        scratch_shapes=[pltpu.VMEM((chunk * span, kv.shape[1]), f32)],
    )
    return pl.pallas_call(
        functools.partial(attend_back_kernel, span, repeat, chunk),
        out_shape=[
            jax.ShapeDtypeStruct((rows, width), f32),
            jax.ShapeDtypeStruct(kv.shape, bf16),
        ],
        grid_spec=spec,
        compiler_params=pltpu.CompilerParams(dimension_semantics=("arbitrary",)),
        cost_estimate=pl.CostEstimate(
            flops=5 * rows * kv.shape[0] * width,
            bytes_accessed=2 * kv.size * 2,
            transcendentals=rows * kv.shape[0] * repeat,
        ),
    )(q_pos, k_pos, boundary, q, grad, lse, dsum, kv)


def on_device(
    plan,
    tokens,
    cotangent,
    span_order,
    segments,
    w_query,
    w_key,
    w_value,
    w_out,
    w_gate,
    w_up,
    w_down,
    gain_attn_in,
    gain_attn_out,
    gain_ffn_in,
    gain_ffn_out,
):
    rows, width = tokens.shape
    contexts, ulysses = plan.contexts, plan.ulysses
    layers, sides, cores, halves = plan.layers, plan.sides, plan.cores, plan.halves
    group_rows = rows * ulysses
    span = group_rows // 2
    q_scale = float(HEAD_DIM) ** (-0.5)
    ctx = lax.axis_index("ctx")
    layer, side, row, core = plan.here()

    ctx_ring = Ring(
        plan, sides, layers, lambda w, out, inn: (inn, out, w[2], w[3]), lambda w: (w[1], w[0])
    )
    ffn_ring = Ring(
        plan, plan.rows, layers, lambda w, out, inn: (inn, w[1], out, w[3]), lambda w: (w[2], w[0])
    )
    side_ring = Ring(
        plan, 1, sides, lambda w, out, inn: (w[0], inn, w[2], w[3]), lambda w: (0, w[1])
    )
    row_ring = Ring(
        plan, 1, plan.rows, lambda w, out, inn: (w[0], w[1], inn, w[3]), lambda w: (0, w[2])
    )
    core_ring = Ring(
        plan, 1, cores, lambda w, out, inn: (w[0], w[1], w[2], inn), lambda w: (0, w[3])
    )
    ctx_cells = jnp.array([inn * sides + out for out, inn in ctx_ring.cells], jnp.int32)
    ctx_place = ctx_ring.position(side, layer)
    ring_ctx = [ctx_cells[(ctx_place + k) % contexts] for k in range(contexts)]

    def group_gather(values):
        mine = ring_gather(values, row_ring)
        blocks, where = [], []
        for k, block in enumerate(mine):
            for m, found in enumerate(ring_gather(block, core_ring)):
                blocks.append(found)
                where.append((row + k) % plan.rows * cores + (core + m) % cores)
        return place_rows(blocks, where, ulysses).reshape(group_rows, values.shape[1])

    def group_scatter(values):
        parts = values.reshape(plan.rows, cores, rows, values.shape[1])

        def part(k, m):
            at = ((row + k) % plan.rows, (core + m) % cores, 0, 0)
            return lax.dynamic_slice(parts, at, (1, 1, *parts.shape[2:]))[0, 0]

        summed = [
            ring_scatter([part(k, m) for m in range(cores)], core_ring) for k in range(plan.rows)
        ]
        return ring_scatter(summed, row_ring)

    def ctx_scatter(arrays):
        size = arrays[0].shape[0] // contexts

        def part(k):
            blocks = [take_block(array, ring_ctx[k], size) for array in arrays]
            return jnp.concatenate(blocks, axis=1) if len(blocks) > 1 else blocks[0]

        return ring_scatter([part(k) for k in range(contexts)], ctx_ring, bf16)

    shard = gain_attn_in.shape[0]
    packed = jnp.stack([gain_attn_in, gain_attn_out, gain_ffn_in, gain_ffn_out])
    packed = jnp.pad(packed, ((0, 4), (0, -shard % 128)))
    tok_group, col_qkv, col_out, gains, ffn_gate = fetch_weights(
        plan, tokens, w_query, w_key, w_value, w_out, packed.astype(f32), w_gate
    )
    tok_group = tok_group.reshape(group_rows, width)
    col_qkv = col_qkv.reshape(width, -1)
    col_out = col_out.reshape(width, -1)
    gains = jnp.transpose(gains[:, :4, :shard], (1, 0, 2)).reshape(4, width)
    weight_one, weight_two, weight_three, weight_four = (1.0 + gains[k][None] for k in range(4))

    own_spans = lax.dynamic_slice_in_dim(span_order, 2 * ctx, 2, 0) * span
    boundary = jnp.sum((segments == 0).astype(jnp.int32)).reshape(1)
    key_spans = span_order * span
    group_pos = (own_spans[:, None] + jnp.arange(span, dtype=jnp.int32)[None, :]).reshape(-1)
    half = HEAD_DIM // 2
    freqs = rotary_base ** (-jnp.arange(half).astype(f32) / half)
    angles = group_pos.astype(f32)[:, None] * freqs[None, :]
    cosines, sines = jnp.cos(angles), jnp.sin(angles)

    q_cols, k_cols = w_query.shape[1] // ulysses, w_key.shape[1] // ulysses
    tok_rows = tok_group.astype(f32)
    normed_in = norm_apply(tok_rows, weight_one).astype(bf16)
    qkv = dot(normed_in, col_qkv)
    queries = (rotary(qkv[:, :q_cols], cosines, sines, 1.0) * q_scale).astype(bf16)
    keys = rotary(qkv[:, q_cols : q_cols + k_cols], cosines, sines, 1.0).astype(bf16)
    values = qkv[:, q_cols + k_cols :].astype(bf16)
    kv, ffn_up = fetch_keys(plan, jnp.concatenate([keys, values], axis=1), w_up)
    kv = kv.reshape(contexts * group_rows, -1)
    ffn_gate, ffn_up = ffn_gate.reshape(width, -1), ffn_up.reshape(width, -1)

    slice_cols = w_gate.shape[1] // halves

    def slice_perm(p):
        return plan.perm(lambda l, s, r, c: (c * halves + (l + p) % halves, s, r, l // halves))

    def slice_back(p):
        return [(b, a) for a, b in slice_perm(p)]

    def pick(options, index):
        out = options[0]
        for k in range(1, len(options)):
            out = jnp.where(index == k, options[k], out)
        return out

    def slice_fetch(weights):
        cuts = [weights[:, h * slice_cols : (h + 1) * slice_cols] for h in range(halves)]
        size = weights.shape[0]
        got = [move(pick(cuts, (layer + p) % halves), slice_perm(p)) for p in range(halves)]
        sided = ring_gather(jnp.concatenate(got, axis=0), side_ring)
        cored = ring_gather(jnp.concatenate(sided, axis=0), core_ring)
        blocks, where = [], []
        for m, found in enumerate(cored):
            for k in range(sides):
                for p in range(halves):
                    n = k * halves + p
                    blocks.append(found[n * size : (n + 1) * size])
                    origin = (core + m) % cores * halves + (layer - p) % halves
                    where.append(origin * sides + (side + k) % sides)
        return place_rows(blocks, where, contexts).reshape(width, slice_cols)

    def slice_start(lefts, right, earlier):
        others = []
        for m in range(1, cores):
            piece = dot(after(lefts[m], earlier), right, 0, 0).astype(bf16)
            perm = plan.perm(lambda l, s, r, c, m=m: (l, s, r, (c + m) % cores))
            others.append(move(piece, perm))
        own = dot(after(lefts[0], earlier), right, 0, 0).astype(bf16)
        arrays = [x.reshape(halves, sides, -1, slice_cols) for x in (own, *others)]
        size = arrays[0].shape[2]

        def side_part(k):
            at = (0, (side + k) % sides, 0, 0)
            shape = (halves, 1, size, slice_cols)
            found = sum(lax.dynamic_slice(x, at, shape).astype(f32) for x in arrays)
            return found.reshape(halves * size, slice_cols)

        sent = [side_part(k).astype(bf16) for k in range(1, sides)]
        summed = ring_scatter([side_part(0), *sent], side_ring, bf16)
        return summed.astype(bf16).reshape(halves, size, slice_cols)

    def slice_end(summed):
        got = []
        for p in range(halves):
            piece = lax.dynamic_index_in_dim(summed, (layer - p) % halves, 0, keepdims=False)
            got.append(move(piece, slice_back(p)))
        cuts = [pick(got, (h - layer) % halves) for h in range(halves)]
        return jnp.concatenate(cuts, axis=1).astype(f32)

    ffn_down = slice_fetch(after(w_down, kv))
    head_o, lse = attend(queries, kv, own_spans, key_spans, boundary, span)
    attn_out = group_scatter(dot(head_o, col_out, 1, 1))
    tok_own = tokens.astype(f32)
    hidden_in = tok_own + norm_apply(attn_out, weight_two)
    normed_own = norm_apply(hidden_in, weight_three).astype(bf16)

    size = ffn_ring.size
    order = [0]
    for k in range(1, size // 2):
        order += [k, size - k]
    order.append(size // 2)
    near = max(size - 3, 1)

    def ffn_gather(values):
        found = ring_gather(values, ffn_ring)
        return [
            jnp.concatenate([found[k] for k in ks], axis=0) for ks in (order[:near], order[near:])
        ]

    def ffn_scatter(chunk):
        parts = [None] * size
        far = chunk(1, None)
        for values, ks in ((far, order[near:]), (chunk(0, far), order[:near])):
            for n, k in enumerate(ks):
                parts[k] = values[n * rows : (n + 1) * rows]
        landed = []
        return ring_scatter(parts, ffn_ring, bf16, landed), landed

    normed_mid = ffn_gather(normed_own)
    gate = [dot(x, ffn_gate) for x in normed_mid]
    upper = [dot(x, ffn_up) for x in normed_mid]
    hidden = [(gelu_parts(g)[0] * u).astype(bf16) for g, u in zip(gate, upper, strict=True)]

    def down_part(n, far):
        rows_in = hidden[n] if far is None else after(hidden[n], far)
        return dot(rows_in, ffn_down, 1, 1).astype(bf16)

    ffn_out, _ = ffn_scatter(down_part)
    block_out = (hidden_in + norm_apply(ffn_out, weight_four)).astype(bf16)
    cot_own = cotangent.astype(f32)
    d_ffn = ffn_gather(norm_grad(ffn_out, weight_four, cot_own).astype(bf16))
    d_gate, d_upper = [], []
    for n in range(2):
        d_hidden = dot(d_ffn[n], ffn_down)
        gate_value, gate_slope = gelu_parts(gate[n])
        d_gate.append((d_hidden * upper[n] * gate_slope).astype(bf16))
        d_upper.append((d_hidden * gate_value).astype(bf16))

    def mid_part(n, far):
        left, right = d_gate[n], d_upper[n]
        if far is not None:
            left, right = after(left, far), after(right, far)
        first = lax.optimization_barrier(dot(left, ffn_gate, 1, 1).astype(bf16))
        return (first.astype(f32) + dot(right, ffn_up, 1, 1)).astype(bf16)

    d_mid, landed = ffn_scatter(mid_part)
    grad_hidden = cot_own + norm_grad(hidden_in, weight_three, d_mid)

    def by_core(pieces):
        cols = width // cores
        cut = lambda x, m: lax.dynamic_slice_in_dim(x, (core + m) % cores * cols, cols, 1)
        return [jnp.concatenate([cut(x, m) for x in pieces], axis=0) for m in range(cores)]

    d_ffn, normed_mid = by_core(d_ffn), by_core(normed_mid)
    hidden, d_gate, d_upper = (jnp.concatenate(x, axis=0) for x in (hidden, d_gate, d_upper))
    sum_down = slice_start(d_ffn, hidden, landed[0])
    sum_gate = slice_start(normed_mid, d_gate, landed[min(1, len(landed) - 1)])
    sum_up = slice_start(normed_mid, d_upper, d_mid)
    grad_down = slice_end(after(sum_down, d_mid))
    grad_gate = slice_end(after(sum_gate, d_mid))

    d_attn = group_gather(norm_grad(attn_out, weight_two, grad_hidden).astype(bf16))
    out_part = dot(d_attn, head_o, 0, 0).astype(bf16)
    grad_o = dot(d_attn, col_out).astype(bf16)
    products = grad_o.astype(f32) * head_o.astype(f32)
    dsum = jnp.concatenate(
        [
            jnp.broadcast_to(
                jnp.sum(products[:, s : s + HEAD_DIM], axis=1, keepdims=True), (group_rows, 128)
            )
            for s in range(0, q_cols, HEAD_DIM)
        ],
        axis=1,
    )
    grad_q, grad_kv = attend_back(
        queries, grad_o, lse, dsum, kv, own_spans, key_spans, boundary, span
    )
    grad_kv = ctx_scatter([grad_kv])
    grad_up = slice_end(after(sum_up, grad_q))
    grad_q = (rotary(grad_q, cosines, sines, -1.0) * q_scale).astype(bf16)
    k_cosines, k_sines = after(cosines, grad_kv), after(sines, grad_kv)
    grad_k = rotary(grad_kv[:, :k_cols], k_cosines, k_sines, -1.0).astype(bf16)
    grad_v = grad_kv[:, k_cols:].astype(bf16)
    grad_kv = jnp.concatenate([grad_k, grad_v], axis=1)
    q_part = dot(normed_in, grad_q, 0, 0).astype(bf16)
    kv_part = dot(normed_in, grad_kv, 0, 0).astype(bf16)
    d_in_part = dot(grad_q, col_qkv[:, :q_cols], 1, 1)
    d_in_part = (d_in_part + dot(grad_kv, col_qkv[:, q_cols:], 1, 1)).astype(bf16)

    gain_parts = jnp.stack(
        [
            gain_part(attn_out, after(grad_hidden, grad_q)),
            gain_part(hidden_in, after(d_mid, grad_q)),
            gain_part(ffn_out, after(cot_own, grad_q)),
        ]
    ).reshape(3, contexts * ulysses, shard)
    gain_parts = jnp.pad(jnp.transpose(gain_parts, (1, 0, 2)), ((0, 0), (0, 5), (0, -shard % 128)))
    grad_query, grad_key, grad_value, grad_outproj, d_in, gain_grads = sum_grads(
        plan,
        q_part.reshape(contexts * ulysses, shard, -1),
        kv_part.reshape(contexts * ulysses, shard, -1),
        out_part.reshape(contexts * ulysses, shard, -1),
        d_in_part.reshape(ulysses, rows, width),
        gain_parts,
        w_query.shape[1],
        w_key.shape[1],
    )
    grad_outproj = grad_outproj.reshape(w_out.shape)
    gain_grads = gain_grads[:, :shard]
    grad_tokens = grad_hidden + norm_grad(tok_own, weight_one, d_in)
    products = [
        jnp.sum(w.astype(f32) * g, axis=1)
        for w, g in ((w_query, grad_query), (w_key, grad_key), (w_value, grad_value))
    ]
    gain_first = (products[0] + products[1] + products[2]) / (1.0 + gain_attn_in.astype(f32))
    return (
        block_out,
        grad_tokens,
        grad_query,
        grad_key,
        grad_value,
        grad_outproj,
        grad_gate,
        grad_up,
        grad_down,
        gain_first,
        gain_grads[0],
        gain_grads[1],
        gain_grads[2],
    )


def solution(mesh):
    flat, cut, line = P(AXES, None), P("ctx", "uly"), P(AXES)
    in_specs = (flat, flat, P(), P(), flat, flat, flat, cut, cut, cut, cut, line, line, line, line)
    out_specs = (flat, flat, flat, flat, flat, cut, cut, cut, cut, line, line, line, line)
    plan = Plan(mesh)

    def body(*args):
        return on_device(plan, *args)

    return jax.shard_map(
        body, mesh=mesh, in_specs=in_specs, out_specs=out_specs, check_vma=False
    )
```

```python
import functools

import jax
import jax.numpy as jnp
from jax import lax
from jax.experimental import pallas as pl
from jax.experimental.pallas import tpu as pltpu
from jax.sharding import PartitionSpec as P


HEAD_DIM = 256
AXES = ("ctx", "uly")

norm_eps = 1e-06
soft_cap = 50.0
rotary_base = 10000.0
gelu_coef = 0.7978845608028654
cubic_coef = 0.044715


bf16 = jnp.bfloat16
f32 = jnp.float32


def rms_scale(values):
    return lax.rsqrt(jnp.mean(values * values, axis=-1, keepdims=True) + norm_eps)


def norm_apply(values, weight):
    return values * rms_scale(values) * weight


def norm_grad(values, weight, grad):
    scale = rms_scale(values)
    inner = jnp.mean(grad * weight * values, axis=-1, keepdims=True)
    return scale * weight * grad - values * (scale * scale * scale) * inner


def gain_part(values, grad):
    return jnp.sum(grad * values * rms_scale(values), axis=0)


def gelu_parts(values):
    inner = gelu_coef * (values + cubic_coef * values * values * values)
    tanh_part = jnp.tanh(inner)
    value = 0.5 * values * (1.0 + tanh_part)
    slope = 0.5 * (1.0 + tanh_part) + 0.5 * values * (1.0 - tanh_part * tanh_part) * gelu_coef * (
        1.0 + 3.0 * cubic_coef * values * values
    )
    return value, slope


def rotary(values, cosines, sines, sign):
    half = HEAD_DIM // 2
    parts = []
    for start in range(0, values.shape[1], HEAD_DIM):
        first = values[:, start : start + half]
        second = values[:, start + half : start + HEAD_DIM]
        parts.append(first * cosines - sign * second * sines)
        parts.append(second * cosines + sign * first * sines)
    return jnp.concatenate(parts, axis=1)


def dot(left, right, left_dim=1, right_dim=0):
    return lax.dot_general(
        left, right, (((left_dim,), (right_dim,)), ((), ())), preferred_element_type=f32
    )


class Plan:
    def __init__(self, mesh):
        grid = mesh.devices
        self.contexts, self.ulysses = mesh.shape["ctx"], mesh.shape["uly"]
        self.cores = sum(tuple(d.coords) == tuple(grid[0, 0].coords) for d in grid[0])
        self.layers = len({d.coords[2] for d in grid[:, 0]})
        self.sides = self.contexts // self.layers
        self.rows = self.ulysses // self.cores
        self.halves = self.layers // self.cores

    def split(self, device):
        ctx, uly = divmod(device, self.ulysses)
        return (*divmod(ctx, self.sides), *divmod(uly, self.cores))

    def join(self, layer, side, row, core):
        return (layer * self.sides + side) * self.ulysses + row * self.cores + core

    def perm(self, target):
        count = self.contexts * self.ulysses
        return [(d, self.join(*target(*self.split(d)))) for d in range(count)]

    def here(self):
        layer, side = jnp.divmod(lax.axis_index("ctx"), self.sides)
        row, core = jnp.divmod(lax.axis_index("uly"), self.cores)
        return layer, side, row, core


class Ring:
    def __init__(self, plan, outer, inner, place, locate):
        self.size = outer * inner
        self.inner = inner

        def cell(index):
            out, rest = divmod(index % self.size, inner)
            return out, (rest if out % 2 == 0 else inner - 1 - rest)

        def index_of(out, inn):
            return out * inner + (inn if out % 2 == 0 else inner - 1 - inn)

        self.cells = [cell(i) for i in range(self.size)]

        def shifted(step):
            def target(*where):
                return place(where, *cell(index_of(*locate(where)) + step))

            return plan.perm(target)

        self.ahead, self.behind = shifted(1), shifted(-1)

    def position(self, out, inn):
        rest = jnp.where(out % 2 == 0, inn, self.inner - 1 - inn)
        return out * self.inner + rest


def move(values, perm):
    return lax.ppermute(values, AXES, perm)


def both(*values):
    return lax.optimization_barrier(values)


def after(values, *earlier):
    return lax.optimization_barrier((values, *earlier))[0]


def ring_gather(block, ring):
    size = ring.size
    found = {0: block}
    if size == 2:
        found[1] = move(block, ring.ahead)
        return [found[0], found[1]]
    forth = back = block
    middle = size // 2
    for step in range(1, middle):
        forth = move(forth, ring.ahead)
        back = move(back, ring.behind)
        forth, back = both(forth, back)
        found[size - step], found[step] = forth, back
    cut = block.shape[0] // 2
    forth = move(forth[:cut], ring.ahead)
    back = move(back[cut:], ring.behind)
    found[middle] = jnp.concatenate([forth, back], axis=0)
    return [found[k] for k in range(size)]


def ring_scatter(parts, ring, kind=bf16, landed=None):
    size = ring.size
    if size == 2:
        return parts[0].astype(f32) + move(parts[1].astype(kind), ring.ahead).astype(f32)
    middle = size // 2
    cut = parts[0].shape[0] // 2
    forth = move(parts[middle][:cut].astype(kind), ring.ahead)
    back = move(parts[middle][cut:].astype(kind), ring.behind)
    forth, back = both(forth, back)
    landed = [] if landed is None else landed
    for left in range(middle - 1, 0, -1):
        landed.append(forth)
        fore, aft = parts[left].astype(f32), parts[size - left].astype(f32)
        if left == middle - 1:
            fore = jnp.concatenate([fore[:cut] + forth.astype(f32), fore[cut:]], axis=0)
            aft = jnp.concatenate([aft[:cut], aft[cut:] + back.astype(f32)], axis=0)
        else:
            fore, aft = fore + forth.astype(f32), aft + back.astype(f32)
        forth = move(fore.astype(kind), ring.ahead)
        back = move(aft.astype(kind), ring.behind)
        forth, back = both(forth, back)
    return parts[0].astype(f32) + forth.astype(f32) + back.astype(f32)


def place_rows(blocks, indices, count):
    first = blocks[0]
    out = jnp.zeros((count, *first.shape), first.dtype)
    for block, index in zip(blocks, indices, strict=True):
        out = lax.dynamic_update_slice(out, block[None], (index, *(0,) * first.ndim))
    return out


def take_block(values, index, size):
    return lax.dynamic_slice_in_dim(values, index * size, size, 0)


class Sender:
    def __init__(self, plan, send, recv):
        self.plan, self.send, self.recv, self.sent = plan, send, recv, []
        self.ctx, self.uly = lax.axis_index("ctx"), lax.axis_index("uly")
        self.layer, self.side = self.ctx // plan.sides, self.ctx % plan.sides
        self.row, self.core = self.uly // plan.cores, self.uly % plan.cores
        flip = self.side % 2
        self.here = self.side * plan.layers + (
            self.layer * (1 - flip) + (plan.layers - 1 - self.layer) * flip
        )

    def at(self, layer, side, row, core):
        plan = self.plan
        return {"ctx": layer * plan.sides + side, "uly": row * plan.cores + core}

    def group(self):
        plan = self.plan
        for dr in range(plan.rows - 1, -1, -1):
            for dc in range(plan.cores):
                if (dr, dc) != (0, 0):
                    row, core = (self.row + dr) % plan.rows, (self.core + dc) % plan.cores
                    yield self.at(self.layer, self.side, row, core), row * plan.cores + core

    def meet(self):
        plan = self.plan
        friends = [friend for friend, _ in self.group()]
        for dl in range(1, plan.layers):
            for dc in range(plan.cores):
                layer, core = (self.layer + dl) % plan.layers, (self.core + dc) % plan.cores
                friends.append(self.at(layer, self.side, self.row, core))
        for ds in sorted({1 % plan.sides, plan.sides - 1} - {0}):
            side = (self.side + ds) % plan.sides
            friends.append(self.at(self.layer, side, self.row, self.core))
        barrier = pltpu.get_barrier_semaphore()
        for friend in friends:
            pl.semaphore_signal(
                barrier, inc=1, device_id=friend, device_id_type=pl.DeviceIdType.MESH
            )
        pl.semaphore_wait(barrier, len(friends))

    def push(self, source, target, device):
        k = len(self.sent)
        copy = pltpu.make_async_remote_copy(
            source,
            target,
            self.send.at[k],
            self.recv.at[k],
            device_id=device,
            device_id_type=pl.DeviceIdType.MESH,
        )
        copy.start()
        self.sent.append(copy)
        return copy

    def finish(self):
        for copy in self.sent:
            copy.wait_send()

    def spot(self, index):
        plan = self.plan
        out, low = index // plan.layers, index % plan.layers
        flip = out % 2
        return (low * (1 - flip) + (plan.layers - 1 - low) * flip) * plan.sides + out

    def ring(self, piece, cut, own=None):
        count = self.plan.contexts
        middle = count // 2
        ahead = {"ctx": self.spot((self.here + 1) % count), "uly": self.uly}
        behind = {"ctx": self.spot((self.here + count - 1) % count), "uly": self.uly}
        last = ()
        for step in range(middle):
            for copy in last:
                copy.wait_recv()
            fore = piece(self.spot((self.here + count - step) % count))
            aft = piece(self.spot((self.here + step) % count))
            first, second = (fore, aft) if step or own is None else (own, own)
            if step == middle - 1:
                fore, first = fore.at[:cut], first.at[:cut]
                aft, second = aft.at[cut:], second.at[cut:]
            last = (self.push(first, fore, ahead), self.push(second, aft, behind))
            yield
        for copy in last:
            copy.wait_recv()

    def slice_send(self, matrix, result, p):
        plan = self.plan
        h = (self.layer + p) % plan.halves
        target = self.at(
            self.core * plan.halves + h,
            self.side,
            self.row,
            plan.cores - 1 - self.layer // plan.halves,
        )
        width = matrix.shape[1] // plan.halves
        cols = pl.ds(pl.multiple_of(h * width, 128), width)
        return self.push(matrix.at[:, cols], result.at[self.ctx], target)

    def slice_pass(self, result, p, held):
        plan = self.plan
        origin = (plan.cores - 1 - self.core) * plan.halves
        origin = origin + (self.layer - p + plan.halves) % plan.halves
        passed = []
        for step in range(plan.sides):
            held.wait_recv()
            slot = result.at[origin * plan.sides + (self.side - step + plan.sides) % plan.sides]
            for dc in range(1, plan.cores):
                core = (self.core + dc) % plan.cores
                passed.append(self.push(slot, slot, self.at(self.layer, self.side, self.row, core)))
            if step < plan.sides - 1:
                side = (self.side + 1) % plan.sides
                held = self.push(slot, slot, self.at(self.layer, side, self.row, self.core))
            yield
        for copy in passed:
            copy.wait_recv()

    def run(self, rings, slices):
        flying, moving = [], []
        tasks = [(m, r, p) for m, r in slices for p in range(self.plan.halves)]

        def drive(generators):
            return [g for g in generators if next(g, "end") != "end"]

        while rings or tasks or flying or moving:
            rings = drive(rings)
            if flying:
                moving.append(self.slice_pass(*flying.pop(0)))
            if tasks:
                matrix, result, p = tasks.pop(0)
                flying.append((result, p, self.slice_send(matrix, result, p)))
            moving = drive(moving)


def copies_of(plan, slices):
    return slices * plan.halves * (1 + plan.sides - 1 + plan.sides * (plan.cores - 1))


def weights_kernel(plan, *refs):
    tok_in, wq, wk, wv, out_in, gain_in, gate_in = refs[:7]
    tok_all, qkv, out_all, gain_all, gate_all = refs[7:12]
    tok_tmp, qkv_tmp, out_tmp, gain_tmp, local, send, recv = refs[12:]
    link = Sender(plan, send, recv)
    link.meet()
    ulysses, ctx, uly = plan.ulysses, link.ctx, link.uly
    q_cols, k_cols = wq.shape[1] // ulysses, wk.shape[1] // ulysses

    def parts(u):
        yield wq.at[:, pl.ds(pl.multiple_of(u * q_cols, 128), q_cols)], pl.ds(0, q_cols)
        for k, matrix in enumerate((wk, wv)):
            cols = pl.ds(pl.multiple_of(u * k_cols, 128), k_cols)
            yield matrix.at[:, cols], pl.ds(q_cols + k * k_cols, k_cols)

    pairs = [(src, qkv_tmp.at[:, cols]) for src, cols in parts(uly)]
    pairs += [(gain_in, gain_tmp), (out_in, out_tmp), (tok_in, tok_tmp)]
    pulls = [pltpu.make_async_copy(*pair, local.at[k]) for k, pair in enumerate(pairs)]
    for pull in pulls:
        pull.start()
    place = ctx * ulysses + uly
    first = []
    for friend, u in link.group():
        for source, cols in parts(u):
            first.append(link.push(source, qkv.at[place, :, cols], friend))
        first.append(link.push(gain_in, gain_all.at[place], friend))
    for pull in pulls:
        pull.wait()
    pairs = [
        (qkv_tmp, qkv.at[place]),
        (gain_tmp, gain_all.at[place]),
        (out_tmp, out_all.at[ctx]),
        (tok_tmp, tok_all.at[uly]),
    ]
    puts = [pltpu.make_async_copy(*pair, local.at[6 + k]) for k, pair in enumerate(pairs)]
    for put in puts:
        put.start()
    for put in puts:
        put.wait()
    for copy in first:
        copy.wait_recv()
    tokens = [link.push(tok_in, tok_all.at[uly], friend) for friend, _ in link.group()]

    def block(array):
        return lambda c: array.at[pl.ds(c * ulysses, ulysses)]

    rings = [
        link.ring(block(qkv), ulysses // 2),
        link.ring(block(gain_all), ulysses // 2),
        link.ring(lambda c: out_all.at[c], out_all.shape[1] // 16 * 8),
    ]
    link.run(rings, [(gate_in, gate_all)])
    for copy in tokens:
        copy.wait_recv()
    link.finish()


anywhere = pl.BlockSpec(memory_space=pl.ANY)


def sliced(plan, weights):
    shape = (plan.contexts, weights.shape[0], weights.shape[1] // plan.halves)
    return jax.ShapeDtypeStruct(shape, weights.dtype)


def fetch_weights(plan, tokens, wq, wk, wv, w_out, gains, w_gate):
    shard, contexts, ulysses = wq.shape[0], plan.contexts, plan.ulysses
    cols = (wq.shape[1] + wk.shape[1] + wv.shape[1]) // ulysses
    results = [
        jax.ShapeDtypeStruct((ulysses, *tokens.shape), tokens.dtype),
        jax.ShapeDtypeStruct((contexts * ulysses, shard, cols), wq.dtype),
        jax.ShapeDtypeStruct((contexts, *w_out.shape), w_out.dtype),
        jax.ShapeDtypeStruct((contexts * ulysses, *gains.shape), gains.dtype),
        sliced(plan, w_gate),
    ]
    copies = 5 * (ulysses - 1) + 3 * contexts + copies_of(plan, 1)
    return pl.pallas_call(
        functools.partial(weights_kernel, plan),
        out_shape=results,
        in_specs=[anywhere] * 7,
        out_specs=[anywhere] * len(results),
        scratch_shapes=[
            pltpu.VMEM(tokens.shape, tokens.dtype),
            pltpu.VMEM((shard, cols), wq.dtype),
            pltpu.VMEM(w_out.shape, w_out.dtype),
            pltpu.VMEM(gains.shape, gains.dtype),
            pltpu.SemaphoreType.DMA((10,)),
            pltpu.SemaphoreType.DMA((copies,)),
            pltpu.SemaphoreType.DMA((copies,)),
        ],
        compiler_params=pltpu.CompilerParams(collective_id=1, has_side_effects=True),
    )(tokens, wq, wk, wv, w_out, gains, w_gate)


def keys_kernel(plan, kv_in, up_in, kv_all, up_all, tmp, local, send, recv):
    link = Sender(plan, send, recv)
    link.meet()
    pull = pltpu.make_async_copy(kv_in, tmp, local.at[0])
    put = pltpu.make_async_copy(tmp, kv_all.at[link.ctx], local.at[1])
    pull.start()
    pull.wait()
    put.start()
    ring = link.ring(lambda c: kv_all.at[c], kv_in.shape[0] // 2, kv_in)
    link.run([ring], [(up_in, up_all)])
    put.wait()
    link.finish()


def fetch_keys(plan, kv, w_up):
    copies = plan.contexts + copies_of(plan, 1)
    return pl.pallas_call(
        functools.partial(keys_kernel, plan),
        out_shape=[
            jax.ShapeDtypeStruct((plan.contexts, *kv.shape), kv.dtype),
            sliced(plan, w_up),
        ],
        in_specs=[anywhere] * 2,
        out_specs=[anywhere] * 2,
        scratch_shapes=[
            pltpu.VMEM(kv.shape, kv.dtype),
            pltpu.SemaphoreType.DMA((2,)),
            pltpu.SemaphoreType.DMA((copies,)),
            pltpu.SemaphoreType.DMA((copies,)),
        ],
        compiler_params=pltpu.CompilerParams(collective_id=2, has_side_effects=True),
    )(kv, w_up)


def grads_kernel(plan, q_in, kv_in, out_in, rows_in, gain_in, *refs):
    parts = (q_in, kv_in, out_in)
    lows = (0, q_in.shape[2], q_in.shape[2] + kv_in.shape[2])
    query_out, key_out, value_out, out_out, rows_out, gain_out = refs[:6]
    main_send, main_recv, gain_send, gain_recv, turn_send, turn_recv, gain_last, gain_turn = refs[6:14]
    core_recv, row_send, row_recv, send, recv = refs[14:]
    link = Sender(plan, send, recv)
    count, ulysses, cores = plan.contexts, plan.ulysses, plan.cores
    middle = count // 2
    ctx, uly = link.ctx, link.uly
    ahead = {"ctx": link.spot((link.here + 1) % count), "uly": uly}
    behind = {"ctx": link.spot((link.here + count - 1) % count), "uly": uly}
    link.meet()

    half = max(ulysses // 2, 1)
    lanes = [range(half), range(half, ulysses)]

    def pass_on(step, way, lane):
        left = middle - step
        there = link.spot((link.here + (left if way == 0 else count - left)) % count)
        received = step > 1 or (step == 1 and lane == way)
        for m in lanes[lane]:
            place = there * ulysses + m
            gain = gain_in[place]
            for array, low in zip(parts, lows, strict=True):
                high = low + array.shape[2]
                block = array[place]
                if received:
                    block = block.astype(f32) + main_recv[step - 1, way, m, :, low:high].astype(f32)
                main_send[step, way, m, :, low:high] = block.astype(bf16)
            gain_send[step, way, m] = gain + gain_recv[step - 1, way, m] if received else gain
        device = ahead if way == 0 else behind
        rows = pl.ds(lanes[lane][0], len(lanes[lane]))
        return [
            link.push(main_send.at[step, way, rows], main_recv.at[step, way, rows], device),
            link.push(gain_send.at[step, way, rows], gain_recv.at[step, way, rows], device),
        ]

    last = {}
    core_copies, row_copies = [], []
    for step in range(middle):
        sent = {}
        for lane in range(2):
            for way in range(2):
                for copy in last.get((lane, way), ()):
                    copy.wait_recv()
                if step or lane == way:
                    sent[lane, way] = pass_on(step, way, lane)
        last = sent
        if step == 0:
            for dc in range(1, cores):
                core = (link.core + dc) % cores
                for r in range(plan.rows):
                    device = link.at(link.layer, link.side, link.row, core)
                    source = rows_in.at[r * cores + core]
                    core_copies.append(link.push(source, core_recv.at[dc - 1, r], device))
        if step == min(1, middle - 1):
            for copy in core_copies:
                copy.wait_recv()

            def total(r):
                found = rows_in[r * cores + link.core].astype(f32)
                for dc in range(1, cores):
                    found = found + core_recv[dc - 1, r].astype(f32)
                return found

            for dr in range(1, plan.rows):
                row_send[dr - 1] = total((link.row + dr) % plan.rows).astype(bf16)
            rows_out[...] = total(link.row)
            for dr in range(1, plan.rows):
                device = link.at(link.layer, link.side, (link.row + dr) % plan.rows, link.core)
                row_copies.append(link.push(row_send.at[dr - 1], row_recv.at[dr - 1], device))
    for copies in last.values():
        for copy in copies:
            copy.wait_recv()
    place = ctx * ulysses

    def finish(m, array, received, low):
        high = low + array.shape[2]
        found = array[place + m].astype(f32)
        if middle > 1:
            return found + received[middle - 1, 0, m, :, low:high].astype(f32) + received[
                middle - 1, 1, m, :, low:high
            ].astype(f32)
        way = 0 if m < ulysses // 2 else 1
        return found + received[0, way, m, :, low:high].astype(f32)

    for m in range(ulysses):
        turn_send[m, :, : lows[1]] = finish(m, q_in, main_recv, 0).astype(bf16)
        turn_send[m, :, lows[1] :] = finish(m, kv_in, main_recv, lows[1]).astype(bf16)
        gain_last[m] = finish(m, gain_in, gain_recv, 0)
    turn_recv[uly] = turn_send[uly]
    gain_turn[uly] = gain_last[uly]
    turned = []
    for friend, u in link.group():
        turned.append(link.push(turn_send.at[u], turn_recv.at[uly], friend))
        turned.append(link.push(gain_last.at[u], gain_turn.at[uly], friend))
    for m in range(ulysses):
        out_out[m] = finish(m, out_in, main_recv, lows[2])
    for dr, copy in enumerate(row_copies):
        copy.wait_recv()
        rows_out[...] += row_recv[dr].astype(f32)
    for copy in turned:
        copy.wait_recv()
    q_cols, k_cols = query_out.shape[1] // ulysses, key_out.shape[1] // ulysses
    for u in range(ulysses):
        query_out[:, u * q_cols : (u + 1) * q_cols] = turn_recv[u, :, :q_cols].astype(f32)
        cols = slice(u * k_cols, (u + 1) * k_cols)
        key_out[:, cols] = turn_recv[u, :, q_cols : q_cols + k_cols].astype(f32)
        value_out[:, cols] = turn_recv[u, :, q_cols + k_cols :].astype(f32)
    gain_out[...] = gain_turn[0]
    for u in range(1, ulysses):
        gain_out[...] += gain_turn[u]
    link.finish()


def sum_grads(plan, q, kv, out, rows, gains, q_width, k_width):
    contexts, ulysses = plan.contexts, plan.ulysses
    shard = q.shape[1]
    turned = (ulysses, shard, q.shape[2] + kv.shape[2])
    middle, tail = contexts // 2, gains.shape[1:]
    wide = (shard, turned[2] + out.shape[2])
    block = rows.shape[1:]
    results = [
        jax.ShapeDtypeStruct((shard, q_width), f32),
        jax.ShapeDtypeStruct((shard, k_width), f32),
        jax.ShapeDtypeStruct((shard, k_width), f32),
        jax.ShapeDtypeStruct((ulysses, *out.shape[1:]), f32),
        jax.ShapeDtypeStruct(block, f32),
        jax.ShapeDtypeStruct(tail, f32),
    ]
    copies = 8 * middle + (plan.cores - 1) * plan.rows + plan.rows - 1 + 2 * (ulysses - 1)
    local = pl.BlockSpec(memory_space=pltpu.VMEM)
    return pl.pallas_call(
        functools.partial(grads_kernel, plan),
        out_shape=results,
        in_specs=[local] * 5,
        out_specs=[local] * len(results),
        scratch_shapes=[
            pltpu.VMEM((middle, 2, ulysses, *wide), bf16),
            pltpu.VMEM((middle, 2, ulysses, *wide), bf16),
            pltpu.VMEM((middle, 2, ulysses, *tail), f32),
            pltpu.VMEM((middle, 2, ulysses, *tail), f32),
            pltpu.VMEM(turned, bf16),
            pltpu.VMEM(turned, bf16),
            pltpu.VMEM((ulysses, *tail), f32),
            pltpu.VMEM((ulysses, *tail), f32),
            pltpu.VMEM((max(plan.cores - 1, 1), plan.rows, *block), bf16),
            pltpu.VMEM((max(plan.rows - 1, 1), *block), bf16),
            pltpu.VMEM((max(plan.rows - 1, 1), *block), bf16),
            pltpu.SemaphoreType.DMA((copies,)),
            pltpu.SemaphoreType.DMA((copies,)),
        ],
        compiler_params=pltpu.CompilerParams(collective_id=3, has_side_effects=True),
    )(q, kv, out, rows, gains)


def visible(q_first, k_first, boundary, span):
    q_pos = q_first + lax.broadcasted_iota(jnp.int32, (span, span), 0)
    k_pos = k_first + lax.broadcasted_iota(jnp.int32, (span, span), 1)
    low = jnp.where(q_pos >= boundary, boundary, 0)
    return (k_pos <= q_pos) & (k_pos >= low)


def active(q_first, k_first, boundary, span):
    split = (q_first >= boundary) & (k_first + span <= boundary)
    return (k_first <= q_first) & jnp.logical_not(split)


def whole(q_first, k_first, boundary, span):
    same = (k_first >= boundary) | (q_first + span <= boundary)
    return (k_first + span <= q_first) & same


def over_pairs(span, blocks, chunk, qp, kp, bd, work):
    start = pl.program_id(0) * chunk

    def pair(t, carry):
        i, j = t % blocks, t // blocks
        q_first, k_first, boundary = qp[i], kp[start + j], bd[0]
        q_rows = pl.ds(pl.multiple_of(i * span, span), span)
        k_rows = pl.ds(pl.multiple_of(j * span, span), span)
        full = whole(q_first, k_first, boundary, span)

        @pl.when(full)
        def _():
            work(q_rows, k_rows, None)

        @pl.when(active(q_first, k_first, boundary, span) & jnp.logical_not(full))
        def _():
            work(q_rows, k_rows, visible(q_first, k_first, boundary, span))

        return carry

    lax.fori_loop(0, blocks * chunk, pair, 0)


def attend_kernel(span, repeat, steps, chunk, qp, kp, bd, q_ref, kv_ref, o_ref, lse_ref, acc, den):
    step = pl.program_id(0)

    @pl.when(step == 0)
    def _():
        acc[...] = jnp.zeros_like(acc)
        den[...] = jnp.zeros_like(den)

    def work(q_rows, k_rows, allowed):
        keys, values = kv_ref[k_rows, :HEAD_DIM], kv_ref[k_rows, HEAD_DIM:]
        for r in range(repeat):
            cols = slice(r * HEAD_DIM, (r + 1) * HEAD_DIM)
            scores = dot(q_ref[q_rows, cols], keys, 1, 1)
            weights = jnp.exp(soft_cap * jnp.tanh(scores * (1.0 / soft_cap)))
            if allowed is not None:
                weights = jnp.where(allowed, weights, 0.0)
            folded = weights[:, :128]
            for k in range(128, span, 128):
                folded = folded + weights[:, k : k + 128]
            den[q_rows, r * 128 : (r + 1) * 128] += folded
            acc[q_rows, cols] += dot(weights.astype(bf16), values)

    over_pairs(span, q_ref.shape[0] // span, chunk, qp, kp, bd, work)

    @pl.when(step == steps - 1)
    def _():
        for r in range(repeat):
            cols, lanes = slice(r * HEAD_DIM, (r + 1) * HEAD_DIM), slice(r * 128, (r + 1) * 128)
            total = jnp.sum(den[:, lanes], axis=1, keepdims=True)
            o_ref[:, cols] = (acc[:, cols] / total).astype(bf16)
            lse_ref[:, lanes] = jnp.broadcast_to(jnp.log(total), den[:, lanes].shape)


def key_chunk(count):
    return next(c for c in (4, 2, 1) if count % c == 0)


def attend(q, kv, q_pos, k_pos, boundary, span):
    rows, width = q.shape
    repeat = width // HEAD_DIM
    count = kv.shape[0] // span
    chunk = key_chunk(count)
    spec = pltpu.PrefetchScalarGridSpec(
        num_scalar_prefetch=3,
        grid=(count // chunk,),
        in_specs=[
            pl.BlockSpec((rows, width), lambda j, *_: (0, 0)),
            pl.BlockSpec((chunk * span, kv.shape[1]), lambda j, *_: (j, 0)),
        ],
        out_specs=[
            pl.BlockSpec((rows, width), lambda j, *_: (0, 0)),
            pl.BlockSpec((rows, 128 * repeat), lambda j, *_: (0, 0)),
        ],
        scratch_shapes=[
            pltpu.VMEM((rows, width), f32),
            pltpu.VMEM((rows, 128 * repeat), f32),
        ],
    )
    return pl.pallas_call(
        functools.partial(attend_kernel, span, repeat, count // chunk, chunk),
        out_shape=[
            jax.ShapeDtypeStruct((rows, width), bf16),
            jax.ShapeDtypeStruct((rows, 128 * repeat), f32),
        ],
        grid_spec=spec,
        compiler_params=pltpu.CompilerParams(dimension_semantics=("arbitrary",)),
        cost_estimate=pl.CostEstimate(
            flops=2 * rows * kv.shape[0] * width,
            bytes_accessed=2 * kv.size * 2,
            transcendentals=rows * kv.shape[0] * repeat,
        ),
    )(q_pos, k_pos, boundary, q, kv)


def attend_back_kernel(
    span, repeat, chunk, qp, kp, bd, q_ref, g_ref, lse_ref, ds_ref, kv_ref, dq_ref, dkv_ref, acc
):
    step = pl.program_id(0)

    @pl.when(step == 0)
    def _():
        dq_ref[...] = jnp.zeros_like(dq_ref)

    acc[...] = jnp.zeros_like(acc)

    def work(q_rows, k_rows, allowed):
        keys, values = kv_ref[k_rows, :HEAD_DIM], kv_ref[k_rows, HEAD_DIM:]
        for r in range(repeat):
            cols = slice(r * HEAD_DIM, (r + 1) * HEAD_DIM)
            query, grad = q_ref[q_rows, cols], g_ref[q_rows, cols]
            lse = lse_ref[q_rows, r * 128 : r * 128 + 1]
            dsum = ds_ref[q_rows, r * 128 : r * 128 + 1]
            bent = jnp.tanh(dot(query, keys, 1, 1) * (1.0 / soft_cap))
            probs = jnp.exp(soft_cap * bent - lse)
            if allowed is not None:
                probs = jnp.where(allowed, probs, 0.0)
            dprob = dot(grad, values, 1, 1)
            dscore = (probs * (dprob - dsum) * (1.0 - bent * bent)).astype(bf16)
            dq_ref[q_rows, cols] += dot(dscore, keys)
            acc[k_rows, :HEAD_DIM] += dot(dscore, query, 0, 0)
            acc[k_rows, HEAD_DIM:] += dot(probs.astype(bf16), grad, 0, 0)

    over_pairs(span, q_ref.shape[0] // span, chunk, qp, kp, bd, work)
    dkv_ref[...] = acc[...].astype(dkv_ref.dtype)


def attend_back(q, grad, lse, dsum, kv, q_pos, k_pos, boundary, span):
    rows, width = q.shape
    repeat = width // HEAD_DIM
    count = kv.shape[0] // span
    chunk = key_chunk(count)
    fixed = lambda w: pl.BlockSpec((rows, w), lambda j, *_: (0, 0))
    moving = pl.BlockSpec((chunk * span, kv.shape[1]), lambda j, *_: (j, 0))
    spec = pltpu.PrefetchScalarGridSpec(
        num_scalar_prefetch=3,
        grid=(count // chunk,),
        in_specs=[fixed(width), fixed(width), fixed(128 * repeat), fixed(128 * repeat), moving],
        out_specs=[fixed(width), moving],
        scratch_shapes=[pltpu.VMEM((chunk * span, kv.shape[1]), f32)],
    )
    return pl.pallas_call(
        functools.partial(attend_back_kernel, span, repeat, chunk),
        out_shape=[
            jax.ShapeDtypeStruct((rows, width), f32),
            jax.ShapeDtypeStruct(kv.shape, bf16),
        ],
        grid_spec=spec,
        compiler_params=pltpu.CompilerParams(dimension_semantics=("arbitrary",)),
        cost_estimate=pl.CostEstimate(
            flops=5 * rows * kv.shape[0] * width,
            bytes_accessed=2 * kv.size * 2,
            transcendentals=rows * kv.shape[0] * repeat,
        ),
    )(q_pos, k_pos, boundary, q, grad, lse, dsum, kv)


def on_device(
    plan,
    tokens,
    cotangent,
    span_order,
    segments,
    w_query,
    w_key,
    w_value,
    w_out,
    w_gate,
    w_up,
    w_down,
    gain_attn_in,
    gain_attn_out,
    gain_ffn_in,
    gain_ffn_out,
):
    rows, width = tokens.shape
    contexts, ulysses = plan.contexts, plan.ulysses
    layers, sides, cores, halves = plan.layers, plan.sides, plan.cores, plan.halves
    group_rows = rows * ulysses
    span = group_rows // 2
    q_scale = float(HEAD_DIM) ** (-0.5)
    ctx = lax.axis_index("ctx")
    layer, side, row, core = plan.here()

    ctx_ring = Ring(
        plan, sides, layers, lambda w, out, inn: (inn, out, w[2], w[3]), lambda w: (w[1], w[0])
    )
    ffn_ring = Ring(
        plan, plan.rows, layers, lambda w, out, inn: (inn, w[1], out, w[3]), lambda w: (w[2], w[0])
    )
    side_ring = Ring(
        plan, 1, sides, lambda w, out, inn: (w[0], inn, w[2], w[3]), lambda w: (0, w[1])
    )
    row_ring = Ring(
        plan, 1, plan.rows, lambda w, out, inn: (w[0], w[1], inn, w[3]), lambda w: (0, w[2])
    )
    core_ring = Ring(
        plan, 1, cores, lambda w, out, inn: (w[0], w[1], w[2], inn), lambda w: (0, w[3])
    )
    ctx_cells = jnp.array([inn * sides + out for out, inn in ctx_ring.cells], jnp.int32)
    ctx_place = ctx_ring.position(side, layer)
    ring_ctx = [ctx_cells[(ctx_place + k) % contexts] for k in range(contexts)]

    def group_gather(values):
        mine = ring_gather(values, row_ring)
        blocks, where = [], []
        for k, block in enumerate(mine):
            for m, found in enumerate(ring_gather(block, core_ring)):
                blocks.append(found)
                where.append((row + k) % plan.rows * cores + (core + m) % cores)
        return place_rows(blocks, where, ulysses).reshape(group_rows, values.shape[1])

    def group_scatter(values):
        parts = values.reshape(plan.rows, cores, rows, values.shape[1])

        def part(k, m):
            at = ((row + k) % plan.rows, (core + m) % cores, 0, 0)
            return lax.dynamic_slice(parts, at, (1, 1, *parts.shape[2:]))[0, 0]

        summed = [
            ring_scatter([part(k, m) for m in range(cores)], core_ring) for k in range(plan.rows)
        ]
        return ring_scatter(summed, row_ring)

    def ctx_scatter(arrays):
        size = arrays[0].shape[0] // contexts

        def part(k):
            blocks = [take_block(array, ring_ctx[k], size) for array in arrays]
            return jnp.concatenate(blocks, axis=1) if len(blocks) > 1 else blocks[0]

        return ring_scatter([part(k) for k in range(contexts)], ctx_ring, bf16)

    shard = gain_attn_in.shape[0]
    packed = jnp.stack([gain_attn_in, gain_attn_out, gain_ffn_in, gain_ffn_out])
    packed = jnp.pad(packed, ((0, 4), (0, -shard % 128)))
    tok_group, col_qkv, col_out, gains, ffn_gate = fetch_weights(
        plan, tokens, w_query, w_key, w_value, w_out, packed.astype(f32), w_gate
    )
    tok_group = tok_group.reshape(group_rows, width)
    col_qkv = col_qkv.reshape(width, -1)
    col_out = col_out.reshape(width, -1)
    gains = jnp.transpose(gains[:, :4, :shard], (1, 0, 2)).reshape(4, width)
    weight_one, weight_two, weight_three, weight_four = (1.0 + gains[k][None] for k in range(4))

    own_spans = lax.dynamic_slice_in_dim(span_order, 2 * ctx, 2, 0) * span
    boundary = jnp.sum((segments == 0).astype(jnp.int32)).reshape(1)
    key_spans = span_order * span
    group_pos = (own_spans[:, None] + jnp.arange(span, dtype=jnp.int32)[None, :]).reshape(-1)
    half = HEAD_DIM // 2
    freqs = rotary_base ** (-jnp.arange(half).astype(f32) / half)
    angles = group_pos.astype(f32)[:, None] * freqs[None, :]
    cosines, sines = jnp.cos(angles), jnp.sin(angles)

    q_cols, k_cols = w_query.shape[1] // ulysses, w_key.shape[1] // ulysses
    tok_rows = tok_group.astype(f32)
    normed_in = norm_apply(tok_rows, weight_one).astype(bf16)
    qkv = dot(normed_in, col_qkv)
    queries = (rotary(qkv[:, :q_cols], cosines, sines, 1.0) * q_scale).astype(bf16)
    keys = rotary(qkv[:, q_cols : q_cols + k_cols], cosines, sines, 1.0).astype(bf16)
    values = qkv[:, q_cols + k_cols :].astype(bf16)
    kv, ffn_up = fetch_keys(plan, jnp.concatenate([keys, values], axis=1), w_up)
    kv = kv.reshape(contexts * group_rows, -1)
    ffn_gate, ffn_up = ffn_gate.reshape(width, -1), ffn_up.reshape(width, -1)

    slice_cols = w_gate.shape[1] // halves

    def slice_perm(p):
        def target(l, s, r, c):
            return c * halves + (l + p) % halves, s, r, (l // halves + 1) % cores

        return plan.perm(target)

    def slice_back(p):
        return [(b, a) for a, b in slice_perm(p)]

    def pick(options, index):
        out = options[0]
        for k in range(1, len(options)):
            out = jnp.where(index == k, options[k], out)
        return out

    def slice_fetch(weights):
        cuts = [weights[:, h * slice_cols : (h + 1) * slice_cols] for h in range(halves)]
        size = weights.shape[0]
        got = [move(pick(cuts, (layer + p) % halves), slice_perm(p)) for p in range(halves)]
        sided = ring_gather(jnp.concatenate(got, axis=0), side_ring)
        cored = ring_gather(jnp.concatenate(sided, axis=0), core_ring)
        blocks, where = [], []
        for m, found in enumerate(cored):
            for k in range(sides):
                for p in range(halves):
                    n = k * halves + p
                    blocks.append(found[n * size : (n + 1) * size])
                    origin = (core + m + cores - 1) % cores * halves + (layer - p) % halves
                    where.append(origin * sides + (side + k) % sides)
        return place_rows(blocks, where, contexts).reshape(width, slice_cols)

    def slice_start(lefts, right, earlier):
        others = []
        for m in range(1, cores):
            piece = dot(after(lefts[m], earlier), right, 0, 0).astype(bf16)
            perm = plan.perm(lambda l, s, r, c, m=m: (l, s, r, (c + m) % cores))
            others.append(move(piece, perm))
        own = dot(after(lefts[0], earlier), right, 0, 0).astype(bf16)
        arrays = [x.reshape(halves, sides, -1, slice_cols) for x in (own, *others)]
        size = arrays[0].shape[2]

        def side_part(k):
            at = (0, (side + k) % sides, 0, 0)
            shape = (halves, 1, size, slice_cols)
            found = sum(lax.dynamic_slice(x, at, shape).astype(f32) for x in arrays)
            return found.reshape(halves * size, slice_cols)

        sent = [side_part(k).astype(bf16) for k in range(1, sides)]
        summed = ring_scatter([side_part(0), *sent], side_ring, bf16)
        return summed.astype(bf16).reshape(halves, size, slice_cols)

    def slice_end(summed):
        got = []
        for p in range(halves):
            piece = lax.dynamic_index_in_dim(summed, (layer - p) % halves, 0, keepdims=False)
            got.append(move(piece, slice_back(p)))
        cuts = [pick(got, (h - layer) % halves) for h in range(halves)]
        return jnp.concatenate(cuts, axis=1).astype(f32)

    ffn_down = slice_fetch(after(w_down, kv))
    head_o, lse = attend(queries, kv, own_spans, key_spans, boundary, span)
    attn_out = group_scatter(dot(head_o, col_out, 1, 1).astype(bf16))
    tok_own = tokens.astype(f32)
    hidden_in = tok_own + norm_apply(attn_out, weight_two)
    normed_own = norm_apply(hidden_in, weight_three).astype(bf16)

    size = ffn_ring.size
    order = [0]
    for k in range(1, size // 2):
        order += [k, size - k]
    order.append(size // 2)
    near = max(size - 3, 1)

    def ffn_gather(values):
        found = ring_gather(values, ffn_ring)
        return [
            jnp.concatenate([found[k] for k in ks], axis=0) for ks in (order[:near], order[near:])
        ]

    def ffn_scatter(chunk):
        parts = [None] * size
        far = chunk(1, None)
        for values, ks in ((far, order[near:]), (chunk(0, far), order[:near])):
            for n, k in enumerate(ks):
                parts[k] = values[n * rows : (n + 1) * rows]
        landed = []
        return ring_scatter(parts, ffn_ring, bf16, landed), landed

    normed_mid = ffn_gather(normed_own)
    gate = [dot(x, ffn_gate) for x in normed_mid]
    upper = [dot(x, ffn_up) for x in normed_mid]
    hidden = [(gelu_parts(g)[0] * u).astype(bf16) for g, u in zip(gate, upper, strict=True)]

    def down_part(n, far):
        rows_in = hidden[n] if far is None else after(hidden[n], far)
        return dot(rows_in, ffn_down, 1, 1).astype(bf16)

    ffn_out, _ = ffn_scatter(down_part)
    block_out = (hidden_in + norm_apply(ffn_out, weight_four)).astype(bf16)
    cot_own = cotangent.astype(f32)
    d_ffn = ffn_gather(norm_grad(ffn_out, weight_four, cot_own).astype(bf16))
    d_gate, d_upper = [], []
    for n in range(2):
        d_hidden = dot(d_ffn[n], ffn_down)
        gate_value, gate_slope = gelu_parts(gate[n])
        d_gate.append((d_hidden * upper[n] * gate_slope).astype(bf16))
        d_upper.append((d_hidden * gate_value).astype(bf16))

    def mid_part(n, far):
        left, right = d_gate[n], d_upper[n]
        if far is not None:
            left, right = after(left, far), after(right, far)
        first = lax.optimization_barrier(dot(left, ffn_gate, 1, 1).astype(bf16))
        return (first.astype(f32) + dot(right, ffn_up, 1, 1)).astype(bf16)

    d_mid, landed = ffn_scatter(mid_part)
    grad_hidden = cot_own + norm_grad(hidden_in, weight_three, d_mid)

    def by_core(pieces):
        cols = width // cores
        place = lambda m: (core + m + cores - 1) % cores * cols
        cut = lambda x, m: lax.dynamic_slice_in_dim(x, place(m), cols, 1)
        return [jnp.concatenate([cut(x, m) for x in pieces], axis=0) for m in range(cores)]

    d_ffn, normed_mid = by_core(d_ffn), by_core(normed_mid)
    hidden, d_gate, d_upper = (jnp.concatenate(x, axis=0) for x in (hidden, d_gate, d_upper))
    sum_down = slice_start(d_ffn, hidden, landed[0])
    sum_gate = slice_start(normed_mid, d_gate, landed[min(1, len(landed) - 1)])
    sum_up = slice_start(normed_mid, d_upper, d_mid)
    grad_down = slice_end(after(sum_down, d_mid))
    grad_gate = slice_end(after(sum_gate, d_mid))

    d_attn = group_gather(norm_grad(attn_out, weight_two, grad_hidden).astype(bf16))
    out_part = dot(d_attn, head_o, 0, 0).astype(bf16)
    grad_o = dot(d_attn, col_out).astype(bf16)
    products = grad_o.astype(f32) * head_o.astype(f32)
    dsum = jnp.concatenate(
        [
            jnp.broadcast_to(
                jnp.sum(products[:, s : s + HEAD_DIM], axis=1, keepdims=True), (group_rows, 128)
            )
            for s in range(0, q_cols, HEAD_DIM)
        ],
        axis=1,
    )
    grad_q, grad_kv = attend_back(
        queries, grad_o, lse, dsum, kv, own_spans, key_spans, boundary, span
    )
    grad_kv = ctx_scatter([grad_kv])
    grad_up = slice_end(after(sum_up, grad_q))
    grad_q = (rotary(grad_q, cosines, sines, -1.0) * q_scale).astype(bf16)
    k_cosines, k_sines = after(cosines, grad_kv), after(sines, grad_kv)
    grad_k = rotary(grad_kv[:, :k_cols], k_cosines, k_sines, -1.0).astype(bf16)
    grad_v = grad_kv[:, k_cols:].astype(bf16)
    grad_kv = jnp.concatenate([grad_k, grad_v], axis=1)
    q_part = dot(normed_in, grad_q, 0, 0).astype(bf16)
    kv_part = dot(normed_in, grad_kv, 0, 0).astype(bf16)
    d_in_part = dot(grad_q, col_qkv[:, :q_cols], 1, 1)
    d_in_part = (d_in_part + dot(grad_kv, col_qkv[:, q_cols:], 1, 1)).astype(bf16)

    gain_parts = jnp.stack(
        [
            gain_part(attn_out, after(grad_hidden, grad_q)),
            gain_part(hidden_in, after(d_mid, grad_q)),
            gain_part(ffn_out, after(cot_own, grad_q)),
        ]
    ).reshape(3, contexts * ulysses, shard)
    gain_parts = jnp.pad(jnp.transpose(gain_parts, (1, 0, 2)), ((0, 0), (0, 5), (0, -shard % 128)))
    grad_query, grad_key, grad_value, grad_outproj, d_in, gain_grads = sum_grads(
        plan,
        q_part.reshape(contexts * ulysses, shard, -1),
        kv_part.reshape(contexts * ulysses, shard, -1),
        out_part.reshape(contexts * ulysses, shard, -1),
        d_in_part.reshape(ulysses, rows, width),
        gain_parts,
        w_query.shape[1],
        w_key.shape[1],
    )
    grad_outproj = grad_outproj.reshape(w_out.shape)
    gain_grads = gain_grads[:, :shard]
    grad_tokens = grad_hidden + norm_grad(tok_own, weight_one, d_in)
    products = [
        jnp.sum(w.astype(f32) * g, axis=1)
        for w, g in ((w_query, grad_query), (w_key, grad_key), (w_value, grad_value))
    ]
    gain_first = (products[0] + products[1] + products[2]) / (1.0 + gain_attn_in.astype(f32))
    return (
        block_out,
        grad_tokens,
        grad_query,
        grad_key,
        grad_value,
        grad_outproj,
        grad_gate,
        grad_up,
        grad_down,
        gain_first,
        gain_grads[0],
        gain_grads[1],
        gain_grads[2],
    )


def solution(mesh):
    flat, cut, line = P(AXES, None), P("ctx", "uly"), P(AXES)
    in_specs = (flat, flat, P(), P(), flat, flat, flat, cut, cut, cut, cut, line, line, line, line)
    out_specs = (flat, flat, flat, flat, flat, cut, cut, cut, cut, line, line, line, line)
    plan = Plan(mesh)

    def body(*args):
        return on_device(plan, *args)

    return jax.shard_map(
        body, mesh=mesh, in_specs=in_specs, out_specs=out_specs, check_vma=False
    )
```
